32 devices in a mesh: mod: 4 (over y, x), seq: 8 (over z, core).
Axes of the slice: x: 2, y: 2, z: 4, core: 2. Of those that a mesh axis runs over, the one named last changes fastest.
Arguments:
- tokens: bfloat16 [2048, 4096], P(('mod', 'seq')), may hold values from -6 to 6
- norm_gain: float32 [3, 4096], replicated, may hold values from 0.2 to 2.6
- qkv_weight: bfloat16 [3, 4096, 12288], P(None, None, 'seq'), may hold values from -0.45 to 0.45
- out_weight: bfloat16 [3, 4096, 4096], P(None, 'seq'), may hold values from -0.375 to 0.375
- modality: int32 [16], replicated, may hold values from 0 to 2
- doc_lengths: int32 [4], replicated, may hold values from 1 to 1024, 2048 in all
Outputs:
- mixed: bfloat16 [2048, 4096], P(('mod', 'seq'))
The draws below stay inside these ranges and needn't reach their ends.
Inputs may be any that keep to these rules, and one draw needn't show every extreme that they name: `doc_lengths`: the lengths sum to 2048; documents follow one another from position 0 in the given order.
All inputs are finite; a program needn't handle non-finite values.
Results may differ from the reference program's by a relative error of at most 0.015.
Values may be sent and summed in bfloat16 or wider, within the bound.
No kernel may reach another device: no remote copies, remote signals or barrier semaphores. Data moves between devices by JAX's collectives and lax.ppermute only.
A program may use at most 128 MiB of HBM per device.

```python
import math
import jax
import jax.numpy as jnp
import numpy as np
from jax import lax

D = 4096
HEADS = 32
HDIM = 128
MODS = 3
DOCS = 4
BLOCK = 128
TOKENS = 2048
BLOCKS = 16
HEAD_DEV = 4
FEATS = 4096
N_SEQ = 8


def draw_norm_gain(key, part):
    normal_draw = jax.random.uniform(jax.random.fold_in(key, 1), (MODS, D), jnp.float32, 0.6, 1.5)
    return normal_draw


def draw_qkv_weight(key, part):
    normal_draw = jax.random.normal(jax.random.fold_in(key, 3), (MODS, D, HEADS, 3, HDIM), jnp.float32)
    fan_scale = 1.0 / jnp.sqrt(jnp.float32(D))
    shared = normal_draw[:, :, :, 0:1, :] * 1.2 * fan_scale
    key_part = normal_draw[:, :, :, 1:2, :] * 1.2 * fan_scale
    values = normal_draw[:, :, :, 2:3, :] * fan_scale
    stacked = jnp.concatenate([shared, key_part, values], axis=3)
    return jnp.clip(stacked, -0.45, 0.45).reshape(MODS, D, HEADS * 3 * HDIM).astype(jnp.bfloat16)


def plant(values, rng, low, largest):
    spot = [jax.random.randint(jax.random.fold_in(rng, axis), (), 0, length) for axis, length in enumerate(values.shape)]
    widest = values.shape.index(max(values.shape))
    beside = spot[:widest] + [(spot[widest] + 1) % values.shape[widest]] + spot[widest + 1:]
    return values.at[tuple(spot)].set(low).at[tuple(beside)].set(largest)


def block_levels(key, dims, split, smallest, high):
    gain, own = 1.0, jax.random.fold_in(key, 6)
    for axis_at, blocks in split:
        draws = jnp.exp(jax.random.uniform(jax.random.fold_in(own, axis_at), (blocks,), jnp.float32, smallest / len(split), high / len(split)))
        gain = gain * jnp.repeat(draws, dims[axis_at] // blocks).reshape([-1 if axis == axis_at else 1 for axis in range(len(dims))])
    return gain


def rank_bounds(amount, slope):
    loads = [(1 << 20) // math.isqrt(grade ** slope) + 1 for grade in range(1, amount + 1)]
    spread = 1 + sum(loads) // (1 << 30)
    return np.cumsum(np.array([max(1, weight // spread) for weight in loads]))


def ranked(own_key, extent, amount, lean):
    grid = rank_bounds(amount, lean)
    lot = jax.random.randint(jax.random.fold_in(own_key, 1), extent, 0, int(grid[amount - 1]))
    grade = jnp.searchsorted(jnp.asarray(grid, jnp.int32), lot, side="right")
    return jax.random.permutation(jax.random.fold_in(own_key, 2), amount)[grade].astype(jnp.int32)


def profile(count, total, most, slope):
    weights = [(1 << 20) // math.isqrt(rank ** slope) + 1 for rank in range(2, count + 1)]
    surplus, counts = total - most - (count - 1), [1] * (count - 1)
    while surplus > 0:
        free = [i for i in range(count - 1) if counts[i] < most]
        whole, remaining = sum([weights[i] for i in free]), surplus
        for i in free:
            addition = min(most - counts[i], max(1, remaining * weights[i] // whole), surplus)
            counts[i] = counts[i] + addition
            surplus = surplus - addition
    return np.array([most] + counts)


def ragged_sizes(key, amount, total, limit, lean):
    if amount == 2:
        one = jax.random.randint(key, (), max(1, total - limit), min(limit, total - 1) + 1)
        return jnp.stack([one, total - one])
    sizes = jnp.asarray(profile(amount, total, limit, lean), jnp.int32)
    twos = (amount - 1) // 2
    donor, receiver = sizes[1:1 + 2 * twos:2], sizes[2:2 + 2 * twos:2]
    margin = jnp.minimum(donor - 1, limit - receiver)
    passed = jax.random.randint(jax.random.fold_in(key, 1), (twos,), 0, 1 << 20) % (margin + 1)
    sizes = sizes.at[1:1 + 2 * twos:2].set(donor - passed).at[2:2 + 2 * twos:2].set(receiver + passed)
    return sizes[jax.random.permutation(jax.random.fold_in(key, 2), amount)]


def scatter_about(rng, extent, deviation, limit, shards=(), kind=jnp.bfloat16):
    values = jax.random.normal(rng, extent, jnp.float32) * deviation
    if len(shards) > 0:
        values = block_levels(rng, extent, shards, -0.22, 0.18) * values
    return jnp.clip(values, min=-limit, max=limit).astype(kind)


def setup_inputs(seed: int = 0) -> dict:
    arg_keys = jax.random.split(jax.random.key(seed), 7)
    return {
        "tokens": scatter_about(arg_keys[0], (TOKENS, D), 1.0, 6.0, ((0, 32),)),
        "norm_gain": draw_norm_gain(jax.random.fold_in(arg_keys[6], 71), 0),
        "qkv_weight": draw_qkv_weight(jax.random.fold_in(arg_keys[6], 71), 0),
        "out_weight": scatter_about(arg_keys[3], (MODS, FEATS, D), (FEATS // 16) ** -0.5, 0.375, ((1, 8),)),
        "modality": plant(ranked(arg_keys[4], (BLOCKS,), MODS, 2), jax.random.fold_in(arg_keys[4], 3), 0, MODS - 1).astype(jnp.int32),
        "doc_lengths": ragged_sizes(arg_keys[5], DOCS, TOKENS, TOKENS // 2, 1).astype(jnp.int32),
    }


def reference(tokens, norm_gain, qkv_weight, out_weight, modality, doc_lengths):
    block_rows = tokens.reshape(BLOCKS, BLOCK, D).astype(jnp.float32)
    gain_rows = norm_gain[modality.astype(jnp.int32)]
    mean_square = lax.optimization_barrier(jnp.mean(block_rows * block_rows, axis=2, keepdims=True))
    normed = (block_rows * lax.rsqrt(mean_square + 1e-05) * gain_rows[:, None, :]).astype(jnp.bfloat16)

    def project(block_pair):
        row_block, block_mode = block_pair
        weight = lax.dynamic_index_in_dim(qkv_weight, block_mode, 0, keepdims=False)
        return jnp.dot(row_block, weight, preferred_element_type=jnp.float32).astype(jnp.bfloat16)
    projected = lax.map(project, (normed, modality))
    heads_first = jnp.moveaxis(projected.reshape(TOKENS, HEADS, 3, HDIM), 1, 0)
    doc_ends = jnp.cumsum(doc_lengths).astype(jnp.int32)
    position = jnp.arange(TOKENS, dtype=jnp.int32)
    document = lax.optimization_barrier(jnp.sum((position[:, None] >= doc_ends[None, :]).astype(jnp.int32), axis=1))
    allowed = (position[None, :] <= position[:, None]) & (document[None, :] == document[:, None])
    score_scale = 1.0 / math.sqrt(HDIM)

    def attend(one_head):
        scores = jnp.dot(one_head[:, 0, :], one_head[:, 1, :].T, preferred_element_type=jnp.float32) * score_scale
        row_max = lax.optimization_barrier(jnp.max(jnp.where(allowed, scores, -1e+30), axis=1, keepdims=True))
        weights = jnp.where(allowed, jnp.exp(scores - row_max), 0.0)
        totals = lax.optimization_barrier(jnp.sum(weights, axis=1, keepdims=True))
        summed = jnp.dot(weights.astype(jnp.bfloat16), one_head[:, 2, :], preferred_element_type=jnp.float32)
        return (summed / totals).astype(jnp.bfloat16)
    attended = lax.map(attend, heads_first)
    merged = jnp.moveaxis(attended, 0, 1).reshape(BLOCKS, BLOCK, N_SEQ, HEAD_DEV * HDIM)

    def output(block_pair):
        row_block, block_mode = block_pair
        weight = lax.dynamic_index_in_dim(out_weight, block_mode, 0, keepdims=False)
        weight = weight.reshape(N_SEQ, HEAD_DEV * HDIM, D).astype(jnp.float32)
        parts = jnp.einsum('bgc,gcd->gbd', row_block.astype(jnp.float32), weight)
        rounded = lax.optimization_barrier(parts.astype(jnp.bfloat16))
        return lax.optimization_barrier(jnp.sum(rounded.astype(jnp.float32), axis=0))
    projected_back = lax.map(output, (merged, modality)).reshape(TOKENS, D)
    return (tokens.astype(jnp.float32) + projected_back).astype(jnp.bfloat16)
```

```python
import math

import jax
import jax.numpy as jnp
from jax import lax
from jax.experimental import pallas as pl
from jax.experimental.pallas import tpu as pltpu
from jax.sharding import PartitionSpec as P

HDIM = 128
BLOCK = 128


def modes_of_rows(first_row, row_count, modality):
    block_ids = (first_row + jnp.arange(row_count, dtype=jnp.int32)) // BLOCK
    block_table = jnp.arange(modality.shape[0], dtype=jnp.int32)
    picked = jnp.where(block_ids[:, None] == block_table[None, :], modality[None, :], 0)
    return jnp.sum(picked, axis=1)


def documents(positions, doc_lengths):
    doc_ends = jnp.cumsum(doc_lengths)
    return jnp.sum((positions[:, None] >= doc_ends[None, :]).astype(jnp.int32), axis=1)


def general_body(tokens, norm_gain, qkv_weight, out_weight, modality, doc_lengths):
    row_count = tokens.shape[0]
    seq_count = lax.axis_size("seq")
    mod_count = lax.axis_size("mod")
    group_rows = row_count * seq_count
    mod_index = lax.axis_index("mod")
    own_first = (mod_index * seq_count + lax.axis_index("seq")) * row_count
    row_modes = modes_of_rows(own_first, row_count, modality)
    choose = (
        row_modes[:, None, None] == jnp.arange(norm_gain.shape[0], dtype=jnp.int32)[None, :, None]
    )
    gain_rows = jnp.sum(jnp.where(choose, norm_gain[None, :, :], 0.0), axis=1)
    values = tokens.astype(jnp.float32)
    mean_square = jnp.mean(values * values, axis=1, keepdims=True)
    normed = (values * lax.rsqrt(mean_square + 1e-05) * gain_rows).astype(jnp.bfloat16)
    gathered = lax.all_gather(normed, "seq", axis=0, tiled=True)
    group_first = mod_index * group_rows
    block_count = group_rows // BLOCK
    block_modes = lax.dynamic_slice_in_dim(modality, group_first // BLOCK, block_count)
    heads_here = qkv_weight.shape[2] // (3 * HDIM)

    def project(block_pair):
        row_block, block_mode = block_pair
        weight = lax.dynamic_index_in_dim(qkv_weight, block_mode, 0, keepdims=False)
        return jnp.dot(row_block, weight, preferred_element_type=jnp.float32).astype(jnp.bfloat16)

    projected = lax.map(
        project, (gathered.reshape(block_count, BLOCK, gathered.shape[1]), block_modes)
    )
    projected = projected.reshape(group_rows, heads_here, 3, HDIM)
    queries = projected[:, :, 0, :]
    keys_here = projected[:, :, 1, :]
    values_here = projected[:, :, 2, :]
    quarter = group_rows // mod_count
    local_rows = jnp.arange(group_rows, dtype=jnp.int32)
    query_pos = group_first + local_rows
    query_docs = documents(query_pos, doc_lengths)
    block_size = min(512, quarter)
    block_total = group_rows // block_size
    score_scale = 1.0 / math.sqrt(HDIM)
    query_blocks = queries.reshape(block_total, block_size, heads_here, HDIM)
    pos_blocks = query_pos.reshape(block_total, block_size)
    doc_blocks = query_docs.reshape(block_total, block_size)
    piece_keys = lax.all_gather(keys_here, "mod", axis=0, tiled=True)
    piece_values = lax.all_gather(values_here, "mod", axis=0, tiled=True)
    key_pos = jnp.arange(piece_keys.shape[0], dtype=jnp.int32)
    key_docs = documents(key_pos, doc_lengths)

    def one_block(block_state):
        query_block, block_pos, block_docs = block_state
        scores = (
            jnp.einsum("qhc,khc->hqk", query_block, piece_keys, preferred_element_type=jnp.float32)
            * score_scale
        )
        allowed = (
            (key_pos[None, :] <= block_pos[:, None]) & (key_docs[None, :] == block_docs[:, None])
        )[None, :, :]
        row_max = jnp.max(jnp.where(allowed, scores, -1e30), axis=2)
        weights = jnp.where(allowed, jnp.exp(scores - row_max[:, :, None]), 0.0)
        totals = jnp.sum(weights, axis=2)
        rows = jnp.einsum(
            "hqk,khc->qhc",
            weights.astype(jnp.bfloat16),
            piece_values,
            preferred_element_type=jnp.float32,
        )
        return (rows / jnp.transpose(totals)[:, :, None]).astype(jnp.bfloat16)

    attended = lax.map(one_block, (query_blocks, pos_blocks, doc_blocks))
    attended = attended.reshape(group_rows, heads_here * HDIM)

    def output(block_pair):
        row_block, block_mode = block_pair
        weight = lax.dynamic_index_in_dim(out_weight, block_mode, 0, keepdims=False)
        return jnp.dot(row_block, weight, preferred_element_type=jnp.float32)

    partial_value = lax.map(
        output, (attended.reshape(block_count, BLOCK, attended.shape[1]), block_modes)
    )
    head_sums = lax.psum_scatter(
        partial_value.reshape(group_rows, partial_value.shape[2]).astype(jnp.bfloat16),
        "seq",
        scatter_dimension=0,
        tiled=True,
    ).astype(jnp.float32)
    return (tokens.astype(jnp.float32) + head_sums).astype(jnp.bfloat16)


def smem_spec():
    return pl.BlockSpec(memory_space=pltpu.SMEM)


def vmem_spec():
    return pl.BlockSpec(memory_space=pltpu.VMEM)


def norm_rows(tokens, norm_gain, mode):
    rows, width = tokens.shape

    def kernel(mode_ref, tokens_ref, gain_ref, out_ref):
        gain = gain_ref[pl.ds(mode_ref[0], 1), :]
        step = 16
        for first in range(0, rows, step):
            values = tokens_ref[first : first + step, :].astype(jnp.float32)
            mean_square = jnp.sum(values * values, axis=1, keepdims=True) * (1.0 / width)
            scaled = values * lax.rsqrt(mean_square + 1e-05) * gain
            out_ref[first : first + step, :] = scaled.astype(jnp.bfloat16)

    return pl.pallas_call(
        kernel,
        out_shape=jax.ShapeDtypeStruct((rows, width), jnp.bfloat16),
        in_specs=[smem_spec(), vmem_spec(), vmem_spec()],
        out_specs=vmem_spec(),
        cost_estimate=pl.CostEstimate(flops=4_000_000, bytes_accessed=1 << 20, transcendentals=64),
        name="norm_rows",
    )(mode, tokens, norm_gain)


def project_slots(parts, weight, info):
    slots = len(parts)
    half, width = parts[0][0].shape
    block = 2 * half
    cols = 3 * HDIM
    heads = weight.shape[2] // cols

    def kernel(info_ref, *refs):
        ins = refs[: 2 * slots]
        weight_ref = refs[2 * slots]
        outs = refs[2 * slots + 1 : 2 * slots + 1 + heads]
        rows_ref = refs[-1]
        head_step = pl.program_id(0)
        slot = pl.program_id(1)

        @pl.when((head_step == 0) & (slot == 0))
        def _():
            for s in range(slots):
                rows_ref[s, :half, :] = ins[2 * s][...]
                rows_ref[s, half:, :] = ins[2 * s + 1][...]

        result = jnp.dot(
            rows_ref[slot], weight_ref[0], preferred_element_type=jnp.float32
        ).astype(jnp.bfloat16)
        for d in range(heads):

            @pl.when(head_step == d)
            def _():
                outs[d][pl.ds(pl.multiple_of(slot * block, block), block), :] = result

    row_spec = pl.BlockSpec((half, width), lambda d, s, info: (0, 0))
    out_spec = pl.BlockSpec((slots * block, cols), lambda d, s, info: (0, 0))
    return pl.pallas_call(
        kernel,
        out_shape=[jax.ShapeDtypeStruct((slots * block, cols), jnp.bfloat16)] * heads,
        grid_spec=pltpu.PrefetchScalarGridSpec(
            num_scalar_prefetch=1,
            grid=(heads, slots),
            in_specs=[row_spec] * (2 * slots)
            + [
                pl.BlockSpec(
                    (1, width, cols),
                    lambda d, s, info: (info[s], 0, jnp.bitwise_xor(info[slots], d)),
                )
            ],
            out_specs=[out_spec] * heads,
            scratch_shapes=[pltpu.VMEM((slots, block, width), jnp.bfloat16)],
        ),
        compiler_params=pltpu.CompilerParams(
            dimension_semantics=("arbitrary", "arbitrary"), vmem_limit_bytes=40 << 20
        ),
        cost_estimate=pl.CostEstimate(
            flops=2 * slots * block * width * cols * heads,
            bytes_accessed=slots * width * cols * heads * 2,
            transcendentals=0,
        ),
        name="project_slots",
    )(info, *[piece for pair in parts for piece in pair], weight)


def attend_slots(early, late, info, doc_lengths, query_slots, early_slots, block, chips):
    count = len(early)
    total = count * chips * block
    longest = total // 2
    window = min(longest + block, total)
    half = block // 2
    scale = 1.0 / math.sqrt(HDIM)
    docs = doc_lengths.shape[0]
    n_out = len(query_slots) * count

    def kernel(info_ref, docs_ref, *refs):
        ins = refs[: 2 * count]
        outs = refs[2 * count : 2 * count + n_out]
        keys_ref, values_ref = refs[2 * count + n_out :]
        mu, chip, own_first = info_ref[0], info_ref[1], info_ref[2]

        def slot_rows(d, slot, first, last):
            if slot < early_slots:
                return ins[d][slot * block : (slot + 1) * block, first * HDIM : last * HDIM]
            return ins[count + d][:, first * HDIM : last * HDIM]

        for d in range(count):
            for slot in range(early_slots + 1):
                index = jnp.bitwise_xor(mu, d) * chips + jnp.bitwise_xor(chip, slot)
                place = pl.ds(pl.multiple_of(index * block, block), block)
                keys_ref[place, :] = slot_rows(d, slot, 1, 2)
                values_ref[place, :] = slot_rows(d, slot, 2, 3)

        ends = []
        end = jnp.int32(0)
        for i in range(docs):
            end = end + docs_ref[i]
            ends.append(end)
        row_place = lax.broadcasted_iota(jnp.int32, (block, 1), 0) + own_first
        row_place = jnp.where(row_place >= block, row_place - block, row_place)
        key_iota = lax.broadcasted_iota(jnp.int32, (1, window), 1)
        key_in_block = key_iota % block + own_first
        key_in_block = jnp.where(key_in_block >= block, key_in_block - block, key_in_block)
        key_place = (key_iota // block) * block + key_in_block
        for n, slot in enumerate(query_slots):
            for d in range(count):
                index = jnp.bitwise_xor(mu, d) * chips + jnp.bitwise_xor(chip, slot)
                first_row = index * block
                doc_first = jnp.int32(0)
                for e in ends:
                    doc_first = jnp.where(first_row >= e, e, doc_first)
                start = jnp.minimum(doc_first // block, (total - window) // block) * block
                start = pl.multiple_of(start, block)
                row_pos = row_place + first_row
                row_first = jnp.zeros((block, 1), jnp.int32)
                for e in ends:
                    row_first = jnp.where(row_pos >= e, e, row_first)
                key_pos = key_place + start
                allowed = (key_pos <= row_pos) & (key_pos >= row_first)
                query = slot_rows(d, slot, 0, 1)
                keys = keys_ref[pl.ds(start, window), :]
                scores = lax.dot_general(
                    query, keys, (((1,), (1,)), ((), ())), preferred_element_type=jnp.float32
                )
                scores = jnp.where(allowed, scores * scale, -1e30)
                row_max = jnp.max(scores, axis=1, keepdims=True)
                weights = jnp.where(allowed, jnp.exp(scores - row_max), 0.0)
                totals = jnp.sum(weights, axis=1, keepdims=True)
                summed = jnp.dot(
                    weights.astype(jnp.bfloat16),
                    values_ref[pl.ds(start, window), :],
                    preferred_element_type=jnp.float32,
                )
                outs[n * count + d][...] = (summed / totals).astype(jnp.bfloat16)

    n_queries = len(query_slots) * count
    return pl.pallas_call(
        kernel,
        out_shape=[jax.ShapeDtypeStruct((block, HDIM), jnp.bfloat16)] * n_out,
        in_specs=[smem_spec(), smem_spec()] + [vmem_spec()] * (2 * count),
        out_specs=[vmem_spec()] * n_out,
        scratch_shapes=[
            pltpu.VMEM((total, HDIM), jnp.bfloat16),
            pltpu.VMEM((total, HDIM), jnp.bfloat16),
        ],
        compiler_params=pltpu.CompilerParams(vmem_limit_bytes=24 << 20),
        cost_estimate=pl.CostEstimate(
            flops=n_queries * block * window * HDIM * 8,
            bytes_accessed=3 * total * HDIM * 2,
            transcendentals=n_queries * block * window,
        ),
        name="attend_slots",
    )(info, doc_lengths, *early, *late)


def output_rows(pieces, weight, info):
    count = len(pieces)
    block = pieces[0].shape[0]
    half = block // 2
    depth, width = weight.shape[1:]
    tile = min(1024, width)

    def kernel(info_ref, *refs):
        ins = refs[:count]
        weight_ref, own_ref, partner_ref, heads_ref = refs[count:]

        @pl.when(pl.program_id(0) == 0)
        def _():
            for d in range(count):
                heads_ref[jnp.bitwise_xor(info_ref[1], d)] = ins[d][...]

        rows = jnp.concatenate([heads_ref[h] for h in range(count)], axis=1)
        result = jnp.dot(rows, weight_ref[0], preferred_element_type=jnp.float32)
        result = result.astype(jnp.bfloat16)
        own_ref[...] = result[:half]
        partner_ref[...] = result[half:]

    out_spec = pl.BlockSpec((half, tile), lambda n, info: (0, n))
    return pl.pallas_call(
        kernel,
        out_shape=[jax.ShapeDtypeStruct((half, width), jnp.bfloat16)] * 2,
        grid_spec=pltpu.PrefetchScalarGridSpec(
            num_scalar_prefetch=1,
            grid=(width // tile,),
            in_specs=[pl.BlockSpec((block, HDIM), lambda n, info: (0, 0))] * count
            + [pl.BlockSpec((1, depth, tile), lambda n, info: (info[0], 0, n))],
            out_specs=[out_spec] * 2,
            scratch_shapes=[pltpu.VMEM((count, block, HDIM), jnp.bfloat16)],
        ),
        compiler_params=pltpu.CompilerParams(
            dimension_semantics=("arbitrary",), vmem_limit_bytes=24 << 20
        ),
        cost_estimate=pl.CostEstimate(
            flops=2 * block * depth * width,
            bytes_accessed=depth * width * 2,
            transcendentals=0,
        ),
        name="output_rows",
    )(info, *pieces, weight)


def chip_pairs(pairs):
    return [(2 * a + core, 2 * b + core) for a, b in pairs for core in range(2)]


def line_body(tokens, norm_gain, qkv_weight, out_weight, modality, doc_lengths):
    seq_count = lax.axis_size("seq")
    mod_count = lax.axis_size("mod")
    chips = seq_count // 2
    half = tokens.shape[0]
    block = 2 * half
    mu = lax.axis_index("mod").astype(jnp.int32)
    seq = lax.axis_index("seq").astype(jnp.int32)
    chip, core = seq // 2, seq % 2
    middle = (chip == 1) | (chip == 2)
    group_modes = lax.dynamic_slice_in_dim(modality, mu * chips, chips)
    modes = [
        lax.dynamic_slice_in_dim(group_modes, jnp.bitwise_xor(chip, slot), 1)
        for slot in range(chips)
    ]

    def along(value, pairs):
        return lax.ppermute(value, "seq", chip_pairs(pairs))

    def swap(value):
        return lax.ppermute(value, "seq", [(i, i ^ 1) for i in range(seq_count)])

    def across(value, d):
        return lax.ppermute(value, "mod", [(i, i ^ d) for i in range(mod_count)])

    normed = norm_rows(tokens, norm_gain, modes[0])
    two = along(normed, [(i, i ^ 2) for i in range(chips)])
    one = along(normed, [(i, i ^ 1) for i in range(chips)])
    inner = along(normed, [(1, 2), (2, 1)])
    relayed = along(two, [(2, 3), (1, 0)])
    three = jnp.where(middle, inner, relayed)

    early_parts = [(normed, swap(normed)), (one, swap(one)), (two, swap(two))]
    mu_entry = mu.reshape(1)
    early_out = project_slots(
        early_parts, qkv_weight, jnp.concatenate(modes[:3] + [mu_entry])
    )
    early = [early_out[0]] + [across(early_out[d], d) for d in range(1, mod_count)]
    late_out = project_slots(
        [(three, swap(three))], qkv_weight, jnp.concatenate([modes[3], mu_entry])
    )
    late = [late_out[0]] + [across(late_out[d], d) for d in range(1, mod_count)]

    attend_info = jnp.stack([mu, chip, core * half])

    def attend(slots):
        flat = attend_slots(early, late, attend_info, doc_lengths, slots, 3, block, chips)
        return [flat[i * mod_count : (i + 1) * mod_count] for i in range(len(slots))]

    def finish(pieces, slot):
        pieces = [pieces[0]] + [across(pieces[d], d) for d in range(1, mod_count)]
        own, partner = output_rows(
            pieces, out_weight, jnp.concatenate([modes[slot], mu_entry])
        )
        return (own.astype(jnp.float32) + swap(partner).astype(jnp.float32)).astype(jnp.bfloat16)

    (att3,) = attend((3,))
    sum3 = finish(att3, 3)
    att2, att1, att0 = attend((2, 1, 0))
    from_end = along(sum3, [(3, 2), (0, 1)])
    from_inner = along(sum3, [(1, 2), (2, 1)])
    sum2 = finish(att2, 2)
    from_two_end = along(sum2, [(3, 1), (0, 2)])
    sum2 = (sum2.astype(jnp.float32) + from_end.astype(jnp.float32)).astype(jnp.bfloat16)
    from_two_inner = along(sum2, [(2, 0), (1, 3)])
    sum1 = finish(att1, 1)
    from_one = along(sum1, [(i, i ^ 1) for i in range(chips)])
    sum0 = finish(att0, 0)
    total = tokens.astype(jnp.float32)
    for share in (sum0, from_inner, from_one, from_two_end, from_two_inner):
        total = total + share.astype(jnp.float32)
    return total.astype(jnp.bfloat16)


def solution(mesh):
    def body(tokens, norm_gain, qkv_weight, out_weight, modality, doc_lengths):
        fits = (
            mesh.shape["seq"] == 8
            and mesh.shape["mod"] == 4
            and tokens.shape[0] * 2 == BLOCK
            and qkv_weight.shape[2] == mesh.shape["mod"] * 3 * HDIM
        )
        chosen = line_body if fits else general_body
        return chosen(tokens, norm_gain, qkv_weight, out_weight, modality, doc_lengths)

    return jax.shard_map(
        body,
        mesh=mesh,
        in_specs=(
            P(("mod", "seq"), None),
            P(),
            P(None, None, "seq"),
            P(None, "seq", None),
            P(),
            P(),
        ),
        out_specs=P(("mod", "seq"), None),
        check_vma=False,
    )
```

```python
import math

import jax
import jax.numpy as jnp
from jax import lax
from jax.experimental import pallas as pl
from jax.experimental.pallas import tpu as pltpu
from jax.sharding import PartitionSpec as P


HDIM = 128
BLOCK = 128


def modes_of_rows(first_row, row_count, modality):
    block_ids = (first_row + jnp.arange(row_count, dtype=jnp.int32)) // BLOCK
    block_table = jnp.arange(modality.shape[0], dtype=jnp.int32)
    picked = jnp.where(block_ids[:, None] == block_table[None, :], modality[None, :], 0)
    return jnp.sum(picked, axis=1)


def documents(positions, doc_lengths):
    doc_ends = jnp.cumsum(doc_lengths)
    return jnp.sum((positions[:, None] >= doc_ends[None, :]).astype(jnp.int32), axis=1)


def general_body(tokens, norm_gain, qkv_weight, out_weight, modality, doc_lengths):
    row_count = tokens.shape[0]
    seq_count = lax.axis_size("seq")
    mod_count = lax.axis_size("mod")
    group_rows = row_count * seq_count
    mod_index = lax.axis_index("mod")
    own_first = (mod_index * seq_count + lax.axis_index("seq")) * row_count
    row_modes = modes_of_rows(own_first, row_count, modality)
    choose = (
        row_modes[:, None, None] == jnp.arange(norm_gain.shape[0], dtype=jnp.int32)[None, :, None]
    )
    gain_rows = jnp.sum(jnp.where(choose, norm_gain[None, :, :], 0.0), axis=1)
    values = tokens.astype(jnp.float32)
    mean_square = jnp.mean(values * values, axis=1, keepdims=True)
    normed = (values * lax.rsqrt(mean_square + 1e-05) * gain_rows).astype(jnp.bfloat16)
    gathered = lax.all_gather(normed, "seq", axis=0, tiled=True)
    group_first = mod_index * group_rows
    block_count = group_rows // BLOCK
    block_modes = lax.dynamic_slice_in_dim(modality, group_first // BLOCK, block_count)
    heads_here = qkv_weight.shape[2] // (3 * HDIM)

    def project(block_pair):
        row_block, block_mode = block_pair
        weight = lax.dynamic_index_in_dim(qkv_weight, block_mode, 0, keepdims=False)
        return jnp.dot(row_block, weight, preferred_element_type=jnp.float32).astype(jnp.bfloat16)

    projected = lax.map(
        project, (gathered.reshape(block_count, BLOCK, gathered.shape[1]), block_modes)
    )
    projected = projected.reshape(group_rows, heads_here, 3, HDIM)
    queries = projected[:, :, 0, :]
    keys_here = projected[:, :, 1, :]
    values_here = projected[:, :, 2, :]
    quarter = group_rows // mod_count
    local_rows = jnp.arange(group_rows, dtype=jnp.int32)
    query_pos = group_first + local_rows
    query_docs = documents(query_pos, doc_lengths)
    block_size = min(512, quarter)
    block_total = group_rows // block_size
    score_scale = 1.0 / math.sqrt(HDIM)
    query_blocks = queries.reshape(block_total, block_size, heads_here, HDIM)
    pos_blocks = query_pos.reshape(block_total, block_size)
    doc_blocks = query_docs.reshape(block_total, block_size)
    piece_keys = lax.all_gather(keys_here, "mod", axis=0, tiled=True)
    piece_values = lax.all_gather(values_here, "mod", axis=0, tiled=True)
    key_pos = jnp.arange(piece_keys.shape[0], dtype=jnp.int32)
    key_docs = documents(key_pos, doc_lengths)

    def one_block(block_state):
        query_block, block_pos, block_docs = block_state
        scores = (
            jnp.einsum("qhc,khc->hqk", query_block, piece_keys, preferred_element_type=jnp.float32)
            * score_scale
        )
        allowed = (
            (key_pos[None, :] <= block_pos[:, None]) & (key_docs[None, :] == block_docs[:, None])
        )[None, :, :]
        row_max = jnp.max(jnp.where(allowed, scores, -1e30), axis=2)
        weights = jnp.where(allowed, jnp.exp(scores - row_max[:, :, None]), 0.0)
        totals = jnp.sum(weights, axis=2)
        rows = jnp.einsum(
            "hqk,khc->qhc",
            weights.astype(jnp.bfloat16),
            piece_values,
            preferred_element_type=jnp.float32,
        )
        return (rows / jnp.transpose(totals)[:, :, None]).astype(jnp.bfloat16)

    attended = lax.map(one_block, (query_blocks, pos_blocks, doc_blocks))
    attended = attended.reshape(group_rows, heads_here * HDIM)

    def output(block_pair):
        row_block, block_mode = block_pair
        weight = lax.dynamic_index_in_dim(out_weight, block_mode, 0, keepdims=False)
        return jnp.dot(row_block, weight, preferred_element_type=jnp.float32)

    partial_value = lax.map(
        output, (attended.reshape(block_count, BLOCK, attended.shape[1]), block_modes)
    )
    head_sums = lax.psum_scatter(
        partial_value.reshape(group_rows, partial_value.shape[2]).astype(jnp.bfloat16),
        "seq",
        scatter_dimension=0,
        tiled=True,
    ).astype(jnp.float32)
    return (tokens.astype(jnp.float32) + head_sums).astype(jnp.bfloat16)


SMEM = pl.BlockSpec(memory_space=pltpu.SMEM)
VMEM = pl.BlockSpec(memory_space=pltpu.VMEM)
HBM = pl.BlockSpec(memory_space=pltpu.HBM)
PIECES = 4


def mode_of(ids, modality, chips, slot):
    return modality[ids[0] * chips + jnp.bitwise_xor(ids[1], slot)]


def params(mib):
    return pltpu.CompilerParams(vmem_limit_bytes=mib << 20)


def norm_rows(ids, modality, tokens, norm_gain, chips):
    rows, width = tokens.shape

    def kernel(ids_ref, modality_ref, tokens_ref, gain_ref, out_ref):
        gain = gain_ref[pl.ds(mode_of(ids_ref, modality_ref, chips, 0), 1), :]
        step = 16
        for first in range(0, rows, step):
            values = tokens_ref[first : first + step, :].astype(jnp.float32)
            mean_square = jnp.sum(values * values, axis=1, keepdims=True) * (1.0 / width)
            scaled = values * lax.rsqrt(mean_square + 1e-05) * gain
            out_ref[first : first + step, :] = scaled.astype(jnp.bfloat16)

    return pl.pallas_call(
        kernel,
        out_shape=pltpu.VMEM((rows, width), jnp.bfloat16),
        in_specs=[SMEM, SMEM, VMEM, VMEM],
        out_specs=VMEM,
        compiler_params=params(8),
        cost_estimate=pl.CostEstimate(flops=4_000_000, bytes_accessed=1 << 20, transcendentals=64),
        name="norm_rows",
    )(ids, modality, tokens, norm_gain)


def fetch_weights(ids, modality, qkv_weight, out_weight, chips, slot):
    modes, width, cols = qkv_weight.shape
    pairs = 2
    pair_cols = cols // pairs
    piece = width // PIECES

    def kernel(ids_ref, modality_ref, qkv_ref, out_ref, late_ref, kept_ref, late_sems, kept_sems):
        mode = mode_of(ids_ref, modality_ref, chips, slot)
        copies = []
        for p in range(pairs):
            first = jnp.bitwise_xor(ids_ref[0] // 2, p) * pair_cols
            for k in range(PIECES):
                copies.append(
                    pltpu.make_async_copy(
                        qkv_ref.at[
                            mode,
                            pl.ds(k * piece, piece),
                            pl.ds(pl.multiple_of(first, 128), pair_cols),
                        ],
                        late_ref.at[p, k],
                        late_sems.at[p, k],
                    )
                )
        for m in range(modes):
            copies.append(pltpu.make_async_copy(out_ref.at[m], kept_ref.at[m], kept_sems.at[m]))
        for copy in copies:
            copy.start()
        for copy in copies:
            copy.wait()

    return pl.pallas_call(
        kernel,
        out_shape=[
            pltpu.VMEM((pairs, PIECES, piece, pair_cols), jnp.bfloat16),
            pltpu.VMEM(out_weight.shape, jnp.bfloat16),
        ],
        in_specs=[SMEM, SMEM, HBM, HBM],
        out_specs=[VMEM, VMEM],
        scratch_shapes=[
            pltpu.SemaphoreType.DMA((pairs, PIECES)),
            pltpu.SemaphoreType.DMA((modes,)),
        ],
        compiler_params=params(1),
        cost_estimate=pl.CostEstimate(
            flops=6_000_000_000, bytes_accessed=25 << 20, transcendentals=0
        ),
        name="fetch_weights",
    )(ids, modality, qkv_weight, out_weight)


def store_pair(ids_ref, outs, rows, p, result):
    result = result.astype(jnp.bfloat16)
    cols = result.shape[1] // 2
    odd = ids_ref[0] % 2 == 1
    for e in range(2):
        first, last = result[:, e * cols : (e + 1) * cols], result[:, (1 - e) * cols : (2 - e) * cols]
        outs[2 * p + e][rows, :] = jnp.where(odd, last, first)


def project_slots(ids, modality, parts, weight, chips, slots):
    half, width = parts[0][0].shape
    block = 2 * half
    cols = 3 * HDIM
    heads = weight.shape[2] // cols
    pairs = 2
    pair_cols = weight.shape[2] // pairs
    piece = width // PIECES
    count = len(slots)

    def kernel(ids_ref, modality_ref, *refs):
        ins = refs[: 2 * count]
        weight_ref = refs[2 * count]
        outs = refs[2 * count + 1 : 2 * count + 1 + heads]
        buffer_ref, sems = refs[2 * count + 1 + heads :]

        def copy_of(n, p, k):
            first = jnp.bitwise_xor(ids_ref[0] // 2, p) * pair_cols
            return pltpu.make_async_copy(
                weight_ref.at[
                    mode_of(ids_ref, modality_ref, chips, slots[n]),
                    pl.ds(k * piece, piece),
                    pl.ds(pl.multiple_of(first, 128), pair_cols),
                ],
                buffer_ref.at[p, k],
                sems.at[p, k],
            )

        for p in range(pairs):
            for k in range(PIECES):
                copy_of(0, p, k).start()
        for n in range(count):
            for p in range(pairs):
                result = None
                for k in range(PIECES):
                    copy_of(n, p, k).wait()
                    rows = jnp.concatenate(
                        [ins[2 * n + i][:, k * piece : (k + 1) * piece] for i in range(2)], axis=0
                    )
                    part = jnp.dot(rows, buffer_ref[p, k], preferred_element_type=jnp.float32)
                    result = part if result is None else result + part
                    if n + 1 < count:
                        copy_of(n + 1, p, k).start()
                store_pair(ids_ref, outs, pl.ds(n * block, block), p, result)

    return pl.pallas_call(
        kernel,
        out_shape=[pltpu.VMEM((count * block, cols), jnp.bfloat16)] * heads,
        in_specs=[SMEM, SMEM] + [VMEM] * (2 * count) + [HBM],
        out_specs=[VMEM] * heads,
        scratch_shapes=[
            pltpu.VMEM((pairs, PIECES, piece, pair_cols), jnp.bfloat16),
            pltpu.SemaphoreType.DMA((pairs, PIECES)),
        ],
        compiler_params=params(16),
        cost_estimate=pl.CostEstimate(
            flops=2 * count * block * width * cols * heads,
            bytes_accessed=count * width * cols * heads * 2,
            transcendentals=0,
        ),
        name="project_slots",
    )(ids, modality, *[piece for pair in parts for piece in pair], weight)


def project_late(ids, inner, relayed, weight, cols, chips):
    half, width = inner[0].shape
    block = 2 * half
    pairs, pieces, piece, pair_cols = weight.shape
    heads = pairs * pair_cols // cols

    def kernel(ids_ref, inner_own, inner_partner, relayed_own, relayed_partner, weight_ref, *refs):
        outs, rows_ref = refs[:heads], refs[heads]
        chip = ids_ref[1]
        middle = (chip > 0) & (chip < chips - 1)

        @pl.when(middle)
        def _():
            rows_ref[:half, :] = inner_own[...]
            rows_ref[half:, :] = inner_partner[...]

        @pl.when(jnp.logical_not(middle))
        def _():
            rows_ref[:half, :] = relayed_own[...]
            rows_ref[half:, :] = relayed_partner[...]

        for p in range(pairs):
            result = None
            for k in range(pieces):
                part = jnp.dot(
                    rows_ref[:, k * piece : (k + 1) * piece],
                    weight_ref[p, k],
                    preferred_element_type=jnp.float32,
                )
                result = part if result is None else result + part
            store_pair(ids_ref, outs, pl.ds(0, block), p, result)

    return pl.pallas_call(
        kernel,
        out_shape=[pltpu.VMEM((block, cols), jnp.bfloat16)] * heads,
        in_specs=[SMEM] + [VMEM] * 5,
        out_specs=[VMEM] * heads,
        scratch_shapes=[pltpu.VMEM((block, width), jnp.bfloat16)],
        compiler_params=params(8),
        cost_estimate=pl.CostEstimate(
            flops=2 * block * width * cols * heads,
            bytes_accessed=width * cols * heads * 2,
            transcendentals=0,
        ),
        name="project_late",
    )(ids, *inner, *relayed, weight)


def attend_slots(ids, doc_lengths, sets, query_slots, chips):
    count = len(sets[0][1])
    block = sets[0][1][0].shape[0] // len(sets[0][0])
    total = count * chips * block
    window = min(total // 2 + block, total)
    scale = 1.0 / math.sqrt(HDIM)
    docs = doc_lengths.shape[0]

    def kernel(ids_ref, docs_ref, *refs):
        ins = refs[: len(sets) * count]
        outs = refs[len(sets) * count : (len(sets) + 1) * count]
        keys_ref, values_ref = refs[(len(sets) + 1) * count :]
        mu, chip, own_first = ids_ref[0], ids_ref[1], ids_ref[2] * (block // 2)

        def slot_rows(d, slot, part):
            for i, (slots, _) in enumerate(sets):
                if slot in slots:
                    at = slots.index(slot) * block
                    return ins[i * count + d][at : at + block, part * HDIM : (part + 1) * HDIM]

        for d in range(count):
            for slot in range(chips):
                index = jnp.bitwise_xor(mu, d) * chips + jnp.bitwise_xor(chip, slot)
                place = pl.ds(pl.multiple_of(index * block, block), block)
                keys_ref[place, :] = slot_rows(d, slot, 1)
                values_ref[place, :] = slot_rows(d, slot, 2)

        ends = []
        end = jnp.int32(0)
        for i in range(docs):
            end = end + docs_ref[i]
            ends.append(end)
        row_place = lax.broadcasted_iota(jnp.int32, (block, 1), 0) + own_first
        row_place = jnp.where(row_place >= block, row_place - block, row_place)
        key_iota = lax.broadcasted_iota(jnp.int32, (1, window), 1)
        key_in_block = key_iota % block + own_first
        key_in_block = jnp.where(key_in_block >= block, key_in_block - block, key_in_block)
        key_place = (key_iota // block) * block + key_in_block
        for n, slot in enumerate(query_slots):
            for d in range(count):
                index = jnp.bitwise_xor(mu, d) * chips + jnp.bitwise_xor(chip, slot)
                first_row = index * block
                doc_first = jnp.int32(0)
                for e in ends:
                    doc_first = jnp.where(first_row >= e, e, doc_first)
                start = jnp.minimum(doc_first // block, (total - window) // block) * block
                start = pl.multiple_of(start, block)
                row_pos = row_place + first_row
                row_first = jnp.zeros((block, 1), jnp.int32)
                for e in ends:
                    row_first = jnp.where(row_pos >= e, e, row_first)
                key_pos = key_place + start
                allowed = (key_pos <= row_pos) & (key_pos >= row_first)
                scores = lax.dot_general(
                    slot_rows(d, slot, 0),
                    keys_ref[pl.ds(start, window), :],
                    (((1,), (1,)), ((), ())),
                    preferred_element_type=jnp.float32,
                )
                scores = jnp.where(allowed, scores * scale, -1e30)
                row_max = jnp.max(scores, axis=1, keepdims=True)
                weights = jnp.where(allowed, jnp.exp(scores - row_max), 0.0)
                totals = jnp.sum(weights, axis=1, keepdims=True)
                summed = jnp.dot(
                    weights.astype(jnp.bfloat16),
                    values_ref[pl.ds(start, window), :],
                    preferred_element_type=jnp.float32,
                )
                outs[d][n * block : (n + 1) * block, :] = (summed / totals).astype(jnp.bfloat16)

    n_queries = len(query_slots) * count
    return pl.pallas_call(
        kernel,
        out_shape=[pltpu.VMEM((len(query_slots) * block, HDIM), jnp.bfloat16)] * count,
        in_specs=[SMEM, SMEM] + [VMEM] * (len(sets) * count),
        out_specs=[VMEM] * count,
        scratch_shapes=[
            pltpu.VMEM((total, HDIM), jnp.bfloat16),
            pltpu.VMEM((total, HDIM), jnp.bfloat16),
        ],
        compiler_params=params(18),
        cost_estimate=pl.CostEstimate(
            flops=n_queries * block * window * HDIM * 8,
            bytes_accessed=3 * total * HDIM * 2,
            transcendentals=n_queries * block * window,
        ),
        name="attend_slots",
    )(ids, doc_lengths, *[piece for _, pieces in sets for piece in pieces])


def output_rows(ids, modality, pieces, weight, chips, slots, slot):
    count = len(pieces)
    block = pieces[0].shape[0] // len(slots)
    half = block // 2
    at = slots.index(slot) * block
    depth, width = weight.shape[1:]
    tile = min(1024, width)

    def kernel(ids_ref, modality_ref, *refs):
        ins = refs[:count]
        weight_ref, own_ref, partner_ref, heads_ref = refs[count:]
        mode = mode_of(ids_ref, modality_ref, chips, slot)
        for d in range(count):
            heads_ref[jnp.bitwise_xor(ids_ref[0], d)] = ins[d][at : at + block, :]
        rows = jnp.concatenate([heads_ref[h] for h in range(count)], axis=1)
        for first in range(0, width, tile):
            cols = slice(first, first + tile)
            result = jnp.dot(rows, weight_ref[mode, :, cols], preferred_element_type=jnp.float32)
            result = result.astype(jnp.bfloat16)
            own_ref[:, cols] = result[:half]
            partner_ref[:, cols] = result[half:]

    return pl.pallas_call(
        kernel,
        out_shape=[pltpu.VMEM((half, width), jnp.bfloat16)] * 2,
        in_specs=[SMEM, SMEM] + [VMEM] * (count + 1),
        out_specs=[VMEM] * 2,
        scratch_shapes=[pltpu.VMEM((count, block, HDIM), jnp.bfloat16)],
        compiler_params=params(8),
        cost_estimate=pl.CostEstimate(
            flops=2 * block * depth * width,
            bytes_accessed=depth * width * 2,
            transcendentals=0,
        ),
        name="output_rows",
    )(ids, modality, *pieces, weight)


def chip_pairs(pairs):
    return [(2 * a + core, 2 * b + core) for a, b in pairs for core in range(2)]


def line_body(tokens, norm_gain, qkv_weight, out_weight, modality, doc_lengths):
    seq_count = lax.axis_size("seq")
    mod_count = lax.axis_size("mod")
    chips = seq_count // 2
    mu = lax.axis_index("mod").astype(jnp.int32)
    seq = lax.axis_index("seq").astype(jnp.int32)
    ids = jnp.stack([mu, seq // 2, seq % 2])
    qkv_weight = pltpu.with_memory_space_constraint(qkv_weight, pltpu.HBM)
    out_weight = pltpu.with_memory_space_constraint(out_weight, pltpu.HBM)

    def along(value, pairs):
        return lax.ppermute(value, "seq", chip_pairs(pairs))

    def swap(value):
        return lax.ppermute(value, "seq", [(i, i ^ 1) for i in range(seq_count)])

    def exchange(pieces):
        moved = [pieces[0]]
        for d in range(1, mod_count):
            moved.append(lax.ppermute(pieces[d], "mod", [(i, i ^ d) for i in range(mod_count)]))
        return moved

    normed = norm_rows(ids, modality, tokens, norm_gain, chips)
    two = along(normed, [(i, i ^ 2) for i in range(chips)])
    one = along(normed, [(i, i ^ 1) for i in range(chips)])
    inner = along(normed, [(1, 2), (2, 1)])
    relayed = along(two, [(2, 3), (1, 0)])
    own_pair = (normed, swap(normed))
    two_pair = (two, swap(two))
    one_pair = (one, swap(one))
    inner_pair = (inner, swap(inner))
    relayed_pair = (relayed, swap(relayed))

    own = project_slots(ids, modality, [own_pair], qkv_weight, chips, (0,))
    own = exchange(own)
    late_weight, kept_weight = fetch_weights(ids, modality, qkv_weight, out_weight, chips, 3)
    mid = project_slots(ids, modality, [two_pair, one_pair], qkv_weight, chips, (2, 1))
    mid = exchange(mid)
    late = project_late(ids, inner_pair, relayed_pair, late_weight, 3 * HDIM, chips)
    late = exchange(late)
    sets = (((0,), own), ((2, 1), mid), ((3,), late))

    def add(*shares):
        total = shares[0].astype(jnp.float32)
        for share in shares[1:]:
            total = total + share.astype(jnp.float32)
        return total.astype(jnp.bfloat16)

    def finish(pieces, slots, slot):
        own_share, partner_share = output_rows(
            ids, modality, pieces, kept_weight, chips, slots, slot
        )
        return own_share, swap(partner_share)

    first = attend_slots(ids, doc_lengths, sets, (3,), chips)
    first = exchange(first)
    sum3 = add(*finish(first, (3,), 3))
    from_end = along(sum3, [(3, 2), (0, 1)])
    from_inner = along(sum3, [(1, 2), (2, 1)])
    rest = attend_slots(ids, doc_lengths, sets, (2, 1, 0), chips)
    rest = exchange(rest)
    sum2 = add(*finish(rest, (2, 1, 0), 2))
    from_two_end = along(sum2, [(3, 1), (0, 2)])
    from_two_inner = along(add(sum2, from_end), [(2, 0), (1, 3)])
    sum1 = add(*finish(rest, (2, 1, 0), 1))
    from_one = along(sum1, [(i, i ^ 1) for i in range(chips)])
    shares0 = finish(rest, (2, 1, 0), 0)
    return add(tokens, *shares0, from_inner, from_one, from_two_end, from_two_inner)


def solution(mesh):
    fits = mesh.shape["seq"] == 8 and mesh.shape["mod"] == 4

    def body(tokens, norm_gain, qkv_weight, out_weight, modality, doc_lengths):
        whole = tokens.shape[0] * 2 == BLOCK and qkv_weight.shape[2] == 12 * HDIM
        chosen = line_body if fits and whole else general_body
        return chosen(tokens, norm_gain, qkv_weight, out_weight, modality, doc_lengths)

    return jax.shard_map(
        body,
        mesh=mesh,
        in_specs=(
            P(("mod", "seq"), None),
            P(),
            P(None, None, "seq"),
            P(None, "seq", None),
            P(),
            P(),
        ),
        out_specs=P(("mod", "seq"), None),
        check_vma=False,
    )
```

```python
import math

import jax
import jax.numpy as jnp
from jax import lax
from jax.experimental import pallas as pl
from jax.experimental.pallas import tpu as pltpu
from jax.sharding import PartitionSpec as P


HDIM = 128
BLOCK = 128


def modes_of_rows(first_row, row_count, modality):
    block_ids = (first_row + jnp.arange(row_count, dtype=jnp.int32)) // BLOCK
    block_table = jnp.arange(modality.shape[0], dtype=jnp.int32)
    picked = jnp.where(block_ids[:, None] == block_table[None, :], modality[None, :], 0)
    return jnp.sum(picked, axis=1)


def documents(positions, doc_lengths):
    doc_ends = jnp.cumsum(doc_lengths)
    return jnp.sum((positions[:, None] >= doc_ends[None, :]).astype(jnp.int32), axis=1)


def general_body(tokens, norm_gain, qkv_weight, out_weight, modality, doc_lengths):
    row_count = tokens.shape[0]
    seq_count = lax.axis_size("seq")
    mod_count = lax.axis_size("mod")
    group_rows = row_count * seq_count
    mod_index = lax.axis_index("mod")
    own_first = (mod_index * seq_count + lax.axis_index("seq")) * row_count
    row_modes = modes_of_rows(own_first, row_count, modality)
    choose = (
        row_modes[:, None, None] == jnp.arange(norm_gain.shape[0], dtype=jnp.int32)[None, :, None]
    )
    gain_rows = jnp.sum(jnp.where(choose, norm_gain[None, :, :], 0.0), axis=1)
    values = tokens.astype(jnp.float32)
    mean_square = jnp.mean(values * values, axis=1, keepdims=True)
    normed = (values * lax.rsqrt(mean_square + 1e-05) * gain_rows).astype(jnp.bfloat16)
    gathered = lax.all_gather(normed, "seq", axis=0, tiled=True)
    group_first = mod_index * group_rows
    block_count = group_rows // BLOCK
    block_modes = lax.dynamic_slice_in_dim(modality, group_first // BLOCK, block_count)
    heads_here = qkv_weight.shape[2] // (3 * HDIM)

    def project(block_pair):
        row_block, block_mode = block_pair
        weight = lax.dynamic_index_in_dim(qkv_weight, block_mode, 0, keepdims=False)
        return jnp.dot(row_block, weight, preferred_element_type=jnp.float32).astype(jnp.bfloat16)

    projected = lax.map(
        project, (gathered.reshape(block_count, BLOCK, gathered.shape[1]), block_modes)
    )
    projected = projected.reshape(group_rows, heads_here, 3, HDIM)
    queries = projected[:, :, 0, :]
    keys_here = projected[:, :, 1, :]
    values_here = projected[:, :, 2, :]
    quarter = group_rows // mod_count
    local_rows = jnp.arange(group_rows, dtype=jnp.int32)
    query_pos = group_first + local_rows
    query_docs = documents(query_pos, doc_lengths)
    block_size = min(512, quarter)
    block_total = group_rows // block_size
    score_scale = 1.0 / math.sqrt(HDIM)
    query_blocks = queries.reshape(block_total, block_size, heads_here, HDIM)
    pos_blocks = query_pos.reshape(block_total, block_size)
    doc_blocks = query_docs.reshape(block_total, block_size)
    piece_keys = lax.all_gather(keys_here, "mod", axis=0, tiled=True)
    piece_values = lax.all_gather(values_here, "mod", axis=0, tiled=True)
    key_pos = jnp.arange(piece_keys.shape[0], dtype=jnp.int32)
    key_docs = documents(key_pos, doc_lengths)

    def one_block(block_state):
        query_block, block_pos, block_docs = block_state
        scores = (
            jnp.einsum("qhc,khc->hqk", query_block, piece_keys, preferred_element_type=jnp.float32)
            * score_scale
        )
        allowed = (
            (key_pos[None, :] <= block_pos[:, None]) & (key_docs[None, :] == block_docs[:, None])
        )[None, :, :]
        row_max = jnp.max(jnp.where(allowed, scores, -1e30), axis=2)
        weights = jnp.where(allowed, jnp.exp(scores - row_max[:, :, None]), 0.0)
        totals = jnp.sum(weights, axis=2)
        rows = jnp.einsum(
            "hqk,khc->qhc",
            weights.astype(jnp.bfloat16),
            piece_values,
            preferred_element_type=jnp.float32,
        )
        return (rows / jnp.transpose(totals)[:, :, None]).astype(jnp.bfloat16)

    attended = lax.map(one_block, (query_blocks, pos_blocks, doc_blocks))
    attended = attended.reshape(group_rows, heads_here * HDIM)

    def output(block_pair):
        row_block, block_mode = block_pair
        weight = lax.dynamic_index_in_dim(out_weight, block_mode, 0, keepdims=False)
        return jnp.dot(row_block, weight, preferred_element_type=jnp.float32)

    partial_value = lax.map(
        output, (attended.reshape(block_count, BLOCK, attended.shape[1]), block_modes)
    )
    head_sums = lax.psum_scatter(
        partial_value.reshape(group_rows, partial_value.shape[2]).astype(jnp.bfloat16),
        "seq",
        scatter_dimension=0,
        tiled=True,
    ).astype(jnp.float32)
    return (tokens.astype(jnp.float32) + head_sums).astype(jnp.bfloat16)


SMEM = pl.BlockSpec(memory_space=pltpu.SMEM)
VMEM = pl.BlockSpec(memory_space=pltpu.VMEM)
HBM = pl.BlockSpec(memory_space=pltpu.HBM)
PIECES = 4


def mode_of(info, slot):
    return info[3 + slot]


def params(mib):
    return pltpu.CompilerParams(vmem_limit_bytes=mib << 20)


def norm_rows(ids, modality, tokens, norm_gain, chips):
    rows, width = tokens.shape
    modes = norm_gain.shape[0]
    step = 16
    parts = 4
    part = rows // parts

    def kernel(ids_ref, modality_ref, tokens_ref, gain_ref, out_ref, info_ref, *scratch):
        rows_ref, gains_ref, table_ref, row_sems, sems = scratch
        table_copy = pltpu.make_async_copy(modality_ref, table_ref, sems.at[0])
        table_copy.start()
        gain_copy = pltpu.make_async_copy(gain_ref, gains_ref, sems.at[1])
        gain_copy.start()
        row_copies = [
            pltpu.make_async_copy(
                tokens_ref.at[pl.ds(i * part, part)],
                rows_ref.at[pl.ds(i * part, part)],
                row_sems.at[i],
            )
            for i in range(parts)
        ]
        for copy in row_copies:
            copy.start()
        table_copy.wait()
        for i in range(3):
            info_ref[i] = ids_ref[i]
        for slot in range(chips):
            at = ids_ref[0] * chips + jnp.bitwise_xor(ids_ref[1], slot)
            info_ref[3 + slot] = table_ref[at]
        mode = table_ref[ids_ref[0] * chips + ids_ref[1]]
        gain_copy.wait()
        gain = gains_ref[pl.ds(mode, 1), :]
        for i in range(parts):
            row_copies[i].wait()
            for first in range(i * part, (i + 1) * part, step):
                values = rows_ref[first : first + step, :].astype(jnp.float32)
                mean_square = jnp.sum(values * values, axis=1, keepdims=True) * (1.0 / width)
                scaled = values * lax.rsqrt(mean_square + 1e-05) * gain
                out_ref[first : first + step, :] = scaled.astype(jnp.bfloat16)

    return pl.pallas_call(
        kernel,
        out_shape=[
            pltpu.VMEM((rows, width), jnp.bfloat16),
            jax.ShapeDtypeStruct((3 + chips,), jnp.int32),
        ],
        in_specs=[SMEM, HBM, HBM, HBM],
        out_specs=[VMEM, SMEM],
        scratch_shapes=[
            pltpu.VMEM((rows, width), jnp.bfloat16),
            pltpu.VMEM((modes, width), jnp.float32),
            pltpu.SMEM(modality.shape, jnp.int32),
            pltpu.SemaphoreType.DMA((parts,)),
            pltpu.SemaphoreType.DMA((2,)),
        ],
        compiler_params=params(8),
        cost_estimate=pl.CostEstimate(flops=4_000_000, bytes_accessed=1 << 20, transcendentals=64),
        name="norm_rows",
    )(ids, modality, tokens, norm_gain)


def fetch_weights(info, qkv_weight, slot):
    _, width, cols = qkv_weight.shape
    pairs = 2
    pair_cols = cols // pairs
    piece = width // PIECES

    def kernel(info_ref, qkv_ref, late_ref, late_sems):
        mode = mode_of(info_ref, slot)
        copies = []
        for p in range(pairs):
            first = jnp.bitwise_xor(info_ref[0] // 2, p) * pair_cols
            for k in range(PIECES):
                copies.append(
                    pltpu.make_async_copy(
                        qkv_ref.at[
                            mode,
                            pl.ds(k * piece, piece),
                            pl.ds(pl.multiple_of(first, 128), pair_cols),
                        ],
                        late_ref.at[p, k],
                        late_sems.at[p, k],
                    )
                )
        for copy in copies:
            copy.start()
        for copy in copies:
            copy.wait()

    return pl.pallas_call(
        kernel,
        out_shape=pltpu.VMEM((pairs, PIECES, piece, pair_cols), jnp.bfloat16),
        in_specs=[SMEM, HBM],
        out_specs=VMEM,
        scratch_shapes=[pltpu.SemaphoreType.DMA((pairs, PIECES))],
        compiler_params=params(1),
        cost_estimate=pl.CostEstimate(
            flops=3_000_000_000, bytes_accessed=12 << 20, transcendentals=0
        ),
        name="fetch_weights",
    )(info, qkv_weight)


class Prefetch:
    def __init__(self, out_weight, slots):
        self.weight, self.slots = out_weight, slots
        self.shapes = [pltpu.VMEM(out_weight.shape[1:], jnp.bfloat16)] * len(slots)
        self.scratch = pltpu.SemaphoreType.DMA((len(slots),))

    def copies(self, info_ref, weight_ref, kept_refs, sems):
        return [
            pltpu.make_async_copy(weight_ref.at[mode_of(info_ref, slot)], kept_refs[i], sems.at[i])
            for i, slot in enumerate(self.slots)
        ]


def store_pair(info_ref, outs, rows, p, result):
    result = result.astype(jnp.bfloat16)
    cols = result.shape[1] // 2
    odd = info_ref[0] % 2 == 1
    for e in range(2):
        first, last = result[:, e * cols : (e + 1) * cols], result[:, (1 - e) * cols : (2 - e) * cols]
        outs[2 * p + e][rows, :] = jnp.where(odd, last, first)


def project_slots(info, parts, weight, slots):
    half, width = parts[0][0].shape
    block = 2 * half
    cols = 3 * HDIM
    heads = weight.shape[2] // cols
    pairs = 2
    pair_cols = weight.shape[2] // pairs
    piece = width // PIECES
    count = len(slots)

    def kernel(info_ref, *refs):
        ins = refs[: 2 * count]
        weight_ref = refs[2 * count]
        outs = refs[2 * count + 1 : 2 * count + 1 + heads]
        buffer_ref, sems = refs[2 * count + 1 + heads :]

        def copy_of(n, p, k):
            first = jnp.bitwise_xor(info_ref[0] // 2, p) * pair_cols
            return pltpu.make_async_copy(
                weight_ref.at[
                    mode_of(info_ref, slots[n]),
                    pl.ds(k * piece, piece),
                    pl.ds(pl.multiple_of(first, 128), pair_cols),
                ],
                buffer_ref.at[p, k],
                sems.at[p, k],
            )

        for p in range(pairs):
            for k in range(PIECES):
                copy_of(0, p, k).start()
        for n in range(count):
            for p in range(pairs):
                result = None
                for k in range(PIECES):
                    copy_of(n, p, k).wait()
                    rows = jnp.concatenate(
                        [ins[2 * n + i][:, k * piece : (k + 1) * piece] for i in range(2)], axis=0
                    )
                    part = jnp.dot(rows, buffer_ref[p, k], preferred_element_type=jnp.float32)
                    result = part if result is None else result + part
                    if n + 1 < count:
                        copy_of(n + 1, p, k).start()
                store_pair(info_ref, outs, pl.ds(n * block, block), p, result)

    return pl.pallas_call(
        kernel,
        out_shape=[pltpu.VMEM((count * block, cols), jnp.bfloat16)] * heads,
        in_specs=[SMEM] + [VMEM] * (2 * count) + [HBM],
        out_specs=[VMEM] * heads,
        scratch_shapes=[
            pltpu.VMEM((pairs, PIECES, piece, pair_cols), jnp.bfloat16),
            pltpu.SemaphoreType.DMA((pairs, PIECES)),
        ],
        compiler_params=params(16),
        cost_estimate=pl.CostEstimate(
            flops=2 * count * block * width * cols * heads,
            bytes_accessed=count * width * cols * heads * 2,
            transcendentals=0,
        ),
        name="project_slots",
    )(info, *[piece for pair in parts for piece in pair], weight)


def project_late(info, inner, relayed, weight, cols, chips, prefetch):
    half, width = inner[0].shape
    block = 2 * half
    pairs, pieces, piece, pair_cols = weight.shape
    heads = pairs * pair_cols // cols

    kept = len(prefetch.slots)

    def kernel(info_ref, inner_own, inner_partner, relayed_own, relayed_partner, weight_ref, *refs):
        next_ref, outs, kept_refs = refs[0], refs[1 : 1 + heads], refs[1 + heads : 1 + heads + kept]
        rows_ref, sems = refs[1 + heads + kept :]
        copies = prefetch.copies(info_ref, next_ref, kept_refs, sems)
        for copy in copies:
            copy.start()
        chip = info_ref[1]
        middle = (chip > 0) & (chip < chips - 1)

        @pl.when(middle)
        def _():
            rows_ref[:half, :] = inner_own[...]
            rows_ref[half:, :] = inner_partner[...]

        @pl.when(jnp.logical_not(middle))
        def _():
            rows_ref[:half, :] = relayed_own[...]
            rows_ref[half:, :] = relayed_partner[...]

        for p in range(pairs):
            result = None
            for k in range(pieces):
                part = jnp.dot(
                    rows_ref[:, k * piece : (k + 1) * piece],
                    weight_ref[p, k],
                    preferred_element_type=jnp.float32,
                )
                result = part if result is None else result + part
            store_pair(info_ref, outs, pl.ds(0, block), p, result)
        for copy in copies:
            copy.wait()

    return pl.pallas_call(
        kernel,
        out_shape=[pltpu.VMEM((block, cols), jnp.bfloat16)] * heads + prefetch.shapes,
        in_specs=[SMEM] + [VMEM] * 5 + [HBM],
        out_specs=[VMEM] * (heads + kept),
        scratch_shapes=[pltpu.VMEM((block, width), jnp.bfloat16), prefetch.scratch],
        compiler_params=params(8),
        cost_estimate=pl.CostEstimate(
            flops=2 * block * width * cols * heads,
            bytes_accessed=width * cols * heads * 2,
            transcendentals=0,
        ),
        name="project_late",
    )(info, *inner, *relayed, weight, prefetch.weight)


def attend_slots(info, doc_lengths, sets, query_slots, chips, prefetch):
    count = len(sets[0][1])
    block = sets[0][1][0].shape[0] // len(sets[0][0])
    total = count * chips * block
    window = min(total // 2 + block, total)
    scale = 1.0 / math.sqrt(HDIM)
    docs = doc_lengths.shape[0]

    kept = len(prefetch.slots)

    def kernel(info_ref, docs_ref, *refs):
        ins, refs = refs[: len(sets) * count], refs[len(sets) * count :]
        next_ref, outs, kept_refs = refs[0], refs[1 : 1 + count], refs[1 + count : 1 + count + kept]
        keys_ref, values_ref, sems = refs[1 + count + kept :]
        copies = prefetch.copies(info_ref, next_ref, kept_refs, sems)
        for copy in copies:
            copy.start()
        mu, chip, own_first = info_ref[0], info_ref[1], info_ref[2] * (block // 2)

        def slot_rows(d, slot, part):
            for i, (slots, _) in enumerate(sets):
                if slot in slots:
                    at = slots.index(slot) * block
                    return ins[i * count + d][at : at + block, part * HDIM : (part + 1) * HDIM]

        for d in range(count):
            for slot in range(chips):
                index = jnp.bitwise_xor(mu, d) * chips + jnp.bitwise_xor(chip, slot)
                place = pl.ds(pl.multiple_of(index * block, block), block)
                keys_ref[place, :] = slot_rows(d, slot, 1)
                values_ref[place, :] = slot_rows(d, slot, 2)

        ends = []
        end = jnp.int32(0)
        for i in range(docs):
            end = end + docs_ref[i]
            ends.append(end)
        row_place = lax.broadcasted_iota(jnp.int32, (block, 1), 0) + own_first
        row_place = jnp.where(row_place >= block, row_place - block, row_place)
        key_iota = lax.broadcasted_iota(jnp.int32, (1, window), 1)
        key_in_block = key_iota % block + own_first
        key_in_block = jnp.where(key_in_block >= block, key_in_block - block, key_in_block)
        key_place = (key_iota // block) * block + key_in_block
        for n, slot in enumerate(query_slots):
            for d in range(count):
                index = jnp.bitwise_xor(mu, d) * chips + jnp.bitwise_xor(chip, slot)
                first_row = index * block
                doc_first = jnp.int32(0)
                for e in ends:
                    doc_first = jnp.where(first_row >= e, e, doc_first)
                start = jnp.minimum(doc_first // block, (total - window) // block) * block
                start = pl.multiple_of(start, block)
                row_pos = row_place + first_row
                row_first = jnp.zeros((block, 1), jnp.int32)
                for e in ends:
                    row_first = jnp.where(row_pos >= e, e, row_first)
                key_pos = key_place + start
                allowed = (key_pos <= row_pos) & (key_pos >= row_first)
                scores = lax.dot_general(
                    slot_rows(d, slot, 0),
                    keys_ref[pl.ds(start, window), :],
                    (((1,), (1,)), ((), ())),
                    preferred_element_type=jnp.float32,
                )
                scores = jnp.where(allowed, scores * scale, -1e30)
                row_max = jnp.max(scores, axis=1, keepdims=True)
                weights = jnp.where(allowed, jnp.exp(scores - row_max), 0.0)
                totals = jnp.sum(weights, axis=1, keepdims=True)
                summed = jnp.dot(
                    weights.astype(jnp.bfloat16),
                    values_ref[pl.ds(start, window), :],
                    preferred_element_type=jnp.float32,
                )
                outs[d][n * block : (n + 1) * block, :] = (summed / totals).astype(jnp.bfloat16)
        for copy in copies:
            copy.wait()

    n_queries = len(query_slots) * count
    return pl.pallas_call(
        kernel,
        out_shape=[pltpu.VMEM((len(query_slots) * block, HDIM), jnp.bfloat16)] * count
        + prefetch.shapes,
        in_specs=[SMEM, SMEM] + [VMEM] * (len(sets) * count) + [HBM],
        out_specs=[VMEM] * (count + kept),
        scratch_shapes=[
            pltpu.VMEM((total, HDIM), jnp.bfloat16),
            pltpu.VMEM((total, HDIM), jnp.bfloat16),
            prefetch.scratch,
        ],
        compiler_params=params(18),
        cost_estimate=pl.CostEstimate(
            flops=n_queries * block * window * HDIM * 8,
            bytes_accessed=3 * total * HDIM * 2,
            transcendentals=n_queries * block * window,
        ),
        name="attend_slots",
    )(info, doc_lengths, *[piece for _, pieces in sets for piece in pieces], prefetch.weight)


def output_rows(info, pieces, weight, slots, slot):
    count = len(pieces)
    block = pieces[0].shape[0] // len(slots)
    half = block // 2
    at = slots.index(slot) * block
    depth, width = weight.shape
    tile = min(1024, width)

    def kernel(info_ref, *refs):
        ins = refs[:count]
        weight_ref, own_ref, partner_ref, heads_ref = refs[count:]
        for d in range(count):
            heads_ref[jnp.bitwise_xor(info_ref[0], d)] = ins[d][at : at + block, :]
        rows = jnp.concatenate([heads_ref[h] for h in range(count)], axis=1)
        for first in range(0, width, tile):
            cols = slice(first, first + tile)
            result = jnp.dot(rows, weight_ref[:, cols], preferred_element_type=jnp.float32)
            result = result.astype(jnp.bfloat16)
            own_ref[:, cols] = result[:half]
            partner_ref[:, cols] = result[half:]

    return pl.pallas_call(
        kernel,
        out_shape=[pltpu.VMEM((half, width), jnp.bfloat16)] * 2,
        in_specs=[SMEM] + [VMEM] * (count + 1),
        out_specs=[VMEM] * 2,
        scratch_shapes=[pltpu.VMEM((count, block, HDIM), jnp.bfloat16)],
        compiler_params=params(8),
        cost_estimate=pl.CostEstimate(
            flops=2 * block * depth * width,
            bytes_accessed=depth * width * 2,
            transcendentals=0,
        ),
        name="output_rows",
    )(info, *pieces, weight)


def chip_pairs(pairs):
    return [(2 * a + core, 2 * b + core) for a, b in pairs for core in range(2)]


def line_body(tokens, norm_gain, qkv_weight, out_weight, modality, doc_lengths):
    seq_count = lax.axis_size("seq")
    mod_count = lax.axis_size("mod")
    chips = seq_count // 2
    mu = lax.axis_index("mod").astype(jnp.int32)
    seq = lax.axis_index("seq").astype(jnp.int32)
    ids = jnp.stack([mu, seq // 2, seq % 2])
    qkv_weight = pltpu.with_memory_space_constraint(qkv_weight, pltpu.HBM)
    out_weight = pltpu.with_memory_space_constraint(out_weight, pltpu.HBM)

    def along(value, pairs):
        return lax.ppermute(value, "seq", chip_pairs(pairs))

    def swap(value):
        return lax.ppermute(value, "seq", [(i, i ^ 1) for i in range(seq_count)])

    def exchange(pieces):
        moved = [pieces[0]]
        for d in range(1, mod_count):
            moved.append(lax.ppermute(pieces[d], "mod", [(i, i ^ d) for i in range(mod_count)]))
        return moved

    def add(*shares):
        total = shares[0].astype(jnp.float32)
        for share in shares[1:]:
            total = total + share.astype(jnp.float32)
        return total.astype(jnp.bfloat16)

    in_hbm = [
        pltpu.with_memory_space_constraint(value, pltpu.HBM)
        for value in (modality, tokens, norm_gain)
    ]
    normed, info = norm_rows(ids, *in_hbm, chips)
    two = along(normed, [(i, i ^ 2) for i in range(chips)])
    one = along(normed, [(i, i ^ 1) for i in range(chips)])
    inner = along(normed, [(1, 2), (2, 1)])
    relayed = along(two, [(2, 3), (1, 0)])
    own_pair = (normed, swap(normed))
    two_pair = (two, swap(two))
    one_pair = (one, swap(one))
    inner_pair = (inner, swap(inner))
    relayed_pair = (relayed, swap(relayed))

    own = project_slots(info, [own_pair], qkv_weight, (0,))
    own = exchange(own)
    late_weight = fetch_weights(info, qkv_weight, 3)
    mid = project_slots(info, [two_pair, one_pair], qkv_weight, (2, 1))
    mid = exchange(mid)
    kept = {}
    *late, kept[3] = project_late(
        info,
        inner_pair,
        relayed_pair,
        late_weight,
        3 * HDIM,
        chips,
        Prefetch(out_weight, (3,)),
    )
    late = exchange(late)
    sets = (((0,), own), ((2, 1), mid), ((3,), late))

    def finish(pieces, slots, slot):
        own_share, partner_share = output_rows(info, pieces, kept[slot], slots, slot)
        return own_share, swap(partner_share)

    *first, kept[2], kept[1] = attend_slots(
        info, doc_lengths, sets, (3, 2), chips, Prefetch(out_weight, (2, 1))
    )
    first = exchange(first)
    sum3 = add(*finish(first, (3, 2), 3))
    from_end = along(sum3, [(3, 2), (0, 1)])
    from_inner = along(sum3, [(1, 2), (2, 1)])
    sum2 = add(*finish(first, (3, 2), 2))
    from_two_end = along(sum2, [(3, 1), (0, 2)])
    *rest, kept[0] = attend_slots(
        info, doc_lengths, sets, (1, 0), chips, Prefetch(out_weight, (0,))
    )
    rest = exchange(rest)
    both2 = add(lax.optimization_barrier(sum2), from_end)
    from_two_inner = along(both2, [(2, 0), (1, 3)])
    sum1 = add(*finish(rest, (1, 0), 1))
    from_one = along(sum1, [(i, i ^ 1) for i in range(chips)])
    shares0 = finish(rest, (1, 0), 0)
    return add(tokens, *shares0, from_inner, from_one, from_two_end, from_two_inner)


def solution(mesh):
    fits = mesh.shape["seq"] == 8 and mesh.shape["mod"] == 4

    def body(tokens, norm_gain, qkv_weight, out_weight, modality, doc_lengths):
        whole = tokens.shape[0] * 2 == BLOCK and qkv_weight.shape[2] == 12 * HDIM
        chosen = line_body if fits and whole else general_body
        return chosen(tokens, norm_gain, qkv_weight, out_weight, modality, doc_lengths)

    return jax.shard_map(
        body,
        mesh=mesh,
        in_specs=(
            P(("mod", "seq"), None),
            P(),
            P(None, None, "seq"),
            P(None, "seq", None),
            P(),
            P(),
        ),
        out_specs=P(("mod", "seq"), None),
        check_vma=False,
    )
```

```python
import math

import jax
import jax.numpy as jnp
from jax import lax
from jax.experimental import pallas as pl
from jax.experimental.pallas import tpu as pltpu
from jax.sharding import PartitionSpec as P


HDIM = 128
BLOCK = 128


def modes_of_rows(first_row, row_count, modality):
    block_ids = (first_row + jnp.arange(row_count, dtype=jnp.int32)) // BLOCK
    block_table = jnp.arange(modality.shape[0], dtype=jnp.int32)
    picked = jnp.where(block_ids[:, None] == block_table[None, :], modality[None, :], 0)
    return jnp.sum(picked, axis=1)


def documents(positions, doc_lengths):
    doc_ends = jnp.cumsum(doc_lengths)
    return jnp.sum((positions[:, None] >= doc_ends[None, :]).astype(jnp.int32), axis=1)


def general_body(tokens, norm_gain, qkv_weight, out_weight, modality, doc_lengths):
    row_count = tokens.shape[0]
    seq_count = lax.axis_size("seq")
    mod_count = lax.axis_size("mod")
    group_rows = row_count * seq_count
    mod_index = lax.axis_index("mod")
    own_first = (mod_index * seq_count + lax.axis_index("seq")) * row_count
    row_modes = modes_of_rows(own_first, row_count, modality)
    choose = (
        row_modes[:, None, None] == jnp.arange(norm_gain.shape[0], dtype=jnp.int32)[None, :, None]
    )
    gain_rows = jnp.sum(jnp.where(choose, norm_gain[None, :, :], 0.0), axis=1)
    values = tokens.astype(jnp.float32)
    mean_square = jnp.mean(values * values, axis=1, keepdims=True)
    normed = (values * lax.rsqrt(mean_square + 1e-05) * gain_rows).astype(jnp.bfloat16)
    gathered = lax.all_gather(normed, "seq", axis=0, tiled=True)
    group_first = mod_index * group_rows
    block_count = group_rows // BLOCK
    block_modes = lax.dynamic_slice_in_dim(modality, group_first // BLOCK, block_count)
    heads_here = qkv_weight.shape[2] // (3 * HDIM)

    def project(block_pair):
        row_block, block_mode = block_pair
        weight = lax.dynamic_index_in_dim(qkv_weight, block_mode, 0, keepdims=False)
        return jnp.dot(row_block, weight, preferred_element_type=jnp.float32).astype(jnp.bfloat16)

    projected = lax.map(
        project, (gathered.reshape(block_count, BLOCK, gathered.shape[1]), block_modes)
    )
    projected = projected.reshape(group_rows, heads_here, 3, HDIM)
    queries = projected[:, :, 0, :]
    keys_here = projected[:, :, 1, :]
    values_here = projected[:, :, 2, :]
    quarter = group_rows // mod_count
    local_rows = jnp.arange(group_rows, dtype=jnp.int32)
    query_pos = group_first + local_rows
    query_docs = documents(query_pos, doc_lengths)
    block_size = min(512, quarter)
    block_total = group_rows // block_size
    score_scale = 1.0 / math.sqrt(HDIM)
    query_blocks = queries.reshape(block_total, block_size, heads_here, HDIM)
    pos_blocks = query_pos.reshape(block_total, block_size)
    doc_blocks = query_docs.reshape(block_total, block_size)
    piece_keys = lax.all_gather(keys_here, "mod", axis=0, tiled=True)
    piece_values = lax.all_gather(values_here, "mod", axis=0, tiled=True)
    key_pos = jnp.arange(piece_keys.shape[0], dtype=jnp.int32)
    key_docs = documents(key_pos, doc_lengths)

    def one_block(block_state):
        query_block, block_pos, block_docs = block_state
        scores = (
            jnp.einsum("qhc,khc->hqk", query_block, piece_keys, preferred_element_type=jnp.float32)
            * score_scale
        )
        allowed = (
            (key_pos[None, :] <= block_pos[:, None]) & (key_docs[None, :] == block_docs[:, None])
        )[None, :, :]
        row_max = jnp.max(jnp.where(allowed, scores, -1e30), axis=2)
        weights = jnp.where(allowed, jnp.exp(scores - row_max[:, :, None]), 0.0)
        totals = jnp.sum(weights, axis=2)
        rows = jnp.einsum(
            "hqk,khc->qhc",
            weights.astype(jnp.bfloat16),
            piece_values,
            preferred_element_type=jnp.float32,
        )
        return (rows / jnp.transpose(totals)[:, :, None]).astype(jnp.bfloat16)

    attended = lax.map(one_block, (query_blocks, pos_blocks, doc_blocks))
    attended = attended.reshape(group_rows, heads_here * HDIM)

    def output(block_pair):
        row_block, block_mode = block_pair
        weight = lax.dynamic_index_in_dim(out_weight, block_mode, 0, keepdims=False)
        return jnp.dot(row_block, weight, preferred_element_type=jnp.float32)

    partial_value = lax.map(
        output, (attended.reshape(block_count, BLOCK, attended.shape[1]), block_modes)
    )
    head_sums = lax.psum_scatter(
        partial_value.reshape(group_rows, partial_value.shape[2]).astype(jnp.bfloat16),
        "seq",
        scatter_dimension=0,
        tiled=True,
    ).astype(jnp.float32)
    return (tokens.astype(jnp.float32) + head_sums).astype(jnp.bfloat16)


SMEM = pl.BlockSpec(memory_space=pltpu.SMEM)
VMEM = pl.BlockSpec(memory_space=pltpu.VMEM)
HBM = pl.BlockSpec(memory_space=pltpu.HBM)
PIECES = 4


def is_middle(info, chips):
    return (info[1] > 0) & (info[1] < chips - 1)


def mode_of(info, slot):
    return info[3 + slot]


def params(mib):
    return pltpu.CompilerParams(vmem_limit_bytes=mib << 20)


def norm_rows(ids, modality, tokens, norm_gain, chips):
    rows, width = tokens.shape
    modes = norm_gain.shape[0]
    step = 16
    parts = 4
    part = rows // parts

    def kernel(ids_ref, modality_ref, tokens_ref, gain_ref, out_ref, info_ref, *scratch):
        rows_ref, gains_ref, table_ref, row_sems, sems = scratch
        table_copy = pltpu.make_async_copy(modality_ref, table_ref, sems.at[0])
        table_copy.start()
        gain_copy = pltpu.make_async_copy(gain_ref, gains_ref, sems.at[1])
        gain_copy.start()
        row_copies = [
            pltpu.make_async_copy(
                tokens_ref.at[pl.ds(i * part, part)],
                rows_ref.at[pl.ds(i * part, part)],
                row_sems.at[i],
            )
            for i in range(parts)
        ]
        for copy in row_copies:
            copy.start()
        table_copy.wait()
        for i in range(3):
            info_ref[i] = ids_ref[i]
        for slot in range(chips):
            at = ids_ref[0] * chips + jnp.bitwise_xor(ids_ref[1], slot)
            info_ref[3 + slot] = table_ref[at]
        mode = table_ref[ids_ref[0] * chips + ids_ref[1]]
        gain_copy.wait()
        gain = gains_ref[pl.ds(mode, 1), :]
        for i in range(parts):
            row_copies[i].wait()
            for first in range(i * part, (i + 1) * part, step):
                values = rows_ref[first : first + step, :].astype(jnp.float32)
                mean_square = jnp.sum(values * values, axis=1, keepdims=True) * (1.0 / width)
                scaled = values * lax.rsqrt(mean_square + 1e-05) * gain
                out_ref[first : first + step, :] = scaled.astype(jnp.bfloat16)

    return pl.pallas_call(
        kernel,
        out_shape=[
            pltpu.VMEM((rows, width), jnp.bfloat16),
            jax.ShapeDtypeStruct((3 + chips,), jnp.int32),
        ],
        in_specs=[SMEM, HBM, HBM, HBM],
        out_specs=[VMEM, SMEM],
        scratch_shapes=[
            pltpu.VMEM((rows, width), jnp.bfloat16),
            pltpu.VMEM((modes, width), jnp.float32),
            pltpu.SMEM(modality.shape, jnp.int32),
            pltpu.SemaphoreType.DMA((parts,)),
            pltpu.SemaphoreType.DMA((2,)),
        ],
        compiler_params=params(8),
        cost_estimate=pl.CostEstimate(flops=4_000_000, bytes_accessed=1 << 20, transcendentals=64),
        name="norm_rows",
    )(ids, modality, tokens, norm_gain)


def weight_copies(info_ref, weight_ref, buffer_ref, sems, slot):
    pairs, pieces, piece, pair_cols = buffer_ref.shape
    copies = {}
    for p in range(pairs):
        first = jnp.bitwise_xor(info_ref[0] // 2, p) * pair_cols
        for k in range(pieces):
            copies[p, k] = pltpu.make_async_copy(
                weight_ref.at[
                    mode_of(info_ref, slot),
                    pl.ds(k * piece, piece),
                    pl.ds(pl.multiple_of(first, 128), pair_cols),
                ],
                buffer_ref.at[p, k],
                sems.at[p, k],
            )
    return copies


def weight_shape(weight):
    width, cols = weight.shape[1:]
    return (2, PIECES, width // PIECES, cols // 2)


def fetch_weights(info, qkv_weight, slots):
    shape = weight_shape(qkv_weight)
    count = len(slots)

    def kernel(info_ref, qkv_ref, *refs):
        sems = refs[count]
        copies = []
        for i, slot in enumerate(slots):
            copies += weight_copies(info_ref, qkv_ref, refs[i], sems.at[i], slot).values()
        for copy in copies:
            copy.start()
        for copy in copies:
            copy.wait()

    return pl.pallas_call(
        kernel,
        out_shape=[pltpu.VMEM(shape, jnp.bfloat16)] * count,
        in_specs=[SMEM, HBM],
        out_specs=[VMEM] * count,
        scratch_shapes=[pltpu.SemaphoreType.DMA((count, *shape[:2]))],
        compiler_params=params(1),
        cost_estimate=pl.CostEstimate(
            flops=6_000_000_000, bytes_accessed=25 << 20, transcendentals=0
        ),
        name="fetch_weights",
    )(info, qkv_weight)


class Prefetch:
    def __init__(self, out_weight, turns, chips):
        self.weight, self.turns, self.chips = out_weight, turns, chips
        self.shapes = [pltpu.VMEM(out_weight.shape[1:], jnp.bfloat16)] * len(turns)
        self.scratch = pltpu.SemaphoreType.DMA((len(turns),))

    def copies(self, info_ref, weight_ref, kept_refs, sems):
        middle = is_middle(info_ref, self.chips)
        return [
            pltpu.make_async_copy(
                weight_ref.at[mode_of(info_ref, jnp.where(middle, turn[1], turn[0]))],
                kept_refs[i],
                sems.at[i],
            )
            for i, turn in enumerate(self.turns)
        ]

    def start(self, *refs):
        @pl.when(refs[0][1] >= 0)
        def _():
            for copy in self.copies(*refs):
                copy.start()

    def wait(self, *refs):
        @pl.when(refs[0][1] >= 0)
        def _():
            for copy in self.copies(*refs):
                copy.wait()


def store_pair(info_ref, outs, rows, p, result):
    result = result.astype(jnp.bfloat16)
    cols = result.shape[1] // 2
    odd = info_ref[0] % 2 == 1
    for e in range(2):
        first, last = result[:, e * cols : (e + 1) * cols], result[:, (1 - e) * cols : (2 - e) * cols]
        outs[2 * p + e][rows, :] = jnp.where(odd, last, first)


def project_slots(info, parts, weight, slots, ready=()):
    half, width = parts[0][0].shape
    block = 2 * half
    cols = 3 * HDIM
    heads = weight.shape[2] // cols
    shape = weight_shape(weight)
    pairs, pieces, piece, _ = shape
    count, given = len(slots), len(ready)

    def kernel(info_ref, *refs):
        ins, refs = refs[: 2 * count], refs[2 * count :]
        ready_refs, weight_ref, refs = refs[:given], refs[given], refs[given + 1 :]
        outs, (buffer_ref, sems) = refs[:heads], refs[heads:]
        fetched = [
            weight_copies(info_ref, weight_ref, buffer_ref, sems, slot) for slot in slots[given:]
        ]
        for copy in fetched[0].values():
            copy.start()
        for n in range(count):
            source_ref = ready_refs[n] if n < given else buffer_ref
            for p in range(pairs):
                result = None
                for k in range(pieces):
                    if n >= given:
                        fetched[n - given][p, k].wait()
                    rows = jnp.concatenate(
                        [ins[2 * n + i][:, k * piece : (k + 1) * piece] for i in range(2)], axis=0
                    )
                    part = jnp.dot(rows, source_ref[p, k], preferred_element_type=jnp.float32)
                    result = part if result is None else result + part
                    if given <= n < count - 1:
                        fetched[n - given + 1][p, k].start()
                store_pair(info_ref, outs, pl.ds(n * block, block), p, result)

    return pl.pallas_call(
        kernel,
        out_shape=[pltpu.VMEM((count * block, cols), jnp.bfloat16)] * heads,
        in_specs=[SMEM] + [VMEM] * (2 * count + given) + [HBM],
        out_specs=[VMEM] * heads,
        scratch_shapes=[
            pltpu.VMEM(shape, jnp.bfloat16),
            pltpu.SemaphoreType.DMA(shape[:2]),
        ],
        compiler_params=params(16),
        cost_estimate=pl.CostEstimate(
            flops=2 * count * block * width * cols * heads,
            bytes_accessed=count * width * cols * heads * 2,
            transcendentals=0,
        ),
        name="project_slots",
    )(info, *[piece for pair in parts for piece in pair], *ready, weight)


def project_late(info, inner, relayed, weight, cols, chips, prefetch):
    half, width = inner[0].shape
    block = 2 * half
    pairs, pieces, piece, pair_cols = weight.shape
    heads = pairs * pair_cols // cols

    kept = len(prefetch.turns)

    def kernel(info_ref, inner_own, inner_partner, relayed_own, relayed_partner, weight_ref, *refs):
        next_ref, outs, kept_refs = refs[0], refs[1 : 1 + heads], refs[1 + heads : 1 + heads + kept]
        rows_ref, sems = refs[1 + heads + kept :]
        prefetch.start(info_ref, next_ref, kept_refs, sems)
        middle = is_middle(info_ref, chips)

        @pl.when(middle)
        def _():
            rows_ref[:half, :] = inner_own[...]
            rows_ref[half:, :] = inner_partner[...]

        @pl.when(jnp.logical_not(middle))
        def _():
            rows_ref[:half, :] = relayed_own[...]
            rows_ref[half:, :] = relayed_partner[...]

        for p in range(pairs):
            result = None
            for k in range(pieces):
                part = jnp.dot(
                    rows_ref[:, k * piece : (k + 1) * piece],
                    weight_ref[p, k],
                    preferred_element_type=jnp.float32,
                )
                result = part if result is None else result + part
            store_pair(info_ref, outs, pl.ds(0, block), p, result)
        prefetch.wait(info_ref, next_ref, kept_refs, sems)

    return pl.pallas_call(
        kernel,
        out_shape=[pltpu.VMEM((block, cols), jnp.bfloat16)] * heads + prefetch.shapes,
        in_specs=[SMEM] + [VMEM] * 5 + [HBM],
        out_specs=[VMEM] * (heads + kept),
        scratch_shapes=[pltpu.VMEM((block, width), jnp.bfloat16), prefetch.scratch],
        compiler_params=params(8),
        cost_estimate=pl.CostEstimate(
            flops=2 * block * width * cols * heads,
            bytes_accessed=width * cols * heads * 2,
            transcendentals=0,
        ),
        name="project_late",
    )(info, *inner, *relayed, weight, prefetch.weight)


def attend_slots(info, doc_lengths, sets, turns, chips, prefetch):
    count = len(sets[0][1])
    block = sets[0][1][0].shape[0] // len(sets[0][0])
    total = count * chips * block
    window = min(total // 2 + block, total)
    scale = 1.0 / math.sqrt(HDIM)
    docs = doc_lengths.shape[0]

    kept = len(prefetch.turns)

    def kernel(info_ref, docs_ref, *refs):
        ins, refs = refs[: len(sets) * count], refs[len(sets) * count :]
        next_ref, outs, kept_refs = refs[0], refs[1 : 1 + count], refs[1 + count : 1 + count + kept]
        keys_ref, values_ref, sems = refs[1 + count + kept :]
        prefetch.start(info_ref, next_ref, kept_refs, sems)
        middle = is_middle(info_ref, chips)
        mu, chip, own_first = info_ref[0], info_ref[1], info_ref[2] * (block // 2)

        def slot_rows(d, slot, part):
            for i, (slots, _) in enumerate(sets):
                if slot in slots:
                    at = slots.index(slot) * block
                    return ins[i * count + d][at : at + block, part * HDIM : (part + 1) * HDIM]

        for d in range(count):
            for slot in range(chips):
                index = jnp.bitwise_xor(mu, d) * chips + jnp.bitwise_xor(chip, slot)
                place = pl.ds(pl.multiple_of(index * block, block), block)
                keys_ref[place, :] = slot_rows(d, slot, 1)
                values_ref[place, :] = slot_rows(d, slot, 2)

        ends = []
        end = jnp.int32(0)
        for i in range(docs):
            end = end + docs_ref[i]
            ends.append(end)
        row_place = lax.broadcasted_iota(jnp.int32, (block, 1), 0) + own_first
        row_place = jnp.where(row_place >= block, row_place - block, row_place)
        key_iota = lax.broadcasted_iota(jnp.int32, (1, window), 1)
        key_in_block = key_iota % block + own_first
        key_in_block = jnp.where(key_in_block >= block, key_in_block - block, key_in_block)
        key_place = (key_iota // block) * block + key_in_block
        for n, turn in enumerate(turns):
            slot = jnp.where(middle, turn[1], turn[0])
            for d in range(count):
                index = jnp.bitwise_xor(mu, d) * chips + jnp.bitwise_xor(chip, slot)
                first_row = index * block
                doc_first = jnp.int32(0)
                for e in ends:
                    doc_first = jnp.where(first_row >= e, e, doc_first)
                start = jnp.minimum(doc_first // block, (total - window) // block) * block
                start = pl.multiple_of(start, block)
                row_pos = row_place + first_row
                row_first = jnp.zeros((block, 1), jnp.int32)
                for e in ends:
                    row_first = jnp.where(row_pos >= e, e, row_first)
                key_pos = key_place + start
                allowed = (key_pos <= row_pos) & (key_pos >= row_first)
                query = slot_rows(d, turn[0], 0)
                if turn[1] != turn[0]:
                    query = jnp.where(middle, slot_rows(d, turn[1], 0), query)
                scores = lax.dot_general(
                    query,
                    keys_ref[pl.ds(start, window), :],
                    (((1,), (1,)), ((), ())),
                    preferred_element_type=jnp.float32,
                )
                scores = jnp.where(allowed, scores * scale, -1e30)
                row_max = jnp.max(scores, axis=1, keepdims=True)
                weights = jnp.where(allowed, jnp.exp(scores - row_max), 0.0)
                totals = jnp.sum(weights, axis=1, keepdims=True)
                summed = jnp.dot(
                    weights.astype(jnp.bfloat16),
                    values_ref[pl.ds(start, window), :],
                    preferred_element_type=jnp.float32,
                )
                outs[d][n * block : (n + 1) * block, :] = (summed / totals).astype(jnp.bfloat16)
        prefetch.wait(info_ref, next_ref, kept_refs, sems)

    n_queries = len(turns) * count
    return pl.pallas_call(
        kernel,
        out_shape=[pltpu.VMEM((len(turns) * block, HDIM), jnp.bfloat16)] * count
        + prefetch.shapes,
        in_specs=[SMEM, SMEM] + [VMEM] * (len(sets) * count) + [HBM],
        out_specs=[VMEM] * (count + kept),
        scratch_shapes=[
            pltpu.VMEM((total, HDIM), jnp.bfloat16),
            pltpu.VMEM((total, HDIM), jnp.bfloat16),
            prefetch.scratch,
        ],
        compiler_params=params(18),
        cost_estimate=pl.CostEstimate(
            flops=n_queries * block * window * HDIM * 8,
            bytes_accessed=3 * total * HDIM * 2,
            transcendentals=n_queries * block * window,
        ),
        name="attend_slots",
    )(info, doc_lengths, *[piece for _, pieces in sets for piece in pieces], prefetch.weight)


def output_rows(info, pieces, weight, index, turns, slot=None):
    count = len(pieces)
    block = pieces[0].shape[0] // turns
    half = block // 2
    at = index * block
    depth, width = weight.shape[-2:]
    tile = min(1024, width)
    firsts = range(0, width, tile)

    def kernel(info_ref, *refs):
        ins = refs[:count]
        weight_ref, own_ref, partner_ref, heads_ref = refs[count : count + 4]
        copies = []
        if slot is not None:
            buffer_ref, sems = refs[count + 4 :]
            for i, first in enumerate(firsts):
                part = weight_ref.at[mode_of(info_ref, slot), :, pl.ds(first, tile)]
                copies.append(pltpu.make_async_copy(part, buffer_ref.at[i], sems.at[i]))
            for copy in copies:
                copy.start()
        for d in range(count):
            heads_ref[jnp.bitwise_xor(info_ref[0], d)] = ins[d][at : at + block, :]
        rows = jnp.concatenate([heads_ref[h] for h in range(count)], axis=1)
        for i, first in enumerate(firsts):
            cols = slice(first, first + tile)
            if slot is None:
                part = weight_ref[:, cols]
            else:
                copies[i].wait()
                part = buffer_ref[i]
            result = jnp.dot(rows, part, preferred_element_type=jnp.float32)
            result = result.astype(jnp.bfloat16)
            own_ref[:, cols] = result[:half]
            partner_ref[:, cols] = result[half:]

    streamed = []
    if slot is not None:
        streamed = [
            pltpu.VMEM((len(firsts), depth, tile), jnp.bfloat16),
            pltpu.SemaphoreType.DMA((len(firsts),)),
        ]
    return pl.pallas_call(
        kernel,
        out_shape=[pltpu.VMEM((half, width), jnp.bfloat16)] * 2,
        in_specs=[SMEM] + [VMEM] * count + [VMEM if slot is None else HBM],
        out_specs=[VMEM] * 2,
        scratch_shapes=[pltpu.VMEM((count, block, HDIM), jnp.bfloat16)] + streamed,
        compiler_params=params(8),
        cost_estimate=pl.CostEstimate(
            flops=2 * block * depth * width,
            bytes_accessed=depth * width * 2,
            transcendentals=0,
        ),
        name="output_rows",
    )(info, *pieces, weight)


def chip_pairs(pairs):
    return [(2 * a + core, 2 * b + core) for a, b in pairs for core in range(2)]


def line_body(tokens, norm_gain, qkv_weight, out_weight, modality, doc_lengths):
    seq_count = lax.axis_size("seq")
    mod_count = lax.axis_size("mod")
    chips = seq_count // 2
    mu = lax.axis_index("mod").astype(jnp.int32)
    seq = lax.axis_index("seq").astype(jnp.int32)
    ids = jnp.stack([mu, seq // 2, seq % 2])
    qkv_weight = pltpu.with_memory_space_constraint(qkv_weight, pltpu.HBM)
    out_weight = pltpu.with_memory_space_constraint(out_weight, pltpu.HBM)
    alone = lax.optimization_barrier

    def along(value, pairs):
        return lax.ppermute(value, "seq", chip_pairs(pairs))

    def swap(value):
        return lax.ppermute(value, "seq", [(i, i ^ 1) for i in range(seq_count)])

    def exchange(pieces):
        moved = [pieces[0]]
        for d in range(1, mod_count):
            moved.append(lax.ppermute(pieces[d], "mod", [(i, i ^ d) for i in range(mod_count)]))
        return moved

    def add(*shares):
        total = shares[0].astype(jnp.float32)
        for share in shares[1:]:
            total = total + share.astype(jnp.float32)
        return total.astype(jnp.bfloat16)

    in_hbm = [
        pltpu.with_memory_space_constraint(value, pltpu.HBM)
        for value in (modality, tokens, norm_gain)
    ]
    normed, info = norm_rows(ids, *in_hbm, chips)
    two = along(normed, [(i, i ^ 2) for i in range(chips)])
    one = along(normed, [(i, i ^ 1) for i in range(chips)])
    inner = along(normed, [(1, 2), (2, 1)])
    relayed = along(two, [(i, i ^ 1) for i in range(chips)])
    own_pair = (normed, swap(normed))
    two_pair = (two, swap(two))
    one_pair = (one, swap(one))
    inner_pair = (inner, swap(inner))
    relayed_pair = (relayed, swap(relayed))
    turn_a, turn_b, turn_c, turn_d = (3, 1), (2, 3), (1, 2), (0, 0)

    own = project_slots(info, [own_pair], qkv_weight, (0,))
    own = exchange(own)
    late_weight, two_weight = fetch_weights(info, qkv_weight, (3, 2))
    mid = project_slots(
        info, [two_pair, one_pair], qkv_weight, (2, 1), ready=(two_weight,)
    )
    mid = exchange(mid)
    *late, kept_a = project_late(
        info,
        inner_pair,
        relayed_pair,
        late_weight,
        3 * HDIM,
        chips,
        Prefetch(out_weight, (turn_a,), chips),
    )
    late = exchange(late)
    sets = (((0,), own), ((2, 1), mid), ((3,), late))

    def finish(pieces, kept, index, slot=None):
        own_share, partner_share = output_rows(info, pieces, kept, index, 2, slot)
        return own_share, swap(partner_share)

    *first, kept_b = attend_slots(
        info,
        doc_lengths,
        sets,
        (turn_a, turn_b),
        chips,
        Prefetch(out_weight, (turn_b,), chips),
    )
    first = exchange(first)
    sum_a = alone(add(*finish(first, kept_a, 0)))
    own_b, partner_b = finish(first, kept_b, 1)
    own_b, sum_a = alone((own_b, sum_a))
    from_one = along(sum_a, [(i, i ^ 1) for i in range(chips)])
    sum_b = alone(add(own_b, partner_b))
    from_inner = along(sum_b, [(1, 2), (2, 1)])
    *rest, kept_c = attend_slots(
        info,
        doc_lengths,
        sets,
        (turn_c, turn_d),
        chips,
        Prefetch(out_weight, (turn_c,), chips),
    )
    rest = exchange(rest)
    sum_c = alone(add(*finish(rest, kept_c, 0)))
    chip = seq // 2
    middle = (chip > 0) & (chip < chips - 1)
    relay_sum = jnp.where(middle, add(sum_c, from_one), sum_b)
    from_two = along(relay_sum, [(i, i ^ 2) for i in range(chips)])
    from_end = along(sum_c, [(i, i ^ 1) for i in range(chips)])
    shares_d = finish(rest, out_weight, 1, slot=0)
    near = jnp.where(middle, from_inner, from_one)
    far = jnp.where(middle, from_end, jnp.zeros_like(from_end))
    return add(tokens, *shares_d, near, from_two, far)


def solution(mesh):
    fits = mesh.shape["seq"] == 8 and mesh.shape["mod"] == 4

    def body(tokens, norm_gain, qkv_weight, out_weight, modality, doc_lengths):
        whole = tokens.shape[0] * 2 == BLOCK and qkv_weight.shape[2] == 12 * HDIM
        chosen = line_body if fits and whole else general_body
        return chosen(tokens, norm_gain, qkv_weight, out_weight, modality, doc_lengths)

    return jax.shard_map(
        body,
        mesh=mesh,
        in_specs=(
            P(("mod", "seq"), None),
            P(),
            P(None, None, "seq"),
            P(None, "seq", None),
            P(),
            P(),
        ),
        out_specs=P(("mod", "seq"), None),
        check_vma=False,
    )
```

```python
import math

import jax
import jax.numpy as jnp
from jax import lax
from jax.experimental import pallas as pl
from jax.experimental.pallas import tpu as pltpu
from jax.sharding import PartitionSpec as P


HDIM = 128
BLOCK = 128


def modes_of_rows(first_row, row_count, modality):
    block_ids = (first_row + jnp.arange(row_count, dtype=jnp.int32)) // BLOCK
    block_table = jnp.arange(modality.shape[0], dtype=jnp.int32)
    picked = jnp.where(block_ids[:, None] == block_table[None, :], modality[None, :], 0)
    return jnp.sum(picked, axis=1)


def documents(positions, doc_lengths):
    doc_ends = jnp.cumsum(doc_lengths)
    return jnp.sum((positions[:, None] >= doc_ends[None, :]).astype(jnp.int32), axis=1)


def general_body(tokens, norm_gain, qkv_weight, out_weight, modality, doc_lengths):
    row_count = tokens.shape[0]
    seq_count = lax.axis_size("seq")
    mod_count = lax.axis_size("mod")
    group_rows = row_count * seq_count
    mod_index = lax.axis_index("mod")
    own_first = (mod_index * seq_count + lax.axis_index("seq")) * row_count
    row_modes = modes_of_rows(own_first, row_count, modality)
    choose = (
        row_modes[:, None, None] == jnp.arange(norm_gain.shape[0], dtype=jnp.int32)[None, :, None]
    )
    gain_rows = jnp.sum(jnp.where(choose, norm_gain[None, :, :], 0.0), axis=1)
    values = tokens.astype(jnp.float32)
    mean_square = jnp.mean(values * values, axis=1, keepdims=True)
    normed = (values * lax.rsqrt(mean_square + 1e-05) * gain_rows).astype(jnp.bfloat16)
    gathered = lax.all_gather(normed, "seq", axis=0, tiled=True)
    group_first = mod_index * group_rows
    block_count = group_rows // BLOCK
    block_modes = lax.dynamic_slice_in_dim(modality, group_first // BLOCK, block_count)
    heads_here = qkv_weight.shape[2] // (3 * HDIM)

    def project(block_pair):
        row_block, block_mode = block_pair
        weight = lax.dynamic_index_in_dim(qkv_weight, block_mode, 0, keepdims=False)
        return jnp.dot(row_block, weight, preferred_element_type=jnp.float32).astype(jnp.bfloat16)

    projected = lax.map(
        project, (gathered.reshape(block_count, BLOCK, gathered.shape[1]), block_modes)
    )
    projected = projected.reshape(group_rows, heads_here, 3, HDIM)
    queries = projected[:, :, 0, :]
    keys_here = projected[:, :, 1, :]
    values_here = projected[:, :, 2, :]
    quarter = group_rows // mod_count
    local_rows = jnp.arange(group_rows, dtype=jnp.int32)
    query_pos = group_first + local_rows
    query_docs = documents(query_pos, doc_lengths)
    block_size = min(512, quarter)
    block_total = group_rows // block_size
    score_scale = 1.0 / math.sqrt(HDIM)
    query_blocks = queries.reshape(block_total, block_size, heads_here, HDIM)
    pos_blocks = query_pos.reshape(block_total, block_size)
    doc_blocks = query_docs.reshape(block_total, block_size)
    piece_keys = lax.all_gather(keys_here, "mod", axis=0, tiled=True)
    piece_values = lax.all_gather(values_here, "mod", axis=0, tiled=True)
    key_pos = jnp.arange(piece_keys.shape[0], dtype=jnp.int32)
    key_docs = documents(key_pos, doc_lengths)

    def one_block(block_state):
        query_block, block_pos, block_docs = block_state
        scores = (
            jnp.einsum("qhc,khc->hqk", query_block, piece_keys, preferred_element_type=jnp.float32)
            * score_scale
        )
        allowed = (
            (key_pos[None, :] <= block_pos[:, None]) & (key_docs[None, :] == block_docs[:, None])
        )[None, :, :]
        row_max = jnp.max(jnp.where(allowed, scores, -1e30), axis=2)
        weights = jnp.where(allowed, jnp.exp(scores - row_max[:, :, None]), 0.0)
        totals = jnp.sum(weights, axis=2)
        rows = jnp.einsum(
            "hqk,khc->qhc",
            weights.astype(jnp.bfloat16),
            piece_values,
            preferred_element_type=jnp.float32,
        )
        return (rows / jnp.transpose(totals)[:, :, None]).astype(jnp.bfloat16)

    attended = lax.map(one_block, (query_blocks, pos_blocks, doc_blocks))
    attended = attended.reshape(group_rows, heads_here * HDIM)

    def output(block_pair):
        row_block, block_mode = block_pair
        weight = lax.dynamic_index_in_dim(out_weight, block_mode, 0, keepdims=False)
        return jnp.dot(row_block, weight, preferred_element_type=jnp.float32)

    partial_value = lax.map(
        output, (attended.reshape(block_count, BLOCK, attended.shape[1]), block_modes)
    )
    head_sums = lax.psum_scatter(
        partial_value.reshape(group_rows, partial_value.shape[2]).astype(jnp.bfloat16),
        "seq",
        scatter_dimension=0,
        tiled=True,
    ).astype(jnp.float32)
    return (tokens.astype(jnp.float32) + head_sums).astype(jnp.bfloat16)


SMEM = pl.BlockSpec(memory_space=pltpu.SMEM)
VMEM = pl.BlockSpec(memory_space=pltpu.VMEM)
HBM = pl.BlockSpec(memory_space=pltpu.HBM)
PIECES = 4


def is_middle(info, chips):
    return (info[1] > 0) & (info[1] < chips - 1)


def mode_of(info, slot):
    return info[3 + slot]


def params(mib):
    return pltpu.CompilerParams(vmem_limit_bytes=mib << 20)


def norm_rows(ids, modality, tokens, norm_gain, chips):
    rows, width = tokens.shape
    modes = norm_gain.shape[0]
    step = 16
    parts = 4
    part = rows // parts

    def kernel(ids_ref, modality_ref, tokens_ref, gain_ref, out_ref, info_ref, *scratch):
        rows_ref, gains_ref, table_ref, row_sems, sems = scratch
        table_copy = pltpu.make_async_copy(modality_ref, table_ref, sems.at[0])
        table_copy.start()
        gain_copy = pltpu.make_async_copy(gain_ref, gains_ref, sems.at[1])
        gain_copy.start()
        row_copies = [
            pltpu.make_async_copy(
                tokens_ref.at[pl.ds(i * part, part)],
                rows_ref.at[pl.ds(i * part, part)],
                row_sems.at[i],
            )
            for i in range(parts)
        ]
        for copy in row_copies:
            copy.start()
        table_copy.wait()
        for i in range(3):
            info_ref[i] = ids_ref[i]
        for slot in range(chips):
            at = ids_ref[0] * chips + jnp.bitwise_xor(ids_ref[1], slot)
            info_ref[3 + slot] = table_ref[at]
        mode = table_ref[ids_ref[0] * chips + ids_ref[1]]
        gain_copy.wait()
        gain = gains_ref[pl.ds(mode, 1), :]
        for i in range(parts):
            row_copies[i].wait()
            for first in range(i * part, (i + 1) * part, step):
                values = rows_ref[first : first + step, :].astype(jnp.float32)
                mean_square = jnp.sum(values * values, axis=1, keepdims=True) * (1.0 / width)
                scaled = values * lax.rsqrt(mean_square + 1e-05) * gain
                out_ref[first : first + step, :] = scaled.astype(jnp.bfloat16)

    return pl.pallas_call(
        kernel,
        out_shape=[
            pltpu.VMEM((rows, width), jnp.bfloat16),
            jax.ShapeDtypeStruct((3 + chips,), jnp.int32),
        ],
        in_specs=[SMEM, HBM, HBM, HBM],
        out_specs=[VMEM, SMEM],
        scratch_shapes=[
            pltpu.VMEM((rows, width), jnp.bfloat16),
            pltpu.VMEM((modes, width), jnp.float32),
            pltpu.SMEM(modality.shape, jnp.int32),
            pltpu.SemaphoreType.DMA((parts,)),
            pltpu.SemaphoreType.DMA((2,)),
        ],
        compiler_params=params(8),
        cost_estimate=pl.CostEstimate(flops=4_000_000, bytes_accessed=1 << 20, transcendentals=64),
        name="norm_rows",
    )(ids, modality, tokens, norm_gain)


def weight_copies(info_ref, weight_ref, buffer_ref, sems, slot):
    pairs, pieces, piece, pair_cols = buffer_ref.shape
    copies = {}
    for p in range(pairs):
        first = jnp.bitwise_xor(info_ref[0] // 2, p) * pair_cols
        for k in range(pieces):
            copies[p, k] = pltpu.make_async_copy(
                weight_ref.at[
                    mode_of(info_ref, slot),
                    pl.ds(k * piece, piece),
                    pl.ds(pl.multiple_of(first, 128), pair_cols),
                ],
                buffer_ref.at[p, k],
                sems.at[p, k],
            )
    return copies


def weight_shape(weight):
    width, cols = weight.shape[1:]
    return (2, PIECES, width // PIECES, cols // 2)


def fetch_weights(info, qkv_weight, slots):
    shape = weight_shape(qkv_weight)
    count = len(slots)

    def kernel(info_ref, qkv_ref, *refs):
        sems = refs[count]
        copies = []
        for i, slot in enumerate(slots):
            copies += weight_copies(info_ref, qkv_ref, refs[i], sems.at[i], slot).values()
        for copy in copies:
            copy.start()
        for copy in copies:
            copy.wait()

    return pl.pallas_call(
        kernel,
        out_shape=[pltpu.VMEM(shape, jnp.bfloat16)] * count,
        in_specs=[SMEM, HBM],
        out_specs=[VMEM] * count,
        scratch_shapes=[pltpu.SemaphoreType.DMA((count, *shape[:2]))],
        compiler_params=params(1),
        cost_estimate=pl.CostEstimate(
            flops=6_000_000_000, bytes_accessed=25 << 20, transcendentals=0
        ),
        name="fetch_weights",
    )(info, qkv_weight)


class Prefetch:
    def __init__(self, out_weight, turns, chips):
        self.weight, self.turns, self.chips = out_weight, turns, chips
        self.shapes = [pltpu.VMEM(out_weight.shape[1:], jnp.bfloat16)] * len(turns)
        self.scratch = pltpu.SemaphoreType.DMA((len(turns),))

    def copies(self, info_ref, weight_ref, kept_refs, sems):
        middle = is_middle(info_ref, self.chips)
        return [
            pltpu.make_async_copy(
                weight_ref.at[mode_of(info_ref, jnp.where(middle, turn[1], turn[0]))],
                kept_refs[i],
                sems.at[i],
            )
            for i, turn in enumerate(self.turns)
        ]


    def start(self, *refs):
        for copy in self.copies(*refs):
            copy.start()

    def wait(self, *refs):
        for copy in self.copies(*refs):
            copy.wait()


def store_pair(info_ref, outs, rows, p, result):
    result = result.astype(jnp.bfloat16)
    cols = result.shape[1] // 2
    odd = info_ref[0] % 2 == 1
    for e in range(2):
        first, last = result[:, e * cols : (e + 1) * cols], result[:, (1 - e) * cols : (2 - e) * cols]
        outs[2 * p + e][rows, :] = jnp.where(odd, last, first)


def project_slots(info, parts, weight, slots, ready=()):
    half, width = parts[0][0].shape
    block = 2 * half
    cols = 3 * HDIM
    heads = weight.shape[2] // cols
    shape = weight_shape(weight)
    pairs, pieces, piece, _ = shape
    count, given = len(slots), len(ready)

    def kernel(info_ref, *refs):
        ins, refs = refs[: 2 * count], refs[2 * count :]
        ready_refs, weight_ref, refs = refs[:given], refs[given], refs[given + 1 :]
        outs, (buffer_ref, sems) = refs[:heads], refs[heads:]
        fetched = [
            weight_copies(info_ref, weight_ref, buffer_ref, sems, slot) for slot in slots[given:]
        ]
        for copy in fetched[0].values():
            copy.start()

        def project(n):
            source_ref = ready_refs[n] if n < given else buffer_ref
            for p in range(pairs):
                result = None
                for k in range(pieces):
                    if n >= given:
                        fetched[n - given][p, k].wait()
                    rows = jnp.concatenate(
                        [ins[2 * n + i][:, k * piece : (k + 1) * piece] for i in range(2)], axis=0
                    )
                    part = jnp.dot(rows, source_ref[p, k], preferred_element_type=jnp.float32)
                    result = part if result is None else result + part
                    if given <= n < count - 1:
                        fetched[n - given + 1][p, k].start()
                store_pair(info_ref, outs, pl.ds(n * block, block), p, result)

        for n in range(count):
            if n < given:
                pl.when(info_ref[1] >= 0)(lambda: project(n))
            else:
                project(n)

    return pl.pallas_call(
        kernel,
        out_shape=[pltpu.VMEM((count * block, cols), jnp.bfloat16)] * heads,
        in_specs=[SMEM] + [VMEM] * (2 * count + given) + [HBM],
        out_specs=[VMEM] * heads,
        scratch_shapes=[
            pltpu.VMEM(shape, jnp.bfloat16),
            pltpu.SemaphoreType.DMA(shape[:2]),
        ],
        compiler_params=params(16),
        cost_estimate=pl.CostEstimate(
            flops=2 * count * block * width * cols * heads,
            bytes_accessed=count * width * cols * heads * 2,
            transcendentals=0,
        ),
        name="project_slots",
    )(info, *[piece for pair in parts for piece in pair], *ready, weight)


def project_late(info, inner, relayed, weight, cols, chips, prefetch):
    half, width = inner[0].shape
    block = 2 * half
    pairs, pieces, piece, pair_cols = weight.shape
    heads = pairs * pair_cols // cols

    kept = len(prefetch.turns)

    def kernel(info_ref, inner_own, inner_partner, relayed_own, relayed_partner, weight_ref, *refs):
        next_ref, outs, kept_refs = refs[0], refs[1 : 1 + heads], refs[1 + heads : 1 + heads + kept]
        rows_ref, sems = refs[1 + heads + kept :]
        prefetch.start(info_ref, next_ref, kept_refs, sems)
        middle = is_middle(info_ref, chips)

        @pl.when(middle)
        def _():
            rows_ref[:half, :] = inner_own[...]
            rows_ref[half:, :] = inner_partner[...]

        @pl.when(jnp.logical_not(middle))
        def _():
            rows_ref[:half, :] = relayed_own[...]
            rows_ref[half:, :] = relayed_partner[...]

        for p in range(pairs):
            result = None
            for k in range(pieces):
                part = jnp.dot(
                    rows_ref[:, k * piece : (k + 1) * piece],
                    weight_ref[p, k],
                    preferred_element_type=jnp.float32,
                )
                result = part if result is None else result + part
            store_pair(info_ref, outs, pl.ds(0, block), p, result)
        prefetch.wait(info_ref, next_ref, kept_refs, sems)

    return pl.pallas_call(
        kernel,
        out_shape=[pltpu.VMEM((block, cols), jnp.bfloat16)] * heads + prefetch.shapes,
        in_specs=[SMEM] + [VMEM] * 5 + [HBM],
        out_specs=[VMEM] * (heads + kept),
        scratch_shapes=[pltpu.VMEM((block, width), jnp.bfloat16), prefetch.scratch],
        compiler_params=params(8),
        cost_estimate=pl.CostEstimate(
            flops=2 * block * width * cols * heads,
            bytes_accessed=width * cols * heads * 2,
            transcendentals=0,
        ),
        name="project_late",
    )(info, *inner, *relayed, weight, prefetch.weight)


def attend_slots(info, doc_lengths, sets, turns, chips, prefetch):
    count = len(sets[0][1])
    block = sets[0][1][0].shape[0] // len(sets[0][0])
    total = count * chips * block
    window = min(total // 2 + block, total)
    scale = 1.0 / math.sqrt(HDIM)
    docs = doc_lengths.shape[0]

    kept = len(prefetch.turns)

    def kernel(info_ref, docs_ref, *refs):
        ins, refs = refs[: len(sets) * count], refs[len(sets) * count :]
        next_ref, outs, kept_refs = refs[0], refs[1 : 1 + count], refs[1 + count : 1 + count + kept]
        keys_ref, values_ref, sems = refs[1 + count + kept :]
        prefetch.start(info_ref, next_ref, kept_refs, sems)

        @pl.when(info_ref[1] >= 0)
        def _():
            middle = is_middle(info_ref, chips)
            mu, chip, own_first = info_ref[0], info_ref[1], info_ref[2] * (block // 2)

            def slot_rows(d, slot, part):
                for i, (slots, _) in enumerate(sets):
                    if slot in slots:
                        at = slots.index(slot) * block
                        return ins[i * count + d][at : at + block, part * HDIM : (part + 1) * HDIM]

            for d in range(count):
                for slot in range(chips):
                    index = jnp.bitwise_xor(mu, d) * chips + jnp.bitwise_xor(chip, slot)
                    place = pl.ds(pl.multiple_of(index * block, block), block)
                    keys_ref[place, :] = slot_rows(d, slot, 1)
                    values_ref[place, :] = slot_rows(d, slot, 2)

            ends = []
            end = jnp.int32(0)
            for i in range(docs):
                end = end + docs_ref[i]
                ends.append(end)
            row_place = lax.broadcasted_iota(jnp.int32, (block, 1), 0) + own_first
            row_place = jnp.where(row_place >= block, row_place - block, row_place)
            key_iota = lax.broadcasted_iota(jnp.int32, (1, window), 1)
            key_in_block = key_iota % block + own_first
            key_in_block = jnp.where(key_in_block >= block, key_in_block - block, key_in_block)
            key_place = (key_iota // block) * block + key_in_block
            for n, turn in enumerate(turns):
                slot = jnp.where(middle, turn[1], turn[0])
                for d in range(count):
                    index = jnp.bitwise_xor(mu, d) * chips + jnp.bitwise_xor(chip, slot)
                    first_row = index * block
                    doc_first = jnp.int32(0)
                    for e in ends:
                        doc_first = jnp.where(first_row >= e, e, doc_first)
                    start = jnp.minimum(doc_first // block, (total - window) // block) * block
                    start = pl.multiple_of(start, block)
                    row_pos = row_place + first_row
                    row_first = jnp.zeros((block, 1), jnp.int32)
                    for e in ends:
                        row_first = jnp.where(row_pos >= e, e, row_first)
                    key_pos = key_place + start
                    allowed = (key_pos <= row_pos) & (key_pos >= row_first)
                    query = slot_rows(d, turn[0], 0)
                    if turn[1] != turn[0]:
                        query = jnp.where(middle, slot_rows(d, turn[1], 0), query)
                    scores = lax.dot_general(
                        query,
                        keys_ref[pl.ds(start, window), :],
                        (((1,), (1,)), ((), ())),
                        preferred_element_type=jnp.float32,
                    )
                    scores = jnp.where(allowed, scores * scale, -1e30)
                    row_max = jnp.max(scores, axis=1, keepdims=True)
                    weights = jnp.where(allowed, jnp.exp(scores - row_max), 0.0)
                    totals = jnp.sum(weights, axis=1, keepdims=True)
                    summed = jnp.dot(
                        weights.astype(jnp.bfloat16),
                        values_ref[pl.ds(start, window), :],
                        preferred_element_type=jnp.float32,
                    )
                    outs[d][n * block : (n + 1) * block, :] = (summed / totals).astype(jnp.bfloat16)

        prefetch.wait(info_ref, next_ref, kept_refs, sems)

    n_queries = len(turns) * count
    return pl.pallas_call(
        kernel,
        out_shape=[pltpu.VMEM((len(turns) * block, HDIM), jnp.bfloat16)] * count
        + prefetch.shapes,
        in_specs=[SMEM, SMEM] + [VMEM] * (len(sets) * count) + [HBM],
        out_specs=[VMEM] * (count + kept),
        scratch_shapes=[
            pltpu.VMEM((total, HDIM), jnp.bfloat16),
            pltpu.VMEM((total, HDIM), jnp.bfloat16),
            prefetch.scratch,
        ],
        compiler_params=params(14),
        cost_estimate=pl.CostEstimate(
            flops=n_queries * block * window * HDIM * 8,
            bytes_accessed=3 * total * HDIM * 2,
            transcendentals=n_queries * block * window,
        ),
        name="attend_slots",
    )(info, doc_lengths, *[piece for _, pieces in sets for piece in pieces], prefetch.weight)


def output_rows(info, pieces, weight, index, turns):
    count = len(pieces)
    block = pieces[0].shape[0] // turns
    half = block // 2
    at = index * block
    depth, width = weight.shape
    tile = min(1024, width)

    def kernel(info_ref, *refs):
        ins = refs[:count]
        weight_ref, own_ref, partner_ref, heads_ref = refs[count:]
        for d in range(count):
            heads_ref[jnp.bitwise_xor(info_ref[0], d)] = ins[d][at : at + block, :]
        rows = jnp.concatenate([heads_ref[h] for h in range(count)], axis=1)
        for first in range(0, width, tile):
            cols = slice(first, first + tile)
            result = jnp.dot(rows, weight_ref[:, cols], preferred_element_type=jnp.float32)
            result = result.astype(jnp.bfloat16)
            own_ref[:, cols] = result[:half]
            partner_ref[:, cols] = result[half:]

    return pl.pallas_call(
        kernel,
        out_shape=[pltpu.VMEM((half, width), jnp.bfloat16)] * 2,
        in_specs=[SMEM] + [VMEM] * (count + 1),
        out_specs=[VMEM] * 2,
        scratch_shapes=[pltpu.VMEM((count, block, HDIM), jnp.bfloat16)],
        compiler_params=params(8),
        cost_estimate=pl.CostEstimate(
            flops=2 * block * depth * width,
            bytes_accessed=depth * width * 2,
            transcendentals=0,
        ),
        name="output_rows",
    )(info, *pieces, weight)


def add_rows(info, chips, first, second, otherwise=None):
    values = [first, second] + ([] if otherwise is None else [otherwise])
    values = [pltpu.with_memory_space_constraint(value, pltpu.VMEM) for value in values]

    def kernel(info_ref, first_ref, second_ref, *refs):
        def add():
            total = first_ref[...].astype(jnp.float32) + second_ref[...].astype(jnp.float32)
            refs[-1][...] = total.astype(jnp.bfloat16)

        if otherwise is None:
            add()
            return
        middle = is_middle(info_ref, chips)
        pl.when(middle)(lambda: add())

        @pl.when(jnp.logical_not(middle))
        def _():
            refs[-1][...] = refs[0][...]

    return pl.pallas_call(
        kernel,
        out_shape=pltpu.VMEM(first.shape, jnp.bfloat16),
        in_specs=[SMEM] + [VMEM] * len(values),
        out_specs=VMEM,
        compiler_params=params(4),
        cost_estimate=pl.CostEstimate(
            flops=4 * first.size, bytes_accessed=6 * first.size, transcendentals=0
        ),
        name="add_rows",
    )(info, *values)


def last_rows(info, chips, early, far, middle_only):
    values = [
        pltpu.with_memory_space_constraint(value, pltpu.VMEM)
        for value in (early, far, middle_only)
    ]

    def kernel(info_ref, early_ref, far_ref, middle_ref, out_ref):
        middle = is_middle(info_ref, chips)

        @pl.when(middle)
        def _():
            total = early_ref[...] + far_ref[...].astype(jnp.float32)
            out_ref[...] = (total + middle_ref[...].astype(jnp.float32)).astype(jnp.bfloat16)

        @pl.when(jnp.logical_not(middle))
        def _():
            total = early_ref[...] + far_ref[...].astype(jnp.float32)
            out_ref[...] = total.astype(jnp.bfloat16)

    return pl.pallas_call(
        kernel,
        out_shape=jax.ShapeDtypeStruct(far.shape, jnp.bfloat16),
        in_specs=[SMEM, VMEM, VMEM, VMEM],
        out_specs=VMEM,
        compiler_params=params(6),
        cost_estimate=pl.CostEstimate(
            flops=4 * far.size, bytes_accessed=10 * far.size, transcendentals=0
        ),
        name="last_rows",
    )(info, *values)


def chip_pairs(pairs):
    return [(2 * a + core, 2 * b + core) for a, b in pairs for core in range(2)]


def line_body(tokens, norm_gain, qkv_weight, out_weight, modality, doc_lengths):
    seq_count = lax.axis_size("seq")
    mod_count = lax.axis_size("mod")
    chips = seq_count // 2
    mu = lax.axis_index("mod").astype(jnp.int32)
    seq = lax.axis_index("seq").astype(jnp.int32)
    ids = jnp.stack([mu, seq // 2, seq % 2])
    qkv_weight = pltpu.with_memory_space_constraint(qkv_weight, pltpu.HBM)
    out_weight = pltpu.with_memory_space_constraint(out_weight, pltpu.HBM)

    def along(value, pairs):
        return lax.ppermute(value, "seq", chip_pairs(pairs))

    def swap(value):
        return lax.ppermute(value, "seq", [(i, i ^ 1) for i in range(seq_count)])

    def exchange(pieces):
        moved = [pieces[0]]
        for d in range(1, mod_count):
            moved.append(lax.ppermute(pieces[d], "mod", [(i, i ^ d) for i in range(mod_count)]))
        return moved

    in_hbm = [
        pltpu.with_memory_space_constraint(value, pltpu.HBM)
        for value in (modality, tokens, norm_gain)
    ]
    normed, info = norm_rows(ids, *in_hbm, chips)
    two = along(normed, [(i, i ^ 2) for i in range(chips)])
    one = along(normed, [(i, i ^ 1) for i in range(chips)])
    inner = along(normed, [(1, 2), (2, 1)])
    relayed = along(two, [(i, i ^ 1) for i in range(chips)])
    own_pair = (normed, swap(normed))
    two_pair = (two, swap(two))
    one_pair = (one, swap(one))
    inner_pair = (inner, swap(inner))
    relayed_pair = (relayed, swap(relayed))
    turn_a, turn_b, turn_c, turn_d = (3, 1), (2, 3), (1, 2), (0, 0)

    own = project_slots(info, [own_pair], qkv_weight, (0,))
    own = exchange(own)
    late_weight, two_weight = fetch_weights(info, qkv_weight, (3, 2))
    mid = project_slots(
        info, [two_pair, one_pair], qkv_weight, (2, 1), ready=(two_weight,)
    )
    mid = exchange(mid)
    *late, kept_a = project_late(
        info,
        inner_pair,
        relayed_pair,
        late_weight,
        3 * HDIM,
        chips,
        Prefetch(out_weight, (turn_a,), chips),
    )
    late = exchange(late)
    sets = (((0,), own), ((2, 1), mid), ((3,), late))

    def finish(pieces, kept, index, turns):
        own_share, partner_share = output_rows(info, pieces, kept, index, turns)
        return own_share, swap(partner_share)

    *first, kept_b = attend_slots(
        info,
        doc_lengths,
        sets,
        (turn_a, turn_b),
        chips,
        Prefetch(out_weight, (turn_b,), chips),
    )
    first = exchange(first)
    sum_a = add_rows(info, chips, *finish(first, kept_a, 0, 2))
    own_b, partner_b = finish(first, kept_b, 1, 2)
    from_one = along(sum_a, [(i, i ^ 1) for i in range(chips)])
    sum_b = add_rows(info, chips, own_b, partner_b)
    from_inner = along(sum_b, [(1, 2), (2, 1)])
    *rest_c, kept_c = attend_slots(
        info, doc_lengths, sets, (turn_c,), chips, Prefetch(out_weight, (turn_c,), chips)
    )
    rest_c = exchange(rest_c)
    sum_c = add_rows(info, chips, *finish(rest_c, kept_c, 0, 1))
    chip = seq // 2
    middle = (chip > 0) & (chip < chips - 1)
    relay_sum = add_rows(info, chips, sum_c, from_one, sum_b)
    from_two = along(relay_sum, [(i, i ^ 2) for i in range(chips)])
    from_end = along(sum_c, [(i, i ^ 1) for i in range(chips)])
    *rest_d, kept_d = attend_slots(
        info, doc_lengths, sets, (turn_d,), chips, Prefetch(out_weight, (turn_d,), chips)
    )
    rest_d = exchange(rest_d)
    shares_d = finish(rest_d, kept_d, 0, 1)
    near = jnp.where(middle, from_inner, from_one)
    early = tokens.astype(jnp.float32)
    for share in (*shares_d, near):
        early = early + share.astype(jnp.float32)
    return last_rows(info, chips, early, from_two, from_end)


def solution(mesh):
    fits = mesh.shape["seq"] == 8 and mesh.shape["mod"] == 4

    def body(tokens, norm_gain, qkv_weight, out_weight, modality, doc_lengths):
        whole = tokens.shape[0] * 2 == BLOCK and qkv_weight.shape[2] == 12 * HDIM
        chosen = line_body if fits and whole else general_body
        return chosen(tokens, norm_gain, qkv_weight, out_weight, modality, doc_lengths)

    return jax.shard_map(
        body,
        mesh=mesh,
        in_specs=(
            P(("mod", "seq"), None),
            P(),
            P(None, None, "seq"),
            P(None, "seq", None),
            P(),
            P(),
        ),
        out_specs=P(("mod", "seq"), None),
        check_vma=False,
    )
```

```python
import math

import jax
import jax.numpy as jnp
from jax import lax
from jax.experimental import pallas as pl
from jax.experimental.pallas import tpu as pltpu
from jax.sharding import PartitionSpec as P


HDIM = 128
BLOCK = 128


def modes_of_rows(first_row, row_count, modality):
    block_ids = (first_row + jnp.arange(row_count, dtype=jnp.int32)) // BLOCK
    block_table = jnp.arange(modality.shape[0], dtype=jnp.int32)
    picked = jnp.where(block_ids[:, None] == block_table[None, :], modality[None, :], 0)
    return jnp.sum(picked, axis=1)


def documents(positions, doc_lengths):
    doc_ends = jnp.cumsum(doc_lengths)
    return jnp.sum((positions[:, None] >= doc_ends[None, :]).astype(jnp.int32), axis=1)


def general_body(tokens, norm_gain, qkv_weight, out_weight, modality, doc_lengths):
    row_count = tokens.shape[0]
    seq_count = lax.axis_size("seq")
    mod_count = lax.axis_size("mod")
    group_rows = row_count * seq_count
    mod_index = lax.axis_index("mod")
    own_first = (mod_index * seq_count + lax.axis_index("seq")) * row_count
    row_modes = modes_of_rows(own_first, row_count, modality)
    choose = (
        row_modes[:, None, None] == jnp.arange(norm_gain.shape[0], dtype=jnp.int32)[None, :, None]
    )
    gain_rows = jnp.sum(jnp.where(choose, norm_gain[None, :, :], 0.0), axis=1)
    values = tokens.astype(jnp.float32)
    mean_square = jnp.mean(values * values, axis=1, keepdims=True)
    normed = (values * lax.rsqrt(mean_square + 1e-05) * gain_rows).astype(jnp.bfloat16)
    gathered = lax.all_gather(normed, "seq", axis=0, tiled=True)
    group_first = mod_index * group_rows
    block_count = group_rows // BLOCK
    block_modes = lax.dynamic_slice_in_dim(modality, group_first // BLOCK, block_count)
    heads_here = qkv_weight.shape[2] // (3 * HDIM)

    def project(block_pair):
        row_block, block_mode = block_pair
        weight = lax.dynamic_index_in_dim(qkv_weight, block_mode, 0, keepdims=False)
        return jnp.dot(row_block, weight, preferred_element_type=jnp.float32).astype(jnp.bfloat16)

    projected = lax.map(
        project, (gathered.reshape(block_count, BLOCK, gathered.shape[1]), block_modes)
    )
    projected = projected.reshape(group_rows, heads_here, 3, HDIM)
    queries = projected[:, :, 0, :]
    keys_here = projected[:, :, 1, :]
    values_here = projected[:, :, 2, :]
    quarter = group_rows // mod_count
    local_rows = jnp.arange(group_rows, dtype=jnp.int32)
    query_pos = group_first + local_rows
    query_docs = documents(query_pos, doc_lengths)
    block_size = min(512, quarter)
    block_total = group_rows // block_size
    score_scale = 1.0 / math.sqrt(HDIM)
    query_blocks = queries.reshape(block_total, block_size, heads_here, HDIM)
    pos_blocks = query_pos.reshape(block_total, block_size)
    doc_blocks = query_docs.reshape(block_total, block_size)
    piece_keys = lax.all_gather(keys_here, "mod", axis=0, tiled=True)
    piece_values = lax.all_gather(values_here, "mod", axis=0, tiled=True)
    key_pos = jnp.arange(piece_keys.shape[0], dtype=jnp.int32)
    key_docs = documents(key_pos, doc_lengths)

    def one_block(block_state):
        query_block, block_pos, block_docs = block_state
        scores = (
            jnp.einsum("qhc,khc->hqk", query_block, piece_keys, preferred_element_type=jnp.float32)
            * score_scale
        )
        allowed = (
            (key_pos[None, :] <= block_pos[:, None]) & (key_docs[None, :] == block_docs[:, None])
        )[None, :, :]
        row_max = jnp.max(jnp.where(allowed, scores, -1e30), axis=2)
        weights = jnp.where(allowed, jnp.exp(scores - row_max[:, :, None]), 0.0)
        totals = jnp.sum(weights, axis=2)
        rows = jnp.einsum(
            "hqk,khc->qhc",
            weights.astype(jnp.bfloat16),
            piece_values,
            preferred_element_type=jnp.float32,
        )
        return (rows / jnp.transpose(totals)[:, :, None]).astype(jnp.bfloat16)

    attended = lax.map(one_block, (query_blocks, pos_blocks, doc_blocks))
    attended = attended.reshape(group_rows, heads_here * HDIM)

    def output(block_pair):
        row_block, block_mode = block_pair
        weight = lax.dynamic_index_in_dim(out_weight, block_mode, 0, keepdims=False)
        return jnp.dot(row_block, weight, preferred_element_type=jnp.float32)

    partial_value = lax.map(
        output, (attended.reshape(block_count, BLOCK, attended.shape[1]), block_modes)
    )
    head_sums = lax.psum_scatter(
        partial_value.reshape(group_rows, partial_value.shape[2]).astype(jnp.bfloat16),
        "seq",
        scatter_dimension=0,
        tiled=True,
    ).astype(jnp.float32)
    return (tokens.astype(jnp.float32) + head_sums).astype(jnp.bfloat16)


SMEM = pl.BlockSpec(memory_space=pltpu.SMEM)
VMEM = pl.BlockSpec(memory_space=pltpu.VMEM)
HBM = pl.BlockSpec(memory_space=pltpu.HBM)
PIECES = 4


def is_middle(info, chips):
    return (info[1] > 0) & (info[1] < chips - 1)


def mode_of(info, slot):
    return info[3 + slot]


def params(mib):
    return pltpu.CompilerParams(vmem_limit_bytes=mib << 20)


def norm_rows(ids, modality, tokens, norm_gain, chips):
    rows, width = tokens.shape
    modes = norm_gain.shape[0]
    step = 16
    parts = 4
    part = rows // parts

    def kernel(ids_ref, modality_ref, tokens_ref, gain_ref, out_ref, info_ref, *scratch):
        rows_ref, gains_ref, table_ref, row_sems, sems = scratch
        table_copy = pltpu.make_async_copy(modality_ref, table_ref, sems.at[0])
        table_copy.start()
        gain_copy = pltpu.make_async_copy(gain_ref, gains_ref, sems.at[1])
        gain_copy.start()
        row_copies = [
            pltpu.make_async_copy(
                tokens_ref.at[pl.ds(i * part, part)],
                rows_ref.at[pl.ds(i * part, part)],
                row_sems.at[i],
            )
            for i in range(parts)
        ]
        for copy in row_copies:
            copy.start()
        table_copy.wait()
        for i in range(3):
            info_ref[i] = ids_ref[i]
        for slot in range(chips):
            at = ids_ref[0] * chips + jnp.bitwise_xor(ids_ref[1], slot)
            info_ref[3 + slot] = table_ref[at]
        mode = table_ref[ids_ref[0] * chips + ids_ref[1]]
        gain_copy.wait()
        gain = gains_ref[pl.ds(mode, 1), :]
        for i in range(parts):
            row_copies[i].wait()
            for first in range(i * part, (i + 1) * part, step):
                values = rows_ref[first : first + step, :].astype(jnp.float32)
                mean_square = jnp.sum(values * values, axis=1, keepdims=True) * (1.0 / width)
                scaled = values * lax.rsqrt(mean_square + 1e-05) * gain
                out_ref[first : first + step, :] = scaled.astype(jnp.bfloat16)

    return pl.pallas_call(
        kernel,
        out_shape=[
            pltpu.VMEM((rows, width), jnp.bfloat16),
            jax.ShapeDtypeStruct((3 + chips,), jnp.int32),
        ],
        in_specs=[SMEM, HBM, HBM, HBM],
        out_specs=[VMEM, SMEM],
        scratch_shapes=[
            pltpu.VMEM((rows, width), jnp.bfloat16),
            pltpu.VMEM((modes, width), jnp.float32),
            pltpu.SMEM(modality.shape, jnp.int32),
            pltpu.SemaphoreType.DMA((parts,)),
            pltpu.SemaphoreType.DMA((2,)),
        ],
        compiler_params=params(8),
        cost_estimate=pl.CostEstimate(flops=4_000_000, bytes_accessed=1 << 20, transcendentals=64),
        name="norm_rows",
    )(ids, modality, tokens, norm_gain)


def weight_copies(info_ref, weight_ref, buffer_ref, sems, slot, pair, at):
    pieces, piece, pair_cols = buffer_ref.shape[1:]
    first = jnp.bitwise_xor(info_ref[0] // 2, pair) * pair_cols
    return [
        pltpu.make_async_copy(
            weight_ref.at[
                mode_of(info_ref, slot),
                pl.ds(k * piece, piece),
                pl.ds(pl.multiple_of(first, 128), pair_cols),
            ],
            buffer_ref.at[at, k],
            sems.at[at, k],
        )
        for k in range(pieces)
    ]


def weight_shape(weight, pairs):
    width, cols = weight.shape[1:]
    return (pairs, PIECES, width // PIECES, cols // 2)


def fetch_weights(info, weight, ahead):
    shapes = [weight_shape(weight, n_pairs) for _, n_pairs in ahead]
    count = len(ahead)

    def kernel(info_ref, weight_ref, *refs):
        copies = [
            copy
            for i, (slot, n_pairs) in enumerate(ahead)
            for p in range(n_pairs)
            for copy in weight_copies(
                info_ref, weight_ref, refs[i], refs[count + i], slot, p, p
            )
        ]
        for copy in copies:
            copy.start()
        for copy in copies:
            copy.wait()

    return pl.pallas_call(
        kernel,
        out_shape=[pltpu.VMEM(shape, jnp.bfloat16) for shape in shapes],
        in_specs=[SMEM, HBM],
        out_specs=[VMEM] * count,
        scratch_shapes=[pltpu.SemaphoreType.DMA(shape[:2]) for shape in shapes],
        compiler_params=params(1),
        cost_estimate=pl.CostEstimate(
            flops=6_000_000_000, bytes_accessed=25 << 20, transcendentals=0
        ),
        name="fetch_weights",
    )(info, weight)


class Prefetch:
    def __init__(self, out_weight, turns, chips):
        self.weight, self.turns, self.chips = out_weight, turns, chips
        self.shapes = [pltpu.VMEM(out_weight.shape[1:], jnp.bfloat16)] * len(turns)
        self.scratch = pltpu.SemaphoreType.DMA((len(turns),))

    def copies(self, info_ref, weight_ref, kept_refs, sems):
        middle = is_middle(info_ref, self.chips)
        return [
            pltpu.make_async_copy(
                weight_ref.at[mode_of(info_ref, jnp.where(middle, turn[1], turn[0]))],
                kept_refs[i],
                sems.at[i],
            )
            for i, turn in enumerate(self.turns)
        ]


    def start(self, *refs):
        for copy in self.copies(*refs):
            copy.start()

    def wait(self, *refs):
        for copy in self.copies(*refs):
            copy.wait()


def store_pair(info_ref, outs, rows, p, result):
    result = result.astype(jnp.bfloat16)
    cols = result.shape[1] // 2
    odd = info_ref[0] % 2 == 1
    for e in range(2):
        first, last = result[:, e * cols : (e + 1) * cols], result[:, (1 - e) * cols : (2 - e) * cols]
        outs[2 * p + e][rows, :] = jnp.where(odd, last, first)


def project_slots(info, parts, weight, slots, ready=(), ahead=()):
    half, width = parts[0][0].shape
    block = 2 * half
    cols = 3 * HDIM
    heads = weight.shape[2] // cols
    pairs = 2
    count, given = len(slots), len(ready)
    steps = [(n, p) for n in range(count) for p in range(pairs)]
    places = [(i, j) for i, array in enumerate(ready) for j in range(array.shape[0])]
    streamed = steps[len(places) :]
    shape = weight_shape(weight, len(streamed))
    ahead_shapes = [weight_shape(weight, n_pairs) for _, n_pairs in ahead]

    def kernel(info_ref, *refs):
        ins, refs = refs[: 2 * count], refs[2 * count :]
        ready_refs, weight_ref, refs = refs[:given], refs[given], refs[given + 1 :]
        outs, refs = refs[:heads], refs[heads:]
        ahead_refs, refs = refs[: len(ahead)], refs[len(ahead) :]
        buffer_ref, sems, ahead_sems = refs[0], refs[1], refs[2:]
        fetched = {
            step: weight_copies(info_ref, weight_ref, buffer_ref, sems, slots[step[0]], step[1], i)
            for i, step in enumerate(streamed)
        }
        later = [
            copy
            for i, (slot, n_pairs) in enumerate(ahead)
            for p in range(n_pairs)
            for copy in weight_copies(
                info_ref, weight_ref, ahead_refs[i], ahead_sems[i], slot, p, p
            )
        ]
        for copy in [copy for copies in fetched.values() for copy in copies] + later:
            copy.start()

        @pl.when(info_ref[1] >= 0)
        def _():
            for i, (n, p) in enumerate(steps):
                result = None
                piece = width // PIECES
                for k in range(PIECES):
                    if (n, p) in fetched:
                        fetched[n, p][k].wait()
                        part_ref, at = buffer_ref, streamed.index((n, p))
                    else:
                        part_ref, at = ready_refs[places[i][0]], places[i][1]
                    rows = jnp.concatenate(
                        [ins[2 * n + i][:, k * piece : (k + 1) * piece] for i in range(2)], axis=0
                    )
                    part = jnp.dot(rows, part_ref[at, k], preferred_element_type=jnp.float32)
                    result = part if result is None else result + part
                store_pair(info_ref, outs, pl.ds(n * block, block), p, result)

        for copy in later:
            copy.wait()

    return pl.pallas_call(
        kernel,
        out_shape=[pltpu.VMEM((count * block, cols), jnp.bfloat16)] * heads
        + [pltpu.VMEM(ahead_shape, jnp.bfloat16) for ahead_shape in ahead_shapes],
        in_specs=[SMEM] + [VMEM] * (2 * count + given) + [HBM],
        out_specs=[VMEM] * (heads + len(ahead)),
        scratch_shapes=[
            pltpu.VMEM(shape, jnp.bfloat16),
            pltpu.SemaphoreType.DMA(shape[:2]),
        ]
        + [pltpu.SemaphoreType.DMA(ahead_shape[:2]) for ahead_shape in ahead_shapes],
        compiler_params=params(4 + 3 * len(streamed) * 2),
        cost_estimate=pl.CostEstimate(
            flops=2 * count * block * width * cols * heads,
            bytes_accessed=count * width * cols * heads * 2,
            transcendentals=0,
        ),
        name="project_slots",
    )(info, *[piece for pair in parts for piece in pair], *ready, weight)


def project_late(info, inner, relayed, weight, cols, chips, prefetch):
    half, width = inner[0].shape
    block = 2 * half
    pairs, pieces, piece, pair_cols = weight.shape
    heads = pairs * pair_cols // cols

    kept = len(prefetch.turns)

    def kernel(info_ref, inner_own, inner_partner, relayed_own, relayed_partner, weight_ref, *refs):
        next_ref, outs, kept_refs = refs[0], refs[1 : 1 + heads], refs[1 + heads : 1 + heads + kept]
        rows_ref, sems = refs[1 + heads + kept :]
        prefetch.start(info_ref, next_ref, kept_refs, sems)
        middle = is_middle(info_ref, chips)

        @pl.when(middle)
        def _():
            rows_ref[:half, :] = inner_own[...]
            rows_ref[half:, :] = inner_partner[...]

        @pl.when(jnp.logical_not(middle))
        def _():
            rows_ref[:half, :] = relayed_own[...]
            rows_ref[half:, :] = relayed_partner[...]

        for p in range(pairs):
            result = None
            for k in range(pieces):
                part = jnp.dot(
                    rows_ref[:, k * piece : (k + 1) * piece],
                    weight_ref[p, k],
                    preferred_element_type=jnp.float32,
                )
                result = part if result is None else result + part
            store_pair(info_ref, outs, pl.ds(0, block), p, result)
        prefetch.wait(info_ref, next_ref, kept_refs, sems)

    return pl.pallas_call(
        kernel,
        out_shape=[pltpu.VMEM((block, cols), jnp.bfloat16)] * heads + prefetch.shapes,
        in_specs=[SMEM] + [VMEM] * 5 + [HBM],
        out_specs=[VMEM] * (heads + kept),
        scratch_shapes=[pltpu.VMEM((block, width), jnp.bfloat16), prefetch.scratch],
        compiler_params=params(8),
        cost_estimate=pl.CostEstimate(
            flops=2 * block * width * cols * heads,
            bytes_accessed=width * cols * heads * 2,
            transcendentals=0,
        ),
        name="project_late",
    )(info, *inner, *relayed, weight, prefetch.weight)


def attend_slots(info, doc_lengths, sets, turns, chips, prefetch):
    count = len(sets[0][1])
    block = sets[0][1][0].shape[0] // len(sets[0][0])
    total = count * chips * block
    window = min(total // 2 + block, total)
    scale = 1.0 / math.sqrt(HDIM)
    docs = doc_lengths.shape[0]

    kept = len(prefetch.turns)

    def kernel(info_ref, docs_ref, *refs):
        ins, refs = refs[: len(sets) * count], refs[len(sets) * count :]
        next_ref, outs, kept_refs = refs[0], refs[1 : 1 + count], refs[1 + count : 1 + count + kept]
        keys_ref, values_ref, sems = refs[1 + count + kept :]
        prefetch.start(info_ref, next_ref, kept_refs, sems)

        @pl.when(info_ref[1] >= 0)
        def _():
            middle = is_middle(info_ref, chips)
            mu, chip, own_first = info_ref[0], info_ref[1], info_ref[2] * (block // 2)

            def slot_rows(d, slot, part):
                for i, (slots, _) in enumerate(sets):
                    if slot in slots:
                        at = slots.index(slot) * block
                        return ins[i * count + d][at : at + block, part * HDIM : (part + 1) * HDIM]

            for d in range(count):
                for slot in range(chips):
                    index = jnp.bitwise_xor(mu, d) * chips + jnp.bitwise_xor(chip, slot)
                    place = pl.ds(pl.multiple_of(index * block, block), block)
                    keys_ref[place, :] = slot_rows(d, slot, 1)
                    values_ref[place, :] = slot_rows(d, slot, 2)

            ends = []
            end = jnp.int32(0)
            for i in range(docs):
                end = end + docs_ref[i]
                ends.append(end)
            row_place = lax.broadcasted_iota(jnp.int32, (block, 1), 0) + own_first
            row_place = jnp.where(row_place >= block, row_place - block, row_place)
            key_iota = lax.broadcasted_iota(jnp.int32, (1, window), 1)
            key_in_block = key_iota % block + own_first
            key_in_block = jnp.where(key_in_block >= block, key_in_block - block, key_in_block)
            key_place = (key_iota // block) * block + key_in_block
            for n, turn in enumerate(turns):
                slot = jnp.where(middle, turn[1], turn[0])
                for d in range(count):
                    index = jnp.bitwise_xor(mu, d) * chips + jnp.bitwise_xor(chip, slot)
                    first_row = index * block
                    doc_first = jnp.int32(0)
                    for e in ends:
                        doc_first = jnp.where(first_row >= e, e, doc_first)
                    start = jnp.minimum(doc_first // block, (total - window) // block) * block
                    start = pl.multiple_of(start, block)
                    row_pos = row_place + first_row
                    row_first = jnp.zeros((block, 1), jnp.int32)
                    for e in ends:
                        row_first = jnp.where(row_pos >= e, e, row_first)
                    key_pos = key_place + start
                    allowed = (key_pos <= row_pos) & (key_pos >= row_first)
                    query = slot_rows(d, turn[0], 0)
                    if turn[1] != turn[0]:
                        query = jnp.where(middle, slot_rows(d, turn[1], 0), query)
                    scores = lax.dot_general(
                        query,
                        keys_ref[pl.ds(start, window), :],
                        (((1,), (1,)), ((), ())),
                        preferred_element_type=jnp.float32,
                    )
                    scores = jnp.where(allowed, scores * scale, -1e30)
                    row_max = jnp.max(scores, axis=1, keepdims=True)
                    weights = jnp.where(allowed, jnp.exp(scores - row_max), 0.0)
                    totals = jnp.sum(weights, axis=1, keepdims=True)
                    summed = jnp.dot(
                        weights.astype(jnp.bfloat16),
                        values_ref[pl.ds(start, window), :],
                        preferred_element_type=jnp.float32,
                    )
                    outs[d][n * block : (n + 1) * block, :] = (summed / totals).astype(jnp.bfloat16)

        prefetch.wait(info_ref, next_ref, kept_refs, sems)

    n_queries = len(turns) * count
    return pl.pallas_call(
        kernel,
        out_shape=[pltpu.VMEM((len(turns) * block, HDIM), jnp.bfloat16)] * count
        + prefetch.shapes,
        in_specs=[SMEM, SMEM] + [VMEM] * (len(sets) * count) + [HBM],
        out_specs=[VMEM] * (count + kept),
        scratch_shapes=[
            pltpu.VMEM((total, HDIM), jnp.bfloat16),
            pltpu.VMEM((total, HDIM), jnp.bfloat16),
            prefetch.scratch,
        ],
        compiler_params=params(14),
        cost_estimate=pl.CostEstimate(
            flops=n_queries * block * window * HDIM * 8,
            bytes_accessed=3 * total * HDIM * 2,
            transcendentals=n_queries * block * window,
        ),
        name="attend_slots",
    )(info, doc_lengths, *[piece for _, pieces in sets for piece in pieces], prefetch.weight)


def output_rows(info, pieces, weight, index, turns):
    count = len(pieces)
    block = pieces[0].shape[0] // turns
    half = block // 2
    at = index * block
    depth, width = weight.shape
    tile = min(1024, width)

    def kernel(info_ref, *refs):
        ins = refs[:count]
        weight_ref, own_ref, partner_ref, heads_ref = refs[count:]
        for d in range(count):
            heads_ref[jnp.bitwise_xor(info_ref[0], d)] = ins[d][at : at + block, :]
        rows = jnp.concatenate([heads_ref[h] for h in range(count)], axis=1)
        for first in range(0, width, tile):
            cols = slice(first, first + tile)
            result = jnp.dot(rows, weight_ref[:, cols], preferred_element_type=jnp.float32)
            result = result.astype(jnp.bfloat16)
            own_ref[:, cols] = result[:half]
            partner_ref[:, cols] = result[half:]

    return pl.pallas_call(
        kernel,
        out_shape=[pltpu.VMEM((half, width), jnp.bfloat16)] * 2,
        in_specs=[SMEM] + [VMEM] * (count + 1),
        out_specs=[VMEM] * 2,
        scratch_shapes=[pltpu.VMEM((count, block, HDIM), jnp.bfloat16)],
        compiler_params=params(8),
        cost_estimate=pl.CostEstimate(
            flops=2 * block * depth * width,
            bytes_accessed=depth * width * 2,
            transcendentals=0,
        ),
        name="output_rows",
    )(info, *pieces, weight)


def in_vmem(*values):
    return [pltpu.with_memory_space_constraint(value, pltpu.VMEM) for value in values]


def add_rows(first, second):
    def kernel(first_ref, second_ref, out_ref):
        total = first_ref[...].astype(jnp.float32) + second_ref[...].astype(jnp.float32)
        out_ref[...] = total.astype(jnp.bfloat16)

    return pl.pallas_call(
        kernel,
        out_shape=pltpu.VMEM(first.shape, jnp.bfloat16),
        in_specs=[VMEM, VMEM],
        out_specs=VMEM,
        compiler_params=params(4),
        cost_estimate=pl.CostEstimate(
            flops=4 * first.size, bytes_accessed=6 * first.size, transcendentals=0
        ),
        name="add_rows",
    )(*in_vmem(first, second))


def relay_rows(info, chips, own, partner, passing, otherwise):
    def kernel(info_ref, own_ref, partner_ref, passing_ref, otherwise_ref, sum_ref, relay_ref):
        middle = is_middle(info_ref, chips)

        @pl.when(middle)
        def _():
            total = own_ref[...].astype(jnp.float32) + partner_ref[...].astype(jnp.float32)
            sum_ref[...] = total.astype(jnp.bfloat16)
            total = total + passing_ref[...].astype(jnp.float32)
            relay_ref[...] = total.astype(jnp.bfloat16)

        @pl.when(jnp.logical_not(middle))
        def _():
            total = own_ref[...].astype(jnp.float32) + partner_ref[...].astype(jnp.float32)
            sum_ref[...] = total.astype(jnp.bfloat16)
            relay_ref[...] = otherwise_ref[...]

    return pl.pallas_call(
        kernel,
        out_shape=[pltpu.VMEM(own.shape, jnp.bfloat16)] * 2,
        in_specs=[SMEM] + [VMEM] * 4,
        out_specs=[VMEM] * 2,
        compiler_params=params(4),
        cost_estimate=pl.CostEstimate(
            flops=4 * own.size, bytes_accessed=12 * own.size, transcendentals=0
        ),
        name="relay_rows",
    )(info, *in_vmem(own, partner, passing, otherwise))


def last_rows(info, chips, early, far, middle_only):
    rows, width = far.shape
    parts = 4
    part = rows // parts

    def kernel(info_ref, early_ref, far_ref, middle_ref, out_ref, done_ref, sems):
        factor = jnp.where(is_middle(info_ref, chips), 1.0, 0.0)
        copies = []
        for i in range(parts):
            at = pl.ds(i * part, part)
            total = early_ref[at] + far_ref[at].astype(jnp.float32)
            total = total + middle_ref[at].astype(jnp.float32) * factor
            done_ref[at] = total.astype(jnp.bfloat16)
            copies.append(pltpu.make_async_copy(done_ref.at[at], out_ref.at[at], sems.at[i]))
            copies[i].start()
        for copy in copies:
            copy.wait()

    return pl.pallas_call(
        kernel,
        out_shape=pltpu.HBM(far.shape, jnp.bfloat16),
        in_specs=[SMEM, VMEM, VMEM, VMEM],
        out_specs=HBM,
        scratch_shapes=[
            pltpu.VMEM((rows, width), jnp.bfloat16),
            pltpu.SemaphoreType.DMA((parts,)),
        ],
        compiler_params=params(6),
        cost_estimate=pl.CostEstimate(
            flops=4 * far.size, bytes_accessed=10 * far.size, transcendentals=0
        ),
        name="last_rows",
    )(info, *in_vmem(early, far, middle_only))


def chip_pairs(pairs):
    return [(2 * a + core, 2 * b + core) for a, b in pairs for core in range(2)]


def line_body(tokens, norm_gain, qkv_weight, out_weight, modality, doc_lengths):
    seq_count = lax.axis_size("seq")
    mod_count = lax.axis_size("mod")
    chips = seq_count // 2
    mu = lax.axis_index("mod").astype(jnp.int32)
    seq = lax.axis_index("seq").astype(jnp.int32)
    ids = jnp.stack([mu, seq // 2, seq % 2])
    qkv_weight = pltpu.with_memory_space_constraint(qkv_weight, pltpu.HBM)
    out_weight = pltpu.with_memory_space_constraint(out_weight, pltpu.HBM)

    def along(value, pairs):
        return lax.ppermute(value, "seq", chip_pairs(pairs))

    def swap(value):
        return lax.ppermute(value, "seq", [(i, i ^ 1) for i in range(seq_count)])

    def exchange(pieces):
        moved = [pieces[0]]
        for d in range(1, mod_count):
            moved.append(lax.ppermute(pieces[d], "mod", [(i, i ^ d) for i in range(mod_count)]))
        return moved

    in_hbm = [
        pltpu.with_memory_space_constraint(value, pltpu.HBM)
        for value in (modality, tokens, norm_gain)
    ]
    normed, info = norm_rows(ids, *in_hbm, chips)
    two = along(normed, [(i, i ^ 2) for i in range(chips)])
    one = along(normed, [(i, i ^ 1) for i in range(chips)])
    inner = along(normed, [(1, 2), (2, 1)])
    relayed = along(two, [(i, i ^ 1) for i in range(chips)])
    own_pair = (normed, swap(normed))
    two_pair = (two, swap(two))
    one_pair = (one, swap(one))
    inner_pair = (inner, swap(inner))
    relayed_pair = (relayed, swap(relayed))
    turn_a, turn_b, turn_c, turn_d = (3, 1), (2, 3), (1, 2), (0, 0)

    *own, late_weight = project_slots(
        info, [own_pair], qkv_weight, (0,), ahead=((3, 2),)
    )
    own = exchange(own)
    two_weight, one_weight = fetch_weights(info, qkv_weight, ((2, 2), (1, 1)))
    mid = project_slots(
        info, [two_pair, one_pair], qkv_weight, (2, 1), ready=(two_weight, one_weight)
    )
    mid = exchange(mid)
    *late, kept_a = project_late(
        info,
        inner_pair,
        relayed_pair,
        late_weight,
        3 * HDIM,
        chips,
        Prefetch(out_weight, (turn_a,), chips),
    )
    late = exchange(late)
    sets = (((0,), own), ((2, 1), mid), ((3,), late))

    def finish(pieces, kept, index, turns):
        own_share, partner_share = output_rows(info, pieces, kept, index, turns)
        return own_share, swap(partner_share)

    *first, kept_b = attend_slots(
        info,
        doc_lengths,
        sets,
        (turn_a, turn_b),
        chips,
        Prefetch(out_weight, (turn_b,), chips),
    )
    first = exchange(first)
    *rest_c, kept_c = attend_slots(
        info, doc_lengths, sets, (turn_c,), chips, Prefetch(out_weight, (turn_c,), chips)
    )
    sum_a = add_rows(*finish(first, kept_a, 0, 2))
    own_b, partner_b = finish(first, kept_b, 1, 2)
    from_one = along(sum_a, [(i, i ^ 1) for i in range(chips)])
    sum_b = add_rows(own_b, partner_b)
    from_inner = along(sum_b, [(1, 2), (2, 1)])
    rest_c = exchange(rest_c)
    shares_c = finish(rest_c, kept_c, 0, 1)
    chip = seq // 2
    middle = (chip > 0) & (chip < chips - 1)
    sum_c, relay_sum = relay_rows(info, chips, *shares_c, from_one, sum_b)
    from_two = along(relay_sum, [(i, i ^ 2) for i in range(chips)])
    from_end = along(sum_c, [(i, i ^ 1) for i in range(chips)])
    *rest_d, kept_d = attend_slots(
        info, doc_lengths, sets, (turn_d,), chips, Prefetch(out_weight, (turn_d,), chips)
    )
    rest_d = exchange(rest_d)
    shares_d = finish(rest_d, kept_d, 0, 1)
    near = jnp.where(middle, from_inner, from_one)
    early = tokens.astype(jnp.float32)
    for share in (*shares_d, near):
        early = early + share.astype(jnp.float32)
    return last_rows(info, chips, early, from_two, from_end)


def solution(mesh):
    fits = mesh.shape["seq"] == 8 and mesh.shape["mod"] == 4

    def body(tokens, norm_gain, qkv_weight, out_weight, modality, doc_lengths):
        whole = tokens.shape[0] * 2 == BLOCK and qkv_weight.shape[2] == 12 * HDIM
        chosen = line_body if fits and whole else general_body
        return chosen(tokens, norm_gain, qkv_weight, out_weight, modality, doc_lengths)

    return jax.shard_map(
        body,
        mesh=mesh,
        in_specs=(
            P(("mod", "seq"), None),
            P(),
            P(None, None, "seq"),
            P(None, "seq", None),
            P(),
            P(),
        ),
        out_specs=P(("mod", "seq"), None),
        check_vma=False,
    )
```

```python
import math

import jax
import jax.numpy as jnp
from jax import lax
from jax.experimental import pallas as pl
from jax.experimental.pallas import tpu as pltpu
from jax.sharding import PartitionSpec as P


HDIM = 128
BLOCK = 128


def modes_of_rows(first_row, row_count, modality):
    block_ids = (first_row + jnp.arange(row_count, dtype=jnp.int32)) // BLOCK
    block_table = jnp.arange(modality.shape[0], dtype=jnp.int32)
    picked = jnp.where(block_ids[:, None] == block_table[None, :], modality[None, :], 0)
    return jnp.sum(picked, axis=1)


def documents(positions, doc_lengths):
    doc_ends = jnp.cumsum(doc_lengths)
    return jnp.sum((positions[:, None] >= doc_ends[None, :]).astype(jnp.int32), axis=1)


def general_body(tokens, norm_gain, qkv_weight, out_weight, modality, doc_lengths):
    row_count = tokens.shape[0]
    seq_count = lax.axis_size("seq")
    mod_count = lax.axis_size("mod")
    group_rows = row_count * seq_count
    mod_index = lax.axis_index("mod")
    own_first = (mod_index * seq_count + lax.axis_index("seq")) * row_count
    row_modes = modes_of_rows(own_first, row_count, modality)
    choose = (
        row_modes[:, None, None] == jnp.arange(norm_gain.shape[0], dtype=jnp.int32)[None, :, None]
    )
    gain_rows = jnp.sum(jnp.where(choose, norm_gain[None, :, :], 0.0), axis=1)
    values = tokens.astype(jnp.float32)
    mean_square = jnp.mean(values * values, axis=1, keepdims=True)
    normed = (values * lax.rsqrt(mean_square + 1e-05) * gain_rows).astype(jnp.bfloat16)
    gathered = lax.all_gather(normed, "seq", axis=0, tiled=True)
    group_first = mod_index * group_rows
    block_count = group_rows // BLOCK
    block_modes = lax.dynamic_slice_in_dim(modality, group_first // BLOCK, block_count)
    heads_here = qkv_weight.shape[2] // (3 * HDIM)

    def project(block_pair):
        row_block, block_mode = block_pair
        weight = lax.dynamic_index_in_dim(qkv_weight, block_mode, 0, keepdims=False)
        return jnp.dot(row_block, weight, preferred_element_type=jnp.float32).astype(jnp.bfloat16)

    projected = lax.map(
        project, (gathered.reshape(block_count, BLOCK, gathered.shape[1]), block_modes)
    )
    projected = projected.reshape(group_rows, heads_here, 3, HDIM)
    queries = projected[:, :, 0, :]
    keys_here = projected[:, :, 1, :]
    values_here = projected[:, :, 2, :]
    quarter = group_rows // mod_count
    local_rows = jnp.arange(group_rows, dtype=jnp.int32)
    query_pos = group_first + local_rows
    query_docs = documents(query_pos, doc_lengths)
    block_size = min(512, quarter)
    block_total = group_rows // block_size
    score_scale = 1.0 / math.sqrt(HDIM)
    query_blocks = queries.reshape(block_total, block_size, heads_here, HDIM)
    pos_blocks = query_pos.reshape(block_total, block_size)
    doc_blocks = query_docs.reshape(block_total, block_size)
    piece_keys = lax.all_gather(keys_here, "mod", axis=0, tiled=True)
    piece_values = lax.all_gather(values_here, "mod", axis=0, tiled=True)
    key_pos = jnp.arange(piece_keys.shape[0], dtype=jnp.int32)
    key_docs = documents(key_pos, doc_lengths)

    def one_block(block_state):
        query_block, block_pos, block_docs = block_state
        scores = (
            jnp.einsum("qhc,khc->hqk", query_block, piece_keys, preferred_element_type=jnp.float32)
            * score_scale
        )
        allowed = (
            (key_pos[None, :] <= block_pos[:, None]) & (key_docs[None, :] == block_docs[:, None])
        )[None, :, :]
        row_max = jnp.max(jnp.where(allowed, scores, -1e30), axis=2)
        weights = jnp.where(allowed, jnp.exp(scores - row_max[:, :, None]), 0.0)
        totals = jnp.sum(weights, axis=2)
        rows = jnp.einsum(
            "hqk,khc->qhc",
            weights.astype(jnp.bfloat16),
            piece_values,
            preferred_element_type=jnp.float32,
        )
        return (rows / jnp.transpose(totals)[:, :, None]).astype(jnp.bfloat16)

    attended = lax.map(one_block, (query_blocks, pos_blocks, doc_blocks))
    attended = attended.reshape(group_rows, heads_here * HDIM)

    def output(block_pair):
        row_block, block_mode = block_pair
        weight = lax.dynamic_index_in_dim(out_weight, block_mode, 0, keepdims=False)
        return jnp.dot(row_block, weight, preferred_element_type=jnp.float32)

    partial_value = lax.map(
        output, (attended.reshape(block_count, BLOCK, attended.shape[1]), block_modes)
    )
    head_sums = lax.psum_scatter(
        partial_value.reshape(group_rows, partial_value.shape[2]).astype(jnp.bfloat16),
        "seq",
        scatter_dimension=0,
        tiled=True,
    ).astype(jnp.float32)
    return (tokens.astype(jnp.float32) + head_sums).astype(jnp.bfloat16)


SMEM = pl.BlockSpec(memory_space=pltpu.SMEM)
VMEM = pl.BlockSpec(memory_space=pltpu.VMEM)
HBM = pl.BlockSpec(memory_space=pltpu.HBM)
PIECES = 4


def mesh_place():
    seq = lax.axis_index("seq")
    return lax.axis_index("mod"), seq // 2, seq % 2


def is_middle(chips):
    chip = mesh_place()[1]
    return (chip > 0) & (chip < chips - 1)


def mode_of(info, slot):
    return info[slot]


def params(mib):
    return pltpu.CompilerParams(vmem_limit_bytes=mib << 20)


def norm_rows(modality, doc_lengths, tokens, norm_gain, chips):
    rows, width = tokens.shape
    modes = norm_gain.shape[0]
    step = 16
    parts = 4
    part = rows // parts
    docs = doc_lengths.shape[0]

    def kernel(modality_ref, docs_ref, tokens_ref, gain_ref, out_ref, info_ref, *scratch):
        rows_ref, gains_ref, table_ref, lengths_ref, row_sems, sems = scratch
        table_copy = pltpu.make_async_copy(modality_ref, table_ref, sems.at[0])
        table_copy.start()
        lengths_copy = pltpu.make_async_copy(docs_ref, lengths_ref, sems.at[2])
        lengths_copy.start()
        gain_copy = pltpu.make_async_copy(gain_ref, gains_ref, sems.at[1])
        gain_copy.start()
        row_copies = [
            pltpu.make_async_copy(
                tokens_ref.at[pl.ds(i * part, part)],
                rows_ref.at[pl.ds(i * part, part)],
                row_sems.at[i],
            )
            for i in range(parts)
        ]
        for copy in row_copies:
            copy.start()
        table_copy.wait()
        lengths_copy.wait()
        mu, chip, _ = mesh_place()
        for slot in range(chips):
            info_ref[slot] = table_ref[mu * chips + jnp.bitwise_xor(chip, slot)]
        end = jnp.int32(0)
        for i in range(docs):
            end = end + lengths_ref[i]
            info_ref[chips + i] = end
        mode = table_ref[mu * chips + chip]
        gain_copy.wait()
        gain = gains_ref[pl.ds(mode, 1), :]
        for i in range(parts):
            row_copies[i].wait()
            for first in range(i * part, (i + 1) * part, step):
                values = rows_ref[first : first + step, :].astype(jnp.float32)
                mean_square = jnp.sum(values * values, axis=1, keepdims=True) * (1.0 / width)
                scaled = values * lax.rsqrt(mean_square + 1e-05) * gain
                out_ref[first : first + step, :] = scaled.astype(jnp.bfloat16)

    return pl.pallas_call(
        kernel,
        out_shape=[
            pltpu.VMEM((rows, width), jnp.bfloat16),
            jax.ShapeDtypeStruct((chips + docs,), jnp.int32),
        ],
        in_specs=[HBM] * 4,
        out_specs=[VMEM, SMEM],
        scratch_shapes=[
            pltpu.VMEM((rows, width), jnp.bfloat16),
            pltpu.VMEM((modes, width), jnp.float32),
            pltpu.SMEM(modality.shape, jnp.int32),
            pltpu.SMEM(doc_lengths.shape, jnp.int32),
            pltpu.SemaphoreType.DMA((parts,)),
            pltpu.SemaphoreType.DMA((3,)),
        ],
        compiler_params=params(8),
        cost_estimate=pl.CostEstimate(flops=4_000_000, bytes_accessed=1 << 20, transcendentals=64),
        name="norm_rows",
    )(modality, doc_lengths, tokens, norm_gain)


def weight_copies(info_ref, weight_ref, buffer_ref, sems, slot, pair, at):
    pieces, piece, pair_cols = buffer_ref.shape[1:]
    first = jnp.bitwise_xor(mesh_place()[0] // 2, pair) * pair_cols
    return [
        pltpu.make_async_copy(
            weight_ref.at[
                mode_of(info_ref, slot),
                pl.ds(k * piece, piece),
                pl.ds(pl.multiple_of(first, 128), pair_cols),
            ],
            buffer_ref.at[at, k],
            sems.at[at, k],
        )
        for k in range(pieces)
    ]


def weight_shape(weight, pairs):
    width, cols = weight.shape[1:]
    return (pairs, PIECES, width // PIECES, cols // 2)


def fetch_weights(info, weight, ahead):
    shapes = [weight_shape(weight, n_pairs) for _, n_pairs in ahead]
    count = len(ahead)

    def kernel(info_ref, weight_ref, *refs):
        copies = [
            copy
            for i, (slot, n_pairs) in enumerate(ahead)
            for p in range(n_pairs)
            for copy in weight_copies(
                info_ref, weight_ref, refs[i], refs[count + i], slot, p, p
            )
        ]
        for copy in copies:
            copy.start()
        for copy in copies:
            copy.wait()

    return pl.pallas_call(
        kernel,
        out_shape=[pltpu.VMEM(shape, jnp.bfloat16) for shape in shapes],
        in_specs=[SMEM, HBM],
        out_specs=[VMEM] * count,
        scratch_shapes=[pltpu.SemaphoreType.DMA(shape[:2]) for shape in shapes],
        compiler_params=params(1),
        cost_estimate=pl.CostEstimate(
            flops=6_000_000_000, bytes_accessed=25 << 20, transcendentals=0
        ),
        name="fetch_weights",
    )(info, weight)


class Prefetch:
    def __init__(self, out_weight, turns, chips):
        self.weight, self.turns, self.chips = out_weight, turns, chips
        self.shapes = [pltpu.VMEM(out_weight.shape[1:], jnp.bfloat16)] * len(turns)
        self.scratch = pltpu.SemaphoreType.DMA((len(turns),))

    def copies(self, info_ref, weight_ref, kept_refs, sems):
        middle = is_middle(self.chips)
        return [
            pltpu.make_async_copy(
                weight_ref.at[mode_of(info_ref, jnp.where(middle, turn[1], turn[0]))],
                kept_refs[i],
                sems.at[i],
            )
            for i, turn in enumerate(self.turns)
        ]


    def start(self, *refs):
        for copy in self.copies(*refs):
            copy.start()

    def wait(self, *refs):
        for copy in self.copies(*refs):
            copy.wait()


def store_pair(outs, rows, p, result):
    result = result.astype(jnp.bfloat16)
    cols = result.shape[1] // 2
    odd = mesh_place()[0] % 2 == 1
    for e in range(2):
        first, last = result[:, e * cols : (e + 1) * cols], result[:, (1 - e) * cols : (2 - e) * cols]
        outs[2 * p + e][rows, :] = jnp.where(odd, last, first)


def project_slots(info, parts, weight, slots, ready=(), ahead=()):
    half, width = parts[0][0].shape
    block = 2 * half
    cols = 3 * HDIM
    heads = weight.shape[2] // cols
    pairs = 2
    count, given = len(slots), len(ready)
    steps = [(n, p) for n in range(count) for p in range(pairs)]
    places = [(i, j) for i, array in enumerate(ready) for j in range(array.shape[0])]
    streamed = steps[len(places) :]
    shape = weight_shape(weight, len(streamed))
    ahead_shapes = [weight_shape(weight, n_pairs) for _, n_pairs in ahead]

    def kernel(info_ref, *refs):
        ins, refs = refs[: 2 * count], refs[2 * count :]
        ready_refs, weight_ref, refs = refs[:given], refs[given], refs[given + 1 :]
        outs, refs = refs[:heads], refs[heads:]
        ahead_refs, refs = refs[: len(ahead)], refs[len(ahead) :]
        buffer_ref, sems, ahead_sems = refs[0], refs[1], refs[2:]
        fetched = {
            step: weight_copies(info_ref, weight_ref, buffer_ref, sems, slots[step[0]], step[1], i)
            for i, step in enumerate(streamed)
        }
        later = [
            copy
            for i, (slot, n_pairs) in enumerate(ahead)
            for p in range(n_pairs)
            for copy in weight_copies(
                info_ref, weight_ref, ahead_refs[i], ahead_sems[i], slot, p, p
            )
        ]
        for copy in [copy for copies in fetched.values() for copy in copies] + later:
            copy.start()

        @pl.when(mesh_place()[1] >= 0)
        def _():
            for i, (n, p) in enumerate(steps):
                result = None
                piece = width // PIECES
                for k in range(PIECES):
                    if (n, p) in fetched:
                        fetched[n, p][k].wait()
                        part_ref, at = buffer_ref, streamed.index((n, p))
                    else:
                        part_ref, at = ready_refs[places[i][0]], places[i][1]
                    rows = jnp.concatenate(
                        [ins[2 * n + i][:, k * piece : (k + 1) * piece] for i in range(2)], axis=0
                    )
                    part = jnp.dot(rows, part_ref[at, k], preferred_element_type=jnp.float32)
                    result = part if result is None else result + part
                store_pair(outs, pl.ds(n * block, block), p, result)

        for copy in later:
            copy.wait()

    return pl.pallas_call(
        kernel,
        out_shape=[pltpu.VMEM((count * block, cols), jnp.bfloat16)] * heads
        + [pltpu.VMEM(ahead_shape, jnp.bfloat16) for ahead_shape in ahead_shapes],
        in_specs=[SMEM] + [VMEM] * (2 * count + given) + [HBM],
        out_specs=[VMEM] * (heads + len(ahead)),
        scratch_shapes=[
            pltpu.VMEM(shape, jnp.bfloat16),
            pltpu.SemaphoreType.DMA(shape[:2]),
        ]
        + [pltpu.SemaphoreType.DMA(ahead_shape[:2]) for ahead_shape in ahead_shapes],
        compiler_params=params(4 + 3 * len(streamed) * 2),
        cost_estimate=pl.CostEstimate(
            flops=2 * count * block * width * cols * heads,
            bytes_accessed=count * width * cols * heads * 2,
            transcendentals=0,
        ),
        name="project_slots",
    )(info, *[piece for pair in parts for piece in pair], *ready, weight)


def project_late(inner, relayed, weight, cols, chips):
    half, width = inner[0].shape
    block = 2 * half
    pairs, pieces, piece, pair_cols = weight.shape
    heads = pairs * pair_cols // cols

    def kernel(inner_own, inner_partner, relayed_own, relayed_partner, weight_ref, *refs):
        outs, rows_ref = refs[:heads], refs[heads]
        middle = is_middle(chips)

        @pl.when(middle)
        def _():
            rows_ref[:half, :] = inner_own[...]
            rows_ref[half:, :] = inner_partner[...]

        @pl.when(jnp.logical_not(middle))
        def _():
            rows_ref[:half, :] = relayed_own[...]
            rows_ref[half:, :] = relayed_partner[...]

        for p in range(pairs):
            result = None
            for k in range(pieces):
                part = jnp.dot(
                    rows_ref[:, k * piece : (k + 1) * piece],
                    weight_ref[p, k],
                    preferred_element_type=jnp.float32,
                )
                result = part if result is None else result + part
            store_pair(outs, pl.ds(0, block), p, result)

    return pl.pallas_call(
        kernel,
        out_shape=[pltpu.VMEM((block, cols), jnp.bfloat16)] * heads,
        in_specs=[VMEM] * 5,
        out_specs=[VMEM] * heads,
        scratch_shapes=[pltpu.VMEM((block, width), jnp.bfloat16)],
        compiler_params=params(8),
        cost_estimate=pl.CostEstimate(
            flops=2 * block * width * cols * heads,
            bytes_accessed=width * cols * heads * 2,
            transcendentals=0,
        ),
        name="project_late",
    )(*inner, *relayed, weight)


def attend_slots(info, docs, sets, turns, chips, prefetch):
    count = len(sets[0][1])
    block = sets[0][1][0].shape[0] // len(sets[0][0])
    total = count * chips * block
    window = min(total // 2 + block, total)
    scale = 1.0 / math.sqrt(HDIM)

    kept = len(prefetch.turns)

    def kernel(info_ref, *refs):
        ins, refs = refs[: len(sets) * count], refs[len(sets) * count :]
        next_ref, outs, kept_refs = refs[0], refs[1 : 1 + count], refs[1 + count : 1 + count + kept]
        keys_ref, values_ref, sems = refs[1 + count + kept :]
        prefetch.start(info_ref, next_ref, kept_refs, sems)

        @pl.when(mesh_place()[1] >= 0)
        def _():
            middle = is_middle(chips)
            mu, chip, core = mesh_place()
            own_first = core * (block // 2)

            def slot_rows(d, slot, part):
                for i, (slots, _) in enumerate(sets):
                    if slot in slots:
                        at = slots.index(slot) * block
                        return ins[i * count + d][at : at + block, part * HDIM : (part + 1) * HDIM]

            for d in range(count):
                for slot in range(chips):
                    index = jnp.bitwise_xor(mu, d) * chips + jnp.bitwise_xor(chip, slot)
                    place = pl.ds(pl.multiple_of(index * block, block), block)
                    keys_ref[place, :] = slot_rows(d, slot, 1)
                    values_ref[place, :] = slot_rows(d, slot, 2)

            ends = [info_ref[chips + i] for i in range(docs)]
            row_place = lax.broadcasted_iota(jnp.int32, (block, 1), 0) + own_first
            row_place = jnp.where(row_place >= block, row_place - block, row_place)
            key_iota = lax.broadcasted_iota(jnp.int32, (1, window), 1)
            key_in_block = key_iota % block + own_first
            key_in_block = jnp.where(key_in_block >= block, key_in_block - block, key_in_block)
            key_place = (key_iota // block) * block + key_in_block
            for n, turn in enumerate(turns):
                slot = jnp.where(middle, turn[1], turn[0])
                for d in range(count):
                    index = jnp.bitwise_xor(mu, d) * chips + jnp.bitwise_xor(chip, slot)
                    first_row = index * block
                    doc_first = jnp.int32(0)
                    for e in ends:
                        doc_first = jnp.where(first_row >= e, e, doc_first)
                    start = jnp.minimum(doc_first // block, (total - window) // block) * block
                    start = pl.multiple_of(start, block)
                    row_pos = row_place + first_row
                    row_first = jnp.zeros((block, 1), jnp.int32)
                    for e in ends:
                        row_first = jnp.where(row_pos >= e, e, row_first)
                    key_pos = key_place + start
                    allowed = (key_pos <= row_pos) & (key_pos >= row_first)
                    query = slot_rows(d, turn[0], 0)
                    if turn[1] != turn[0]:
                        query = jnp.where(middle, slot_rows(d, turn[1], 0), query)
                    scores = lax.dot_general(
                        query,
                        keys_ref[pl.ds(start, window), :],
                        (((1,), (1,)), ((), ())),
                        preferred_element_type=jnp.float32,
                    )
                    scores = jnp.where(allowed, scores * scale, -1e30)
                    row_max = jnp.max(scores, axis=1, keepdims=True)
                    weights = jnp.where(allowed, jnp.exp(scores - row_max), 0.0)
                    totals = jnp.sum(weights, axis=1, keepdims=True)
                    summed = jnp.dot(
                        weights.astype(jnp.bfloat16),
                        values_ref[pl.ds(start, window), :],
                        preferred_element_type=jnp.float32,
                    )
                    outs[d][n * block : (n + 1) * block, :] = (summed / totals).astype(jnp.bfloat16)

        prefetch.wait(info_ref, next_ref, kept_refs, sems)

    n_queries = len(turns) * count
    return pl.pallas_call(
        kernel,
        out_shape=[pltpu.VMEM((len(turns) * block, HDIM), jnp.bfloat16)] * count
        + prefetch.shapes,
        in_specs=[SMEM] + [VMEM] * (len(sets) * count) + [HBM],
        out_specs=[VMEM] * (count + kept),
        scratch_shapes=[
            pltpu.VMEM((total, HDIM), jnp.bfloat16),
            pltpu.VMEM((total, HDIM), jnp.bfloat16),
            prefetch.scratch,
        ],
        compiler_params=params(14),
        cost_estimate=pl.CostEstimate(
            flops=n_queries * block * window * HDIM * 8,
            bytes_accessed=3 * total * HDIM * 2,
            transcendentals=n_queries * block * window,
        ),
        name="attend_slots",
    )(info, *[piece for _, pieces in sets for piece in pieces], prefetch.weight)


def output_rows(pieces, weight, index, turns):
    count = len(pieces)
    block = pieces[0].shape[0] // turns
    half = block // 2
    at = index * block
    depth, width = weight.shape
    tile = min(1024, width)

    def kernel(*refs):
        ins = refs[:count]
        weight_ref, own_ref, partner_ref, heads_ref = refs[count:]
        for d in range(count):
            heads_ref[jnp.bitwise_xor(mesh_place()[0], d)] = ins[d][at : at + block, :]
        rows = jnp.concatenate([heads_ref[h] for h in range(count)], axis=1)
        for first in range(0, width, tile):
            cols = slice(first, first + tile)
            result = jnp.dot(rows, weight_ref[:, cols], preferred_element_type=jnp.float32)
            result = result.astype(jnp.bfloat16)
            own_ref[:, cols] = result[:half]
            partner_ref[:, cols] = result[half:]

    return pl.pallas_call(
        kernel,
        out_shape=[pltpu.VMEM((half, width), jnp.bfloat16)] * 2,
        in_specs= [VMEM] * (count + 1),
        out_specs=[VMEM] * 2,
        scratch_shapes=[pltpu.VMEM((count, block, HDIM), jnp.bfloat16)],
        compiler_params=params(8),
        cost_estimate=pl.CostEstimate(
            flops=2 * block * depth * width,
            bytes_accessed=depth * width * 2,
            transcendentals=0,
        ),
        name="output_rows",
    )(*pieces, weight)


def in_vmem(*values):
    return [pltpu.with_memory_space_constraint(value, pltpu.VMEM) for value in values]


def add_rows(first, second):
    def kernel(first_ref, second_ref, out_ref):
        total = first_ref[...].astype(jnp.float32) + second_ref[...].astype(jnp.float32)
        out_ref[...] = total.astype(jnp.bfloat16)

    return pl.pallas_call(
        kernel,
        out_shape=pltpu.VMEM(first.shape, jnp.bfloat16),
        in_specs=[VMEM, VMEM],
        out_specs=VMEM,
        compiler_params=params(4),
        cost_estimate=pl.CostEstimate(
            flops=4 * first.size, bytes_accessed=6 * first.size, transcendentals=0
        ),
        name="add_rows",
    )(*in_vmem(first, second))


def relay_rows(chips, own, partner, passing, otherwise):
    def kernel(own_ref, partner_ref, passing_ref, otherwise_ref, sum_ref, relay_ref):
        middle = is_middle(chips)

        @pl.when(middle)
        def _():
            total = own_ref[...].astype(jnp.float32) + partner_ref[...].astype(jnp.float32)
            sum_ref[...] = total.astype(jnp.bfloat16)
            total = total + passing_ref[...].astype(jnp.float32)
            relay_ref[...] = total.astype(jnp.bfloat16)

        @pl.when(jnp.logical_not(middle))
        def _():
            total = own_ref[...].astype(jnp.float32) + partner_ref[...].astype(jnp.float32)
            sum_ref[...] = total.astype(jnp.bfloat16)
            relay_ref[...] = otherwise_ref[...]

    return pl.pallas_call(
        kernel,
        out_shape=[pltpu.VMEM(own.shape, jnp.bfloat16)] * 2,
        in_specs=[VMEM] * 4,
        out_specs=[VMEM] * 2,
        compiler_params=params(4),
        cost_estimate=pl.CostEstimate(
            flops=4 * own.size, bytes_accessed=12 * own.size, transcendentals=0
        ),
        name="relay_rows",
    )(*in_vmem(own, partner, passing, otherwise))


def last_rows(chips, early, far, middle_only):
    rows, width = far.shape
    parts = 4
    part = rows // parts

    def kernel(early_ref, far_ref, middle_ref, out_ref, done_ref, sems):
        factor = jnp.where(is_middle(chips), 1.0, 0.0)
        copies = []
        for i in range(parts):
            at = pl.ds(i * part, part)
            total = early_ref[at] + far_ref[at].astype(jnp.float32)
            total = total + middle_ref[at].astype(jnp.float32) * factor
            done_ref[at] = total.astype(jnp.bfloat16)
            copies.append(pltpu.make_async_copy(done_ref.at[at], out_ref.at[at], sems.at[i]))
            copies[i].start()
        for copy in copies:
            copy.wait()

    return pl.pallas_call(
        kernel,
        out_shape=pltpu.HBM(far.shape, jnp.bfloat16),
        in_specs=[VMEM] * 3,
        out_specs=HBM,
        scratch_shapes=[
            pltpu.VMEM((rows, width), jnp.bfloat16),
            pltpu.SemaphoreType.DMA((parts,)),
        ],
        compiler_params=params(6),
        cost_estimate=pl.CostEstimate(
            flops=4 * far.size, bytes_accessed=10 * far.size, transcendentals=0
        ),
        name="last_rows",
    )(*in_vmem(early, far, middle_only))


def chip_pairs(pairs):
    return [(2 * a + core, 2 * b + core) for a, b in pairs for core in range(2)]


def line_body(tokens, norm_gain, qkv_weight, out_weight, modality, doc_lengths):
    seq_count = lax.axis_size("seq")
    mod_count = lax.axis_size("mod")
    chips = seq_count // 2
    seq = lax.axis_index("seq")
    qkv_weight = pltpu.with_memory_space_constraint(qkv_weight, pltpu.HBM)
    out_weight = pltpu.with_memory_space_constraint(out_weight, pltpu.HBM)

    def along(value, pairs):
        return lax.ppermute(value, "seq", chip_pairs(pairs))

    def swap(value):
        return lax.ppermute(value, "seq", [(i, i ^ 1) for i in range(seq_count)])

    def exchange(pieces):
        moved = [pieces[0]]
        for d in range(1, mod_count):
            moved.append(lax.ppermute(pieces[d], "mod", [(i, i ^ d) for i in range(mod_count)]))
        return moved

    in_hbm = [
        pltpu.with_memory_space_constraint(value, pltpu.HBM)
        for value in (modality, doc_lengths, tokens, norm_gain)
    ]
    normed, info = norm_rows(*in_hbm, chips)
    docs = doc_lengths.shape[0]
    two = along(normed, [(i, i ^ 2) for i in range(chips)])
    one = along(normed, [(i, i ^ 1) for i in range(chips)])
    inner = along(normed, [(1, 2), (2, 1)])
    relayed = along(two, [(i, i ^ 1) for i in range(chips)])
    own_pair = (normed, swap(normed))
    two_pair = (two, swap(two))
    one_pair = (one, swap(one))
    inner_pair = (inner, swap(inner))
    relayed_pair = (relayed, swap(relayed))
    turn_a, turn_b, turn_c, turn_d = (3, 1), (2, 3), (1, 2), (0, 0)

    *own, late_weight = project_slots(
        info, [own_pair], qkv_weight, (0,), ahead=((3, 2),)
    )
    own = exchange(own)
    two_weight, one_weight = fetch_weights(info, qkv_weight, ((2, 2), (1, 1)))
    mid = project_slots(
        info, [two_pair, one_pair], qkv_weight, (2, 1), ready=(two_weight, one_weight)
    )
    mid = exchange(mid)
    late = project_late(inner_pair, relayed_pair, late_weight, 3 * HDIM, chips)
    late = exchange(late)
    sets = (((0,), own), ((2, 1), mid), ((3,), late))

    def finish(pieces, kept, index, turns):
        own_share, partner_share = output_rows(pieces, kept, index, turns)
        return own_share, swap(partner_share)

    *first, kept_a, kept_b = attend_slots(
        info,
        docs,
        sets,
        (turn_a, turn_b),
        chips,
        Prefetch(out_weight, (turn_a, turn_b), chips),
    )
    first = exchange(first)
    *rest_c, kept_c = attend_slots(
        info, docs, sets, (turn_c,), chips, Prefetch(out_weight, (turn_c,), chips)
    )
    sum_a = add_rows(*finish(first, kept_a, 0, 2))
    own_b, partner_b = finish(first, kept_b, 1, 2)
    from_one = along(sum_a, [(i, i ^ 1) for i in range(chips)])
    sum_b = add_rows(own_b, partner_b)
    from_inner = along(sum_b, [(1, 2), (2, 1)])
    rest_c = exchange(rest_c)
    shares_c = finish(rest_c, kept_c, 0, 1)
    chip = seq // 2
    middle = (chip > 0) & (chip < chips - 1)
    sum_c, relay_sum = relay_rows(chips, *shares_c, from_one, sum_b)
    from_two = along(relay_sum, [(i, i ^ 2) for i in range(chips)])
    from_end = along(sum_c, [(i, i ^ 1) for i in range(chips)])
    *rest_d, kept_d = attend_slots(
        info, docs, sets, (turn_d,), chips, Prefetch(out_weight, (turn_d,), chips)
    )
    rest_d = exchange(rest_d)
    shares_d = finish(rest_d, kept_d, 0, 1)
    near = jnp.where(middle, from_inner, from_one)
    early = tokens.astype(jnp.float32)
    for share in (*shares_d, near):
        early = early + share.astype(jnp.float32)
    return last_rows(chips, early, from_two, from_end)


def solution(mesh):
    fits = mesh.shape["seq"] == 8 and mesh.shape["mod"] == 4

    def body(tokens, norm_gain, qkv_weight, out_weight, modality, doc_lengths):
        whole = tokens.shape[0] * 2 == BLOCK and qkv_weight.shape[2] == 12 * HDIM
        chosen = line_body if fits and whole else general_body
        return chosen(tokens, norm_gain, qkv_weight, out_weight, modality, doc_lengths)

    return jax.shard_map(
        body,
        mesh=mesh,
        in_specs=(
            P(("mod", "seq"), None),
            P(),
            P(None, None, "seq"),
            P(None, "seq", None),
            P(),
            P(),
        ),
        out_specs=P(("mod", "seq"), None),
        check_vma=False,
    )
```

```python
import math

import jax
import jax.numpy as jnp
from jax import lax
from jax.experimental import pallas as pl
from jax.experimental.pallas import tpu as pltpu
from jax.sharding import PartitionSpec as P


HDIM = 128
BLOCK = 128


def modes_of_rows(first_row, row_count, modality):
    block_ids = (first_row + jnp.arange(row_count, dtype=jnp.int32)) // BLOCK
    block_table = jnp.arange(modality.shape[0], dtype=jnp.int32)
    picked = jnp.where(block_ids[:, None] == block_table[None, :], modality[None, :], 0)
    return jnp.sum(picked, axis=1)


def documents(positions, doc_lengths):
    doc_ends = jnp.cumsum(doc_lengths)
    return jnp.sum((positions[:, None] >= doc_ends[None, :]).astype(jnp.int32), axis=1)


def general_body(tokens, norm_gain, qkv_weight, out_weight, modality, doc_lengths):
    row_count = tokens.shape[0]
    seq_count = lax.axis_size("seq")
    mod_count = lax.axis_size("mod")
    group_rows = row_count * seq_count
    mod_index = lax.axis_index("mod")
    own_first = (mod_index * seq_count + lax.axis_index("seq")) * row_count
    row_modes = modes_of_rows(own_first, row_count, modality)
    choose = (
        row_modes[:, None, None] == jnp.arange(norm_gain.shape[0], dtype=jnp.int32)[None, :, None]
    )
    gain_rows = jnp.sum(jnp.where(choose, norm_gain[None, :, :], 0.0), axis=1)
    values = tokens.astype(jnp.float32)
    mean_square = jnp.mean(values * values, axis=1, keepdims=True)
    normed = (values * lax.rsqrt(mean_square + 1e-05) * gain_rows).astype(jnp.bfloat16)
    gathered = lax.all_gather(normed, "seq", axis=0, tiled=True)
    group_first = mod_index * group_rows
    block_count = group_rows // BLOCK
    block_modes = lax.dynamic_slice_in_dim(modality, group_first // BLOCK, block_count)
    heads_here = qkv_weight.shape[2] // (3 * HDIM)

    def project(block_pair):
        row_block, block_mode = block_pair
        weight = lax.dynamic_index_in_dim(qkv_weight, block_mode, 0, keepdims=False)
        return jnp.dot(row_block, weight, preferred_element_type=jnp.float32).astype(jnp.bfloat16)

    projected = lax.map(
        project, (gathered.reshape(block_count, BLOCK, gathered.shape[1]), block_modes)
    )
    projected = projected.reshape(group_rows, heads_here, 3, HDIM)
    queries = projected[:, :, 0, :]
    keys_here = projected[:, :, 1, :]
    values_here = projected[:, :, 2, :]
    quarter = group_rows // mod_count
    local_rows = jnp.arange(group_rows, dtype=jnp.int32)
    query_pos = group_first + local_rows
    query_docs = documents(query_pos, doc_lengths)
    block_size = min(512, quarter)
    block_total = group_rows // block_size
    score_scale = 1.0 / math.sqrt(HDIM)
    query_blocks = queries.reshape(block_total, block_size, heads_here, HDIM)
    pos_blocks = query_pos.reshape(block_total, block_size)
    doc_blocks = query_docs.reshape(block_total, block_size)
    piece_keys = lax.all_gather(keys_here, "mod", axis=0, tiled=True)
    piece_values = lax.all_gather(values_here, "mod", axis=0, tiled=True)
    key_pos = jnp.arange(piece_keys.shape[0], dtype=jnp.int32)
    key_docs = documents(key_pos, doc_lengths)

    def one_block(block_state):
        query_block, block_pos, block_docs = block_state
        scores = (
            jnp.einsum("qhc,khc->hqk", query_block, piece_keys, preferred_element_type=jnp.float32)
            * score_scale
        )
        allowed = (
            (key_pos[None, :] <= block_pos[:, None]) & (key_docs[None, :] == block_docs[:, None])
        )[None, :, :]
        row_max = jnp.max(jnp.where(allowed, scores, -1e30), axis=2)
        weights = jnp.where(allowed, jnp.exp(scores - row_max[:, :, None]), 0.0)
        totals = jnp.sum(weights, axis=2)
        rows = jnp.einsum(
            "hqk,khc->qhc",
            weights.astype(jnp.bfloat16),
            piece_values,
            preferred_element_type=jnp.float32,
        )
        return (rows / jnp.transpose(totals)[:, :, None]).astype(jnp.bfloat16)

    attended = lax.map(one_block, (query_blocks, pos_blocks, doc_blocks))
    attended = attended.reshape(group_rows, heads_here * HDIM)

    def output(block_pair):
        row_block, block_mode = block_pair
        weight = lax.dynamic_index_in_dim(out_weight, block_mode, 0, keepdims=False)
        return jnp.dot(row_block, weight, preferred_element_type=jnp.float32)

    partial_value = lax.map(
        output, (attended.reshape(block_count, BLOCK, attended.shape[1]), block_modes)
    )
    head_sums = lax.psum_scatter(
        partial_value.reshape(group_rows, partial_value.shape[2]).astype(jnp.bfloat16),
        "seq",
        scatter_dimension=0,
        tiled=True,
    ).astype(jnp.float32)
    return (tokens.astype(jnp.float32) + head_sums).astype(jnp.bfloat16)


SMEM = pl.BlockSpec(memory_space=pltpu.SMEM)
VMEM = pl.BlockSpec(memory_space=pltpu.VMEM)
HBM = pl.BlockSpec(memory_space=pltpu.HBM)
PIECES = 4


def mesh_place():
    seq = lax.axis_index("seq")
    return lax.axis_index("mod"), seq // 2, seq % 2


def is_middle(chips):
    chip = mesh_place()[1]
    return (chip > 0) & (chip < chips - 1)


def mode_of(info, slot):
    return info[slot]


def params(mib):
    return pltpu.CompilerParams(vmem_limit_bytes=mib << 20)


def norm_rows(modality, doc_lengths, tokens, norm_gain, chips):
    rows, width = tokens.shape
    modes = norm_gain.shape[0]
    step = 16
    parts = 4
    part = rows // parts
    docs = doc_lengths.shape[0]

    def kernel(modality_ref, docs_ref, tokens_ref, gain_ref, out_ref, info_ref, *scratch):
        rows_ref, gains_ref, table_ref, lengths_ref, row_sems, sems = scratch
        table_copy = pltpu.make_async_copy(modality_ref, table_ref, sems.at[0])
        table_copy.start()
        lengths_copy = pltpu.make_async_copy(docs_ref, lengths_ref, sems.at[2])
        lengths_copy.start()
        gain_copy = pltpu.make_async_copy(gain_ref, gains_ref, sems.at[1])
        gain_copy.start()
        row_copies = [
            pltpu.make_async_copy(
                tokens_ref.at[pl.ds(i * part, part)],
                rows_ref.at[pl.ds(i * part, part)],
                row_sems.at[i],
            )
            for i in range(parts)
        ]
        for copy in row_copies:
            copy.start()
        table_copy.wait()
        lengths_copy.wait()
        mu, chip, _ = mesh_place()
        for slot in range(chips):
            info_ref[slot] = table_ref[mu * chips + jnp.bitwise_xor(chip, slot)]
        end = jnp.int32(0)
        for i in range(docs):
            end = end + lengths_ref[i]
            info_ref[chips + i] = end
        mode = table_ref[mu * chips + chip]
        gain_copy.wait()
        gain = gains_ref[pl.ds(mode, 1), :]
        for i in range(parts):
            row_copies[i].wait()
            for first in range(i * part, (i + 1) * part, step):
                values = rows_ref[first : first + step, :].astype(jnp.float32)
                mean_square = jnp.sum(values * values, axis=1, keepdims=True) * (1.0 / width)
                scaled = values * lax.rsqrt(mean_square + 1e-05) * gain
                out_ref[first : first + step, :] = scaled.astype(jnp.bfloat16)

    return pl.pallas_call(
        kernel,
        out_shape=[
            pltpu.VMEM((rows, width), jnp.bfloat16),
            jax.ShapeDtypeStruct((chips + docs,), jnp.int32),
        ],
        in_specs=[HBM] * 4,
        out_specs=[VMEM, SMEM],
        scratch_shapes=[
            pltpu.VMEM((rows, width), jnp.bfloat16),
            pltpu.VMEM((modes, width), jnp.float32),
            pltpu.SMEM(modality.shape, jnp.int32),
            pltpu.SMEM(doc_lengths.shape, jnp.int32),
            pltpu.SemaphoreType.DMA((parts,)),
            pltpu.SemaphoreType.DMA((3,)),
        ],
        compiler_params=params(8),
        cost_estimate=pl.CostEstimate(flops=4_000_000, bytes_accessed=1 << 20, transcendentals=64),
        name="norm_rows",
    )(modality, doc_lengths, tokens, norm_gain)


def weight_copies(info_ref, weight_ref, buffer_ref, sems, slot, pair, at):
    pieces, piece, pair_cols = buffer_ref.shape[1:]
    first = jnp.bitwise_xor(mesh_place()[0] // 2, pair) * pair_cols
    return [
        pltpu.make_async_copy(
            weight_ref.at[
                mode_of(info_ref, slot),
                pl.ds(k * piece, piece),
                pl.ds(pl.multiple_of(first, 128), pair_cols),
            ],
            buffer_ref.at[at, k],
            sems.at[at, k],
        )
        for k in range(pieces)
    ]


def weight_shape(weight, pairs):
    width, cols = weight.shape[1:]
    return (pairs, PIECES, width // PIECES, cols // 2)


def fetch_weights(info, weight, ahead):
    shapes = [weight_shape(weight, n_pairs) for _, n_pairs in ahead]
    count = len(ahead)

    def kernel(info_ref, weight_ref, *refs):
        copies = [
            copy
            for i, (slot, n_pairs) in enumerate(ahead)
            for p in range(n_pairs)
            for copy in weight_copies(
                info_ref, weight_ref, refs[i], refs[count + i], slot, p, p
            )
        ]
        for copy in copies:
            copy.start()
        for copy in copies:
            copy.wait()

    return pl.pallas_call(
        kernel,
        out_shape=[pltpu.VMEM(shape, jnp.bfloat16) for shape in shapes],
        in_specs=[SMEM, HBM],
        out_specs=[VMEM] * count,
        scratch_shapes=[pltpu.SemaphoreType.DMA(shape[:2]) for shape in shapes],
        compiler_params=params(1),
        cost_estimate=pl.CostEstimate(
            flops=6_000_000_000, bytes_accessed=25 << 20, transcendentals=0
        ),
        name="fetch_weights",
    )(info, weight)


class Prefetch:
    def __init__(self, out_weight, slots):
        self.weight, self.slots = out_weight, slots
        self.shapes = [pltpu.VMEM(out_weight.shape[1:], jnp.bfloat16)] * len(slots)
        self.scratch = pltpu.SemaphoreType.DMA((len(slots),))

    def copies(self, info_ref, weight_ref, kept_refs, sems):
        return [
            pltpu.make_async_copy(weight_ref.at[mode_of(info_ref, slot)], kept_refs[i], sems.at[i])
            for i, slot in enumerate(self.slots)
        ]

    def start(self, *refs):
        for copy in self.copies(*refs):
            copy.start()

    def wait(self, *refs):
        for copy in self.copies(*refs):
            copy.wait()


def store_pair(outs, rows, p, result):
    result = result.astype(jnp.bfloat16)
    cols = result.shape[1] // 2
    odd = mesh_place()[0] % 2 == 1
    for e in range(2):
        first, last = result[:, e * cols : (e + 1) * cols], result[:, (1 - e) * cols : (2 - e) * cols]
        outs[2 * p + e][rows, :] = jnp.where(odd, last, first)


def project_slots(info, parts, weight, slots, ready=(), ahead=()):
    half, width = parts[0][0].shape
    block = 2 * half
    cols = 3 * HDIM
    heads = weight.shape[2] // cols
    pairs = 2
    count, given = len(slots), len(ready)
    steps = [(n, p) for n in range(count) for p in range(pairs)]
    places = [(i, j) for i, array in enumerate(ready) for j in range(array.shape[0])]
    streamed = steps[len(places) :]
    shape = weight_shape(weight, len(streamed))
    ahead_shapes = [weight_shape(weight, n_pairs) for _, n_pairs in ahead]

    def kernel(info_ref, *refs):
        ins, refs = refs[: 2 * count], refs[2 * count :]
        ready_refs, weight_ref, refs = refs[:given], refs[given], refs[given + 1 :]
        outs, refs = refs[:heads], refs[heads:]
        ahead_refs, refs = refs[: len(ahead)], refs[len(ahead) :]
        rows_ref, buffer_ref, sems, ahead_sems = refs[0], refs[1], refs[2], refs[3:]
        fetched = {
            step: weight_copies(info_ref, weight_ref, buffer_ref, sems, slots[step[0]], step[1], i)
            for i, step in enumerate(streamed)
        }
        later = [
            copy
            for i, (slot, n_pairs) in enumerate(ahead)
            for p in range(n_pairs)
            for copy in weight_copies(
                info_ref, weight_ref, ahead_refs[i], ahead_sems[i], slot, p, p
            )
        ]
        for copy in [copy for copies in fetched.values() for copy in copies] + later:
            copy.start()

        @pl.when(mesh_place()[1] >= 0)
        def _():
            for n in range(count):
                rows_ref[n, :half, :] = ins[2 * n][...]
                rows_ref[n, half:, :] = ins[2 * n + 1][...]
            for i, (n, p) in enumerate(steps):
                result = None
                piece = width // PIECES
                for k in range(PIECES):
                    if (n, p) in fetched:
                        fetched[n, p][k].wait()
                        part_ref, at = buffer_ref, streamed.index((n, p))
                    else:
                        part_ref, at = ready_refs[places[i][0]], places[i][1]
                    rows = rows_ref[n, :, k * piece : (k + 1) * piece]
                    part = jnp.dot(rows, part_ref[at, k], preferred_element_type=jnp.float32)
                    result = part if result is None else result + part
                store_pair(outs, pl.ds(n * block, block), p, result)

        for copy in later:
            copy.wait()

    return pl.pallas_call(
        kernel,
        out_shape=[pltpu.VMEM((count * block, cols), jnp.bfloat16)] * heads
        + [pltpu.VMEM(ahead_shape, jnp.bfloat16) for ahead_shape in ahead_shapes],
        in_specs=[SMEM] + [VMEM] * (2 * count + given) + [HBM],
        out_specs=[VMEM] * (heads + len(ahead)),
        scratch_shapes=[
            pltpu.VMEM((count, block, width), jnp.bfloat16),
            pltpu.VMEM(shape, jnp.bfloat16),
            pltpu.SemaphoreType.DMA(shape[:2]),
        ]
        + [pltpu.SemaphoreType.DMA(ahead_shape[:2]) for ahead_shape in ahead_shapes],
        compiler_params=params(6 + 6 * len(streamed)),
        cost_estimate=pl.CostEstimate(
            flops=2 * count * block * width * cols * heads,
            bytes_accessed=count * width * cols * heads * 2,
            transcendentals=0,
        ),
        name="project_slots",
    )(info, *[piece for pair in parts for piece in pair], *ready, weight)


def project_late(inner, relayed, weight, cols, chips):
    half, width = inner[0].shape
    block = 2 * half
    pairs, pieces, piece, pair_cols = weight.shape
    heads = pairs * pair_cols // cols

    def kernel(inner_own, inner_partner, relayed_own, relayed_partner, weight_ref, *refs):
        outs, rows_ref = refs[:heads], refs[heads]
        middle = is_middle(chips)

        @pl.when(middle)
        def _():
            rows_ref[:half, :] = inner_own[...]
            rows_ref[half:, :] = inner_partner[...]

        @pl.when(jnp.logical_not(middle))
        def _():
            rows_ref[:half, :] = relayed_own[...]
            rows_ref[half:, :] = relayed_partner[...]

        for p in range(pairs):
            result = None
            for k in range(pieces):
                part = jnp.dot(
                    rows_ref[:, k * piece : (k + 1) * piece],
                    weight_ref[p, k],
                    preferred_element_type=jnp.float32,
                )
                result = part if result is None else result + part
            store_pair(outs, pl.ds(0, block), p, result)

    return pl.pallas_call(
        kernel,
        out_shape=[pltpu.VMEM((block, cols), jnp.bfloat16)] * heads,
        in_specs=[VMEM] * 5,
        out_specs=[VMEM] * heads,
        scratch_shapes=[pltpu.VMEM((block, width), jnp.bfloat16)],
        compiler_params=params(8),
        cost_estimate=pl.CostEstimate(
            flops=2 * block * width * cols * heads,
            bytes_accessed=width * cols * heads * 2,
            transcendentals=0,
        ),
        name="project_late",
    )(*inner, *relayed, weight)


def attend_slots(info, docs, sets, query_slots, chips, prefetch):
    count = len(sets[0][1])
    block = sets[0][1][0].shape[0] // len(sets[0][0])
    total = count * chips * block
    window = min(total // 2 + block, total)
    scale = 1.0 / math.sqrt(HDIM)

    kept = len(prefetch.slots)

    def kernel(info_ref, *refs):
        ins, refs = refs[: len(sets) * count], refs[len(sets) * count :]
        next_ref, outs, kept_refs = refs[0], refs[1 : 1 + count], refs[1 + count : 1 + count + kept]
        keys_ref, values_ref, sems = refs[1 + count + kept :]
        prefetch.start(info_ref, next_ref, kept_refs, sems)

        @pl.when(mesh_place()[1] >= 0)
        def _():
            mu, chip, core = mesh_place()
            own_first = core * (block // 2)

            def slot_rows(d, slot, part):
                for i, (slots, _) in enumerate(sets):
                    if slot in slots:
                        at = slots.index(slot) * block
                        return ins[i * count + d][at : at + block, part * HDIM : (part + 1) * HDIM]

            for d in range(count):
                for slot in range(chips):
                    index = jnp.bitwise_xor(mu, d) * chips + jnp.bitwise_xor(chip, slot)
                    place = pl.ds(pl.multiple_of(index * block, block), block)
                    keys_ref[place, :] = slot_rows(d, slot, 1)
                    values_ref[place, :] = slot_rows(d, slot, 2)

            ends = [info_ref[chips + i] for i in range(docs)]
            row_place = lax.broadcasted_iota(jnp.int32, (block, 1), 0) + own_first
            row_place = jnp.where(row_place >= block, row_place - block, row_place)
            key_iota = lax.broadcasted_iota(jnp.int32, (1, window), 1)
            key_in_block = key_iota % block + own_first
            key_in_block = jnp.where(key_in_block >= block, key_in_block - block, key_in_block)
            key_place = (key_iota // block) * block + key_in_block
            for n, slot in enumerate(query_slots):
                for d in range(count):
                    index = jnp.bitwise_xor(mu, d) * chips + jnp.bitwise_xor(chip, slot)
                    first_row = index * block
                    doc_first = jnp.int32(0)
                    for e in ends:
                        doc_first = jnp.where(first_row >= e, e, doc_first)
                    start = jnp.minimum(doc_first // block, (total - window) // block) * block
                    start = pl.multiple_of(start, block)
                    row_pos = row_place + first_row
                    row_first = jnp.zeros((block, 1), jnp.int32)
                    for e in ends:
                        row_first = jnp.where(row_pos >= e, e, row_first)
                    key_pos = key_place + start
                    allowed = (key_pos <= row_pos) & (key_pos >= row_first)
                    scores = lax.dot_general(
                        slot_rows(d, slot, 0),
                        keys_ref[pl.ds(start, window), :],
                        (((1,), (1,)), ((), ())),
                        preferred_element_type=jnp.float32,
                    )
                    scores = jnp.where(allowed, scores * scale, -1e30)
                    row_max = jnp.max(scores, axis=1, keepdims=True)
                    weights = jnp.where(allowed, jnp.exp(scores - row_max), 0.0)
                    totals = jnp.sum(weights, axis=1, keepdims=True)
                    summed = jnp.dot(
                        weights.astype(jnp.bfloat16),
                        values_ref[pl.ds(start, window), :],
                        preferred_element_type=jnp.float32,
                    )
                    outs[d][n * block : (n + 1) * block, :] = (summed / totals).astype(jnp.bfloat16)

        prefetch.wait(info_ref, next_ref, kept_refs, sems)

    n_queries = len(query_slots) * count
    return pl.pallas_call(
        kernel,
        out_shape=[pltpu.VMEM((len(query_slots) * block, HDIM), jnp.bfloat16)] * count
        + prefetch.shapes,
        in_specs=[SMEM] + [VMEM] * (len(sets) * count) + [HBM],
        out_specs=[VMEM] * (count + kept),
        scratch_shapes=[
            pltpu.VMEM((total, HDIM), jnp.bfloat16),
            pltpu.VMEM((total, HDIM), jnp.bfloat16),
            prefetch.scratch,
        ],
        compiler_params=params(14),
        cost_estimate=pl.CostEstimate(
            flops=n_queries * block * window * HDIM * 8,
            bytes_accessed=3 * total * HDIM * 2,
            transcendentals=n_queries * block * window,
        ),
        name="attend_slots",
    )(info, *[piece for _, pieces in sets for piece in pieces], prefetch.weight)


def output_rows(pieces, weight):
    count = len(pieces)
    block = pieces[0].shape[0]
    half = block // 2
    depth, width = weight.shape
    tile = min(1024, width)

    def kernel(*refs):
        ins = refs[:count]
        weight_ref, own_ref, partner_ref, heads_ref = refs[count:]
        for d in range(count):
            heads_ref[jnp.bitwise_xor(mesh_place()[0], d)] = ins[d][...]
        rows = jnp.concatenate([heads_ref[h] for h in range(count)], axis=1)
        for first in range(0, width, tile):
            cols = slice(first, first + tile)
            result = jnp.dot(rows, weight_ref[:, cols], preferred_element_type=jnp.float32)
            result = result.astype(jnp.bfloat16)
            own_ref[:, cols] = result[:half]
            partner_ref[:, cols] = result[half:]

    return pl.pallas_call(
        kernel,
        out_shape=[pltpu.VMEM((half, width), jnp.bfloat16)] * 2,
        in_specs= [VMEM] * (count + 1),
        out_specs=[VMEM] * 2,
        scratch_shapes=[pltpu.VMEM((count, block, HDIM), jnp.bfloat16)],
        compiler_params=params(8),
        cost_estimate=pl.CostEstimate(
            flops=2 * block * depth * width,
            bytes_accessed=depth * width * 2,
            transcendentals=0,
        ),
        name="output_rows",
    )(*pieces, weight)


def in_vmem(*values):
    return [pltpu.with_memory_space_constraint(value, pltpu.VMEM) for value in values]


def add_rows(first, second):
    def kernel(first_ref, second_ref, out_ref):
        total = first_ref[...].astype(jnp.float32) + second_ref[...].astype(jnp.float32)
        out_ref[...] = total.astype(jnp.bfloat16)

    return pl.pallas_call(
        kernel,
        out_shape=pltpu.VMEM(first.shape, jnp.bfloat16),
        in_specs=[VMEM, VMEM],
        out_specs=VMEM,
        compiler_params=params(4),
        cost_estimate=pl.CostEstimate(
            flops=4 * first.size, bytes_accessed=6 * first.size, transcendentals=0
        ),
        name="add_rows",
    )(*in_vmem(first, second))


def relay_rows(chips, own, partner, passing):
    def kernel(own_ref, partner_ref, passing_ref, out_ref):
        middle = is_middle(chips)

        @pl.when(middle)
        def _():
            total = own_ref[...].astype(jnp.float32) + partner_ref[...].astype(jnp.float32)
            total = total + passing_ref[...].astype(jnp.float32)
            out_ref[...] = total.astype(jnp.bfloat16)

        @pl.when(jnp.logical_not(middle))
        def _():
            total = own_ref[...].astype(jnp.float32) + partner_ref[...].astype(jnp.float32)
            out_ref[...] = total.astype(jnp.bfloat16)

    return pl.pallas_call(
        kernel,
        out_shape=pltpu.VMEM(own.shape, jnp.bfloat16),
        in_specs=[VMEM] * 3,
        out_specs=VMEM,
        compiler_params=params(4),
        cost_estimate=pl.CostEstimate(
            flops=4 * own.size, bytes_accessed=8 * own.size, transcendentals=0
        ),
        name="relay_rows",
    )(*in_vmem(own, partner, passing))


def last_rows(early, first, second):
    rows, width = first.shape
    parts = 4
    part = rows // parts

    def kernel(early_ref, first_ref, second_ref, out_ref, done_ref, sems):
        copies = []
        for i in range(parts):
            at = pl.ds(i * part, part)
            total = early_ref[at] + first_ref[at].astype(jnp.float32)
            total = total + second_ref[at].astype(jnp.float32)
            done_ref[at] = total.astype(jnp.bfloat16)
            copies.append(pltpu.make_async_copy(done_ref.at[at], out_ref.at[at], sems.at[i]))
            copies[i].start()
        for copy in copies:
            copy.wait()

    return pl.pallas_call(
        kernel,
        out_shape=pltpu.HBM(first.shape, jnp.bfloat16),
        in_specs=[VMEM] * 3,
        out_specs=HBM,
        scratch_shapes=[
            pltpu.VMEM((rows, width), jnp.bfloat16),
            pltpu.SemaphoreType.DMA((parts,)),
        ],
        compiler_params=params(6),
        cost_estimate=pl.CostEstimate(
            flops=4 * first.size, bytes_accessed=10 * first.size, transcendentals=0
        ),
        name="last_rows",
    )(*in_vmem(early, first, second))


def chip_pairs(pairs):
    return [(2 * a + core, 2 * b + core) for a, b in pairs for core in range(2)]


def line_body(tokens, norm_gain, qkv_weight, out_weight, modality, doc_lengths):
    seq_count = lax.axis_size("seq")
    mod_count = lax.axis_size("mod")
    chips = seq_count // 2
    qkv_weight = pltpu.with_memory_space_constraint(qkv_weight, pltpu.HBM)
    out_weight = pltpu.with_memory_space_constraint(out_weight, pltpu.HBM)

    def along(value, pairs):
        return lax.ppermute(value, "seq", chip_pairs(pairs))

    def swap(value):
        return lax.ppermute(value, "seq", [(i, i ^ 1) for i in range(seq_count)])

    def exchange(pieces):
        moved = [pieces[0]]
        for d in range(1, mod_count):
            moved.append(lax.ppermute(pieces[d], "mod", [(i, i ^ d) for i in range(mod_count)]))
        return moved

    in_hbm = [
        pltpu.with_memory_space_constraint(value, pltpu.HBM)
        for value in (modality, doc_lengths, tokens, norm_gain)
    ]
    normed, info = norm_rows(*in_hbm, chips)
    docs = doc_lengths.shape[0]
    two = along(normed, [(i, i ^ 2) for i in range(chips)])
    one = along(normed, [(i, i ^ 1) for i in range(chips)])
    inner = along(normed, [(1, 2), (2, 1)])
    relayed = along(two, [(i, i ^ 1) for i in range(chips)])
    own_pair = (normed, swap(normed))
    two_pair = (two, swap(two))
    one_pair = (one, swap(one))
    inner_pair = (inner, swap(inner))
    relayed_pair = (relayed, swap(relayed))

    *own, late_weight = project_slots(
        info, [own_pair], qkv_weight, (0,), ahead=((3, 2),)
    )
    own = exchange(own)
    two_weight, one_weight = fetch_weights(info, qkv_weight, ((2, 2), (1, 1)))
    mid = project_slots(
        info, [two_pair, one_pair], qkv_weight, (2, 1), ready=(two_weight, one_weight)
    )
    mid = exchange(mid)
    late = project_late(inner_pair, relayed_pair, late_weight, 3 * HDIM, chips)
    late = exchange(late)
    sets = (((0,), own), ((2, 1), mid), ((3,), late))

    def attend(slot):
        *rows, kept = attend_slots(info, docs, sets, (slot,), chips, Prefetch(out_weight, (slot,)))
        return exchange(rows), kept

    def finish(pieces, kept):
        own_share, partner_share = output_rows(pieces, kept)
        return own_share, swap(partner_share)

    sum_a = add_rows(*finish(*attend(3)))
    from_one = along(sum_a, [(i, i ^ 1) for i in range(chips)])
    from_inner = along(sum_a, [(1, 2), (2, 1)])
    sum_b = relay_rows(chips, *finish(*attend(2)), from_one)
    from_two = along(sum_b, [(i, i ^ 2) for i in range(chips)])
    sum_c = add_rows(*finish(*attend(1)))
    from_end = along(sum_c, [(i, i ^ 1) for i in range(chips)])
    early = tokens.astype(jnp.float32)
    for share in (*finish(*attend(0)), from_inner):
        early = early + share.astype(jnp.float32)
    return last_rows(early, from_two, from_end)


def solution(mesh):
    fits = mesh.shape["seq"] == 8 and mesh.shape["mod"] == 4

    def body(tokens, norm_gain, qkv_weight, out_weight, modality, doc_lengths):
        whole = tokens.shape[0] * 2 == BLOCK and qkv_weight.shape[2] == 12 * HDIM
        chosen = line_body if fits and whole else general_body
        return chosen(tokens, norm_gain, qkv_weight, out_weight, modality, doc_lengths)

    return jax.shard_map(
        body,
        mesh=mesh,
        in_specs=(
            P(("mod", "seq"), None),
            P(),
            P(None, None, "seq"),
            P(None, "seq", None),
            P(),
            P(),
        ),
        out_specs=P(("mod", "seq"), None),
        check_vma=False,
    )
```

```python
import math

import jax
import jax.numpy as jnp
from jax import lax
from jax.experimental import pallas as pl
from jax.experimental.pallas import tpu as pltpu
from jax.sharding import PartitionSpec as P


HDIM = 128
BLOCK = 128


def modes_of_rows(first_row, row_count, modality):
    block_ids = (first_row + jnp.arange(row_count, dtype=jnp.int32)) // BLOCK
    block_table = jnp.arange(modality.shape[0], dtype=jnp.int32)
    picked = jnp.where(block_ids[:, None] == block_table[None, :], modality[None, :], 0)
    return jnp.sum(picked, axis=1)


def documents(positions, doc_lengths):
    doc_ends = jnp.cumsum(doc_lengths)
    return jnp.sum((positions[:, None] >= doc_ends[None, :]).astype(jnp.int32), axis=1)


def general_body(tokens, norm_gain, qkv_weight, out_weight, modality, doc_lengths):
    row_count = tokens.shape[0]
    seq_count = lax.axis_size("seq")
    mod_count = lax.axis_size("mod")
    group_rows = row_count * seq_count
    mod_index = lax.axis_index("mod")
    own_first = (mod_index * seq_count + lax.axis_index("seq")) * row_count
    row_modes = modes_of_rows(own_first, row_count, modality)
    choose = (
        row_modes[:, None, None] == jnp.arange(norm_gain.shape[0], dtype=jnp.int32)[None, :, None]
    )
    gain_rows = jnp.sum(jnp.where(choose, norm_gain[None, :, :], 0.0), axis=1)
    values = tokens.astype(jnp.float32)
    mean_square = jnp.mean(values * values, axis=1, keepdims=True)
    normed = (values * lax.rsqrt(mean_square + 1e-05) * gain_rows).astype(jnp.bfloat16)
    gathered = lax.all_gather(normed, "seq", axis=0, tiled=True)
    group_first = mod_index * group_rows
    block_count = group_rows // BLOCK
    block_modes = lax.dynamic_slice_in_dim(modality, group_first // BLOCK, block_count)
    heads_here = qkv_weight.shape[2] // (3 * HDIM)

    def project(block_pair):
        row_block, block_mode = block_pair
        weight = lax.dynamic_index_in_dim(qkv_weight, block_mode, 0, keepdims=False)
        return jnp.dot(row_block, weight, preferred_element_type=jnp.float32).astype(jnp.bfloat16)

    projected = lax.map(
        project, (gathered.reshape(block_count, BLOCK, gathered.shape[1]), block_modes)
    )
    projected = projected.reshape(group_rows, heads_here, 3, HDIM)
    queries = projected[:, :, 0, :]
    keys_here = projected[:, :, 1, :]
    values_here = projected[:, :, 2, :]
    quarter = group_rows // mod_count
    local_rows = jnp.arange(group_rows, dtype=jnp.int32)
    query_pos = group_first + local_rows
    query_docs = documents(query_pos, doc_lengths)
    block_size = min(512, quarter)
    block_total = group_rows // block_size
    score_scale = 1.0 / math.sqrt(HDIM)
    query_blocks = queries.reshape(block_total, block_size, heads_here, HDIM)
    pos_blocks = query_pos.reshape(block_total, block_size)
    doc_blocks = query_docs.reshape(block_total, block_size)
    piece_keys = lax.all_gather(keys_here, "mod", axis=0, tiled=True)
    piece_values = lax.all_gather(values_here, "mod", axis=0, tiled=True)
    key_pos = jnp.arange(piece_keys.shape[0], dtype=jnp.int32)
    key_docs = documents(key_pos, doc_lengths)

    def one_block(block_state):
        query_block, block_pos, block_docs = block_state
        scores = (
            jnp.einsum("qhc,khc->hqk", query_block, piece_keys, preferred_element_type=jnp.float32)
            * score_scale
        )
        allowed = (
            (key_pos[None, :] <= block_pos[:, None]) & (key_docs[None, :] == block_docs[:, None])
        )[None, :, :]
        row_max = jnp.max(jnp.where(allowed, scores, -1e30), axis=2)
        weights = jnp.where(allowed, jnp.exp(scores - row_max[:, :, None]), 0.0)
        totals = jnp.sum(weights, axis=2)
        rows = jnp.einsum(
            "hqk,khc->qhc",
            weights.astype(jnp.bfloat16),
            piece_values,
            preferred_element_type=jnp.float32,
        )
        return (rows / jnp.transpose(totals)[:, :, None]).astype(jnp.bfloat16)

    attended = lax.map(one_block, (query_blocks, pos_blocks, doc_blocks))
    attended = attended.reshape(group_rows, heads_here * HDIM)

    def output(block_pair):
        row_block, block_mode = block_pair
        weight = lax.dynamic_index_in_dim(out_weight, block_mode, 0, keepdims=False)
        return jnp.dot(row_block, weight, preferred_element_type=jnp.float32)

    partial_value = lax.map(
        output, (attended.reshape(block_count, BLOCK, attended.shape[1]), block_modes)
    )
    head_sums = lax.psum_scatter(
        partial_value.reshape(group_rows, partial_value.shape[2]).astype(jnp.bfloat16),
        "seq",
        scatter_dimension=0,
        tiled=True,
    ).astype(jnp.float32)
    return (tokens.astype(jnp.float32) + head_sums).astype(jnp.bfloat16)


SMEM = pl.BlockSpec(memory_space=pltpu.SMEM)
VMEM = pl.BlockSpec(memory_space=pltpu.VMEM)
HBM = pl.BlockSpec(memory_space=pltpu.HBM)
PIECES = 4


def mesh_place():
    seq = lax.axis_index("seq")
    return lax.axis_index("mod"), seq // 2, seq % 2


def is_middle(chips):
    chip = mesh_place()[1]
    return (chip > 0) & (chip < chips - 1)


def mode_of(info, slot):
    return info[slot]


def params(mib):
    return pltpu.CompilerParams(vmem_limit_bytes=mib << 20)


def norm_rows(modality, doc_lengths, tokens, norm_gain, chips):
    rows, width = tokens.shape
    modes = norm_gain.shape[0]
    step = 16
    parts = 4
    part = rows // parts
    docs = doc_lengths.shape[0]

    def kernel(modality_ref, docs_ref, tokens_ref, gain_ref, out_ref, info_ref, *scratch):
        rows_ref, gains_ref, table_ref, lengths_ref, row_sems, sems = scratch
        table_copy = pltpu.make_async_copy(modality_ref, table_ref, sems.at[0])
        table_copy.start()
        lengths_copy = pltpu.make_async_copy(docs_ref, lengths_ref, sems.at[2])
        lengths_copy.start()
        gain_copy = pltpu.make_async_copy(gain_ref, gains_ref, sems.at[1])
        gain_copy.start()
        row_copies = [
            pltpu.make_async_copy(
                tokens_ref.at[pl.ds(i * part, part)],
                rows_ref.at[pl.ds(i * part, part)],
                row_sems.at[i],
            )
            for i in range(parts)
        ]
        for copy in row_copies:
            copy.start()
        table_copy.wait()
        lengths_copy.wait()
        mu, chip, _ = mesh_place()
        for slot in range(chips):
            info_ref[slot] = table_ref[mu * chips + jnp.bitwise_xor(chip, slot)]
        end = jnp.int32(0)
        for i in range(docs):
            end = end + lengths_ref[i]
            info_ref[chips + i] = end
        mode = table_ref[mu * chips + chip]
        gain_copy.wait()
        gain = gains_ref[pl.ds(mode, 1), :]
        for i in range(parts):
            row_copies[i].wait()
            for first in range(i * part, (i + 1) * part, step):
                values = rows_ref[first : first + step, :].astype(jnp.float32)
                mean_square = jnp.sum(values * values, axis=1, keepdims=True) * (1.0 / width)
                scaled = values * lax.rsqrt(mean_square + 1e-05) * gain
                out_ref[first : first + step, :] = scaled.astype(jnp.bfloat16)

    return pl.pallas_call(
        kernel,
        out_shape=[
            pltpu.VMEM((rows, width), jnp.bfloat16),
            jax.ShapeDtypeStruct((chips + docs,), jnp.int32),
        ],
        in_specs=[HBM] * 4,
        out_specs=[VMEM, SMEM],
        scratch_shapes=[
            pltpu.VMEM((rows, width), jnp.bfloat16),
            pltpu.VMEM((modes, width), jnp.float32),
            pltpu.SMEM(modality.shape, jnp.int32),
            pltpu.SMEM(doc_lengths.shape, jnp.int32),
            pltpu.SemaphoreType.DMA((parts,)),
            pltpu.SemaphoreType.DMA((3,)),
        ],
        compiler_params=params(8),
        cost_estimate=pl.CostEstimate(flops=4_000_000, bytes_accessed=1 << 20, transcendentals=64),
        name="norm_rows",
    )(modality, doc_lengths, tokens, norm_gain)


def weight_copies(info_ref, weight_ref, buffer_ref, sems, slot, pair, at):
    pieces, piece, pair_cols = buffer_ref.shape[1:]
    first = jnp.bitwise_xor(mesh_place()[0] // 2, pair) * pair_cols
    return [
        pltpu.make_async_copy(
            weight_ref.at[
                mode_of(info_ref, slot),
                pl.ds(k * piece, piece),
                pl.ds(pl.multiple_of(first, 128), pair_cols),
            ],
            buffer_ref.at[at, k],
            sems.at[at, k],
        )
        for k in range(pieces)
    ]


def weight_shape(weight, pairs):
    width, cols = weight.shape[1:]
    return (pairs, PIECES, width // PIECES, cols // 2)


def fetch_weights(info, weight, ahead):
    shapes = [weight_shape(weight, n_pairs) for _, n_pairs, _ in ahead]
    count = len(ahead)

    def kernel(info_ref, weight_ref, *refs):
        copies = [
            copy
            for i, (slot, n_pairs, skip) in enumerate(ahead)
            for p in range(n_pairs)
            for copy in weight_copies(
                info_ref, weight_ref, refs[i], refs[count + i], slot, p + skip, p
            )
        ]
        for copy in copies:
            copy.start()
        for copy in copies:
            copy.wait()

    return pl.pallas_call(
        kernel,
        out_shape=[pltpu.VMEM(shape, jnp.bfloat16) for shape in shapes],
        in_specs=[SMEM, HBM],
        out_specs=[VMEM] * count,
        scratch_shapes=[pltpu.SemaphoreType.DMA(shape[:2]) for shape in shapes],
        compiler_params=params(1),
        cost_estimate=pl.CostEstimate(
            flops=6_000_000_000, bytes_accessed=25 << 20, transcendentals=0
        ),
        name="fetch_weights",
    )(info, weight)


class Prefetch:
    def __init__(self, out_weight, slots):
        self.weight, self.slots = out_weight, slots
        self.shapes = [pltpu.VMEM(out_weight.shape[1:], jnp.bfloat16)] * len(slots)
        self.scratch = pltpu.SemaphoreType.DMA((len(slots),))

    def copies(self, info_ref, weight_ref, kept_refs, sems):
        return [
            pltpu.make_async_copy(weight_ref.at[mode_of(info_ref, slot)], kept_refs[i], sems.at[i])
            for i, slot in enumerate(self.slots)
        ]

    def start(self, *refs):
        for copy in self.copies(*refs):
            copy.start()

    def wait(self, *refs):
        for copy in self.copies(*refs):
            copy.wait()


def store_pair(outs, rows, p, result):
    result = result.astype(jnp.bfloat16)
    cols = result.shape[1] // 2
    odd = mesh_place()[0] % 2 == 1
    for e in range(2):
        first, last = result[:, e * cols : (e + 1) * cols], result[:, (1 - e) * cols : (2 - e) * cols]
        outs[2 * p + e][rows, :] = jnp.where(odd, last, first)


def project_slots(info, parts, weight, slots, ready=(), ahead=()):
    half, width = parts[0][0].shape
    block = 2 * half
    cols = 3 * HDIM
    heads = weight.shape[2] // cols
    pairs = 2
    count, given = len(slots), len(ready)
    steps = [(n, p) for n in range(count) for p in range(pairs)]
    places = [(i, j) for i, array in enumerate(ready) for j in range(array.shape[0])]
    streamed = steps[len(places) :]
    shape = weight_shape(weight, len(streamed))
    ahead_shapes = [weight_shape(weight, n_pairs) for _, n_pairs, _ in ahead]

    def kernel(info_ref, *refs):
        ins, refs = refs[: 2 * count], refs[2 * count :]
        ready_refs, weight_ref, refs = refs[:given], refs[given], refs[given + 1 :]
        outs, refs = refs[:heads], refs[heads:]
        ahead_refs, refs = refs[: len(ahead)], refs[len(ahead) :]
        rows_ref, refs = refs[0], refs[1:]
        buffer_ref, sems = refs[:2] if streamed else (None, None)
        ahead_sems = refs[2:] if streamed else refs
        fetched = {
            step: weight_copies(info_ref, weight_ref, buffer_ref, sems, slots[step[0]], step[1], i)
            for i, step in enumerate(streamed)
        }
        later = [
            copy
            for i, (slot, n_pairs, skip) in enumerate(ahead)
            for p in range(n_pairs)
            for copy in weight_copies(
                info_ref, weight_ref, ahead_refs[i], ahead_sems[i], slot, p + skip, p
            )
        ]
        for copy in [copy for copies in fetched.values() for copy in copies] + later:
            copy.start()

        @pl.when(mesh_place()[1] >= 0)
        def _():
            for n in range(count):
                rows_ref[n, :half, :] = ins[2 * n][...]
                rows_ref[n, half:, :] = ins[2 * n + 1][...]
            for i, (n, p) in enumerate(steps):
                result = None
                piece = width // PIECES
                for k in range(PIECES):
                    if (n, p) in fetched:
                        fetched[n, p][k].wait()
                        part_ref, at = buffer_ref, streamed.index((n, p))
                    else:
                        part_ref, at = ready_refs[places[i][0]], places[i][1]
                    rows = rows_ref[n, :, k * piece : (k + 1) * piece]
                    part = jnp.dot(rows, part_ref[at, k], preferred_element_type=jnp.float32)
                    result = part if result is None else result + part
                store_pair(outs, pl.ds(n * block, block), p, result)

        for copy in later:
            copy.wait()

    return pl.pallas_call(
        kernel,
        out_shape=[pltpu.VMEM((count * block, cols), jnp.bfloat16)] * heads
        + [pltpu.VMEM(ahead_shape, jnp.bfloat16) for ahead_shape in ahead_shapes],
        in_specs=[SMEM] + [VMEM] * (2 * count + given) + [HBM],
        out_specs=[VMEM] * (heads + len(ahead)),
        scratch_shapes=[
            pltpu.VMEM((count, block, width), jnp.bfloat16),
        ]
        + (
            [pltpu.VMEM(shape, jnp.bfloat16), pltpu.SemaphoreType.DMA(shape[:2])]
            if streamed
            else []
        )
        + [pltpu.SemaphoreType.DMA(ahead_shape[:2]) for ahead_shape in ahead_shapes],
        compiler_params=params(6 + 6 * len(streamed)),
        cost_estimate=pl.CostEstimate(
            flops=2 * count * block * width * cols * heads,
            bytes_accessed=count * width * cols * heads * 2,
            transcendentals=0,
        ),
        name="project_slots",
    )(info, *[piece for pair in parts for piece in pair], *ready, weight)


def project_late(inner, relayed, weights, cols, chips):
    half, width = inner[0].shape
    block = 2 * half
    pairs = len(weights)
    pieces, piece, pair_cols = weights[0].shape[1:]
    heads = pairs * pair_cols // cols

    def kernel(inner_own, inner_partner, relayed_own, relayed_partner, *refs):
        weight_refs, refs = refs[:pairs], refs[pairs:]
        outs, rows_ref = refs[:heads], refs[heads]
        middle = is_middle(chips)

        @pl.when(middle)
        def _():
            rows_ref[:half, :] = inner_own[...]
            rows_ref[half:, :] = inner_partner[...]

        @pl.when(jnp.logical_not(middle))
        def _():
            rows_ref[:half, :] = relayed_own[...]
            rows_ref[half:, :] = relayed_partner[...]

        for p in range(pairs):
            result = None
            for k in range(pieces):
                part = jnp.dot(
                    rows_ref[:, k * piece : (k + 1) * piece],
                    weight_refs[p][0, k],
                    preferred_element_type=jnp.float32,
                )
                result = part if result is None else result + part
            store_pair(outs, pl.ds(0, block), p, result)

    return pl.pallas_call(
        kernel,
        out_shape=[pltpu.VMEM((block, cols), jnp.bfloat16)] * heads,
        in_specs=[VMEM] * (4 + pairs),
        out_specs=[VMEM] * heads,
        scratch_shapes=[pltpu.VMEM((block, width), jnp.bfloat16)],
        compiler_params=params(8),
        cost_estimate=pl.CostEstimate(
            flops=2 * block * width * cols * heads,
            bytes_accessed=width * cols * heads * 2,
            transcendentals=0,
        ),
        name="project_late",
    )(*inner, *relayed, *weights)


def attend_slots(info, docs, sets, query_slots, chips, prefetch):
    count = len(sets[0][1])
    block = sets[0][1][0].shape[0] // len(sets[0][0])
    total = count * chips * block
    window = min(total // 2 + block, total)
    scale = 1.0 / math.sqrt(HDIM)

    kept = len(prefetch.slots)

    def kernel(info_ref, *refs):
        ins, refs = refs[: len(sets) * count], refs[len(sets) * count :]
        next_ref, outs, kept_refs = refs[0], refs[1 : 1 + count], refs[1 + count : 1 + count + kept]
        keys_ref, values_ref, sems = refs[1 + count + kept :]
        prefetch.start(info_ref, next_ref, kept_refs, sems)

        @pl.when(mesh_place()[1] >= 0)
        def _():
            mu, chip, core = mesh_place()
            own_first = core * (block // 2)

            def slot_rows(d, slot, part):
                for i, (slots, _) in enumerate(sets):
                    if slot in slots:
                        at = slots.index(slot) * block
                        return ins[i * count + d][at : at + block, part * HDIM : (part + 1) * HDIM]

            for d in range(count):
                for slot in range(chips):
                    index = jnp.bitwise_xor(mu, d) * chips + jnp.bitwise_xor(chip, slot)
                    place = pl.ds(pl.multiple_of(index * block, block), block)
                    keys_ref[place, :] = slot_rows(d, slot, 1)
                    values_ref[place, :] = slot_rows(d, slot, 2)

            ends = [info_ref[chips + i] for i in range(docs)]
            row_place = lax.broadcasted_iota(jnp.int32, (block, 1), 0) + own_first
            row_place = jnp.where(row_place >= block, row_place - block, row_place)
            key_iota = lax.broadcasted_iota(jnp.int32, (1, window), 1)
            key_in_block = key_iota % block + own_first
            key_in_block = jnp.where(key_in_block >= block, key_in_block - block, key_in_block)
            key_place = (key_iota // block) * block + key_in_block
            for n, slot in enumerate(query_slots):
                for d in range(count):
                    index = jnp.bitwise_xor(mu, d) * chips + jnp.bitwise_xor(chip, slot)
                    first_row = index * block
                    doc_first = jnp.int32(0)
                    for e in ends:
                        doc_first = jnp.where(first_row >= e, e, doc_first)
                    start = jnp.minimum(doc_first // block, (total - window) // block) * block
                    start = pl.multiple_of(start, block)
                    row_pos = row_place + first_row
                    row_first = jnp.zeros((block, 1), jnp.int32)
                    for e in ends:
                        row_first = jnp.where(row_pos >= e, e, row_first)
                    key_pos = key_place + start
                    allowed = (key_pos <= row_pos) & (key_pos >= row_first)
                    scores = lax.dot_general(
                        slot_rows(d, slot, 0),
                        keys_ref[pl.ds(start, window), :],
                        (((1,), (1,)), ((), ())),
                        preferred_element_type=jnp.float32,
                    )
                    scores = jnp.where(allowed, scores * scale, -1e30)
                    row_max = jnp.max(scores, axis=1, keepdims=True)
                    weights = jnp.where(allowed, jnp.exp(scores - row_max), 0.0)
                    totals = jnp.sum(weights, axis=1, keepdims=True)
                    summed = jnp.dot(
                        weights.astype(jnp.bfloat16),
                        values_ref[pl.ds(start, window), :],
                        preferred_element_type=jnp.float32,
                    )
                    outs[d][n * block : (n + 1) * block, :] = (summed / totals).astype(jnp.bfloat16)

        prefetch.wait(info_ref, next_ref, kept_refs, sems)

    n_queries = len(query_slots) * count
    return pl.pallas_call(
        kernel,
        out_shape=[pltpu.VMEM((len(query_slots) * block, HDIM), jnp.bfloat16)] * count
        + prefetch.shapes,
        in_specs=[SMEM] + [VMEM] * (len(sets) * count) + [HBM],
        out_specs=[VMEM] * (count + kept),
        scratch_shapes=[
            pltpu.VMEM((total, HDIM), jnp.bfloat16),
            pltpu.VMEM((total, HDIM), jnp.bfloat16),
            prefetch.scratch,
        ],
        compiler_params=params(14),
        cost_estimate=pl.CostEstimate(
            flops=n_queries * block * window * HDIM * 8,
            bytes_accessed=3 * total * HDIM * 2,
            transcendentals=n_queries * block * window,
        ),
        name="attend_slots",
    )(info, *[piece for _, pieces in sets for piece in pieces], prefetch.weight)


def output_rows(pieces, weight):
    count = len(pieces)
    block = pieces[0].shape[0]
    half = block // 2
    depth, width = weight.shape
    tile = min(1024, width)

    def kernel(*refs):
        ins = refs[:count]
        weight_ref, own_ref, partner_ref, heads_ref = refs[count:]
        for d in range(count):
            heads_ref[jnp.bitwise_xor(mesh_place()[0], d)] = ins[d][...]
        rows = jnp.concatenate([heads_ref[h] for h in range(count)], axis=1)
        for first in range(0, width, tile):
            cols = slice(first, first + tile)
            result = jnp.dot(rows, weight_ref[:, cols], preferred_element_type=jnp.float32)
            result = result.astype(jnp.bfloat16)
            own_ref[:, cols] = result[:half]
            partner_ref[:, cols] = result[half:]

    return pl.pallas_call(
        kernel,
        out_shape=[pltpu.VMEM((half, width), jnp.bfloat16)] * 2,
        in_specs= [VMEM] * (count + 1),
        out_specs=[VMEM] * 2,
        scratch_shapes=[pltpu.VMEM((count, block, HDIM), jnp.bfloat16)],
        compiler_params=params(8),
        cost_estimate=pl.CostEstimate(
            flops=2 * block * depth * width,
            bytes_accessed=depth * width * 2,
            transcendentals=0,
        ),
        name="output_rows",
    )(*pieces, weight)


def in_vmem(*values):
    return [pltpu.with_memory_space_constraint(value, pltpu.VMEM) for value in values]


def add_rows(first, second):
    def kernel(first_ref, second_ref, out_ref):
        total = first_ref[...].astype(jnp.float32) + second_ref[...].astype(jnp.float32)
        out_ref[...] = total.astype(jnp.bfloat16)

    return pl.pallas_call(
        kernel,
        out_shape=pltpu.VMEM(first.shape, jnp.bfloat16),
        in_specs=[VMEM, VMEM],
        out_specs=VMEM,
        compiler_params=params(4),
        cost_estimate=pl.CostEstimate(
            flops=4 * first.size, bytes_accessed=6 * first.size, transcendentals=0
        ),
        name="add_rows",
    )(*in_vmem(first, second))


def relay_rows(chips, own, partner, passing):
    def kernel(own_ref, partner_ref, passing_ref, out_ref):
        middle = is_middle(chips)

        @pl.when(middle)
        def _():
            total = own_ref[...].astype(jnp.float32) + partner_ref[...].astype(jnp.float32)
            total = total + passing_ref[...].astype(jnp.float32)
            out_ref[...] = total.astype(jnp.bfloat16)

        @pl.when(jnp.logical_not(middle))
        def _():
            total = own_ref[...].astype(jnp.float32) + partner_ref[...].astype(jnp.float32)
            out_ref[...] = total.astype(jnp.bfloat16)

    return pl.pallas_call(
        kernel,
        out_shape=pltpu.VMEM(own.shape, jnp.bfloat16),
        in_specs=[VMEM] * 3,
        out_specs=VMEM,
        compiler_params=params(4),
        cost_estimate=pl.CostEstimate(
            flops=4 * own.size, bytes_accessed=8 * own.size, transcendentals=0
        ),
        name="relay_rows",
    )(*in_vmem(own, partner, passing))


def last_rows(early, first, second):
    rows, width = first.shape
    parts = 4
    part = rows // parts

    def kernel(early_ref, first_ref, second_ref, out_ref, done_ref, sems):
        copies = []
        for i in range(parts):
            at = pl.ds(i * part, part)
            total = early_ref[at] + first_ref[at].astype(jnp.float32)
            total = total + second_ref[at].astype(jnp.float32)
            done_ref[at] = total.astype(jnp.bfloat16)
            copies.append(pltpu.make_async_copy(done_ref.at[at], out_ref.at[at], sems.at[i]))
            copies[i].start()
        for copy in copies:
            copy.wait()

    return pl.pallas_call(
        kernel,
        out_shape=pltpu.HBM(first.shape, jnp.bfloat16),
        in_specs=[VMEM] * 3,
        out_specs=HBM,
        scratch_shapes=[
            pltpu.VMEM((rows, width), jnp.bfloat16),
            pltpu.SemaphoreType.DMA((parts,)),
        ],
        compiler_params=params(6),
        cost_estimate=pl.CostEstimate(
            flops=4 * first.size, bytes_accessed=10 * first.size, transcendentals=0
        ),
        name="last_rows",
    )(*in_vmem(early, first, second))


def chip_pairs(pairs):
    return [(2 * a + core, 2 * b + core) for a, b in pairs for core in range(2)]


def line_body(tokens, norm_gain, qkv_weight, out_weight, modality, doc_lengths):
    seq_count = lax.axis_size("seq")
    mod_count = lax.axis_size("mod")
    chips = seq_count // 2
    qkv_weight = pltpu.with_memory_space_constraint(qkv_weight, pltpu.HBM)
    out_weight = pltpu.with_memory_space_constraint(out_weight, pltpu.HBM)

    def along(value, pairs):
        return lax.ppermute(value, "seq", chip_pairs(pairs))

    def swap(value):
        return lax.ppermute(value, "seq", [(i, i ^ 1) for i in range(seq_count)])

    def exchange(pieces):
        moved = [pieces[0]]
        for d in range(1, mod_count):
            moved.append(lax.ppermute(pieces[d], "mod", [(i, i ^ d) for i in range(mod_count)]))
        return moved

    in_hbm = [
        pltpu.with_memory_space_constraint(value, pltpu.HBM)
        for value in (modality, doc_lengths, tokens, norm_gain)
    ]
    normed, info = norm_rows(*in_hbm, chips)
    docs = doc_lengths.shape[0]
    two = along(normed, [(i, i ^ 2) for i in range(chips)])
    one = along(normed, [(i, i ^ 1) for i in range(chips)])
    inner = along(normed, [(1, 2), (2, 1)])
    relayed = along(two, [(i, i ^ 1) for i in range(chips)])
    own_pair = (normed, swap(normed))
    two_pair = (two, swap(two))
    one_pair = (one, swap(one))
    inner_pair = (inner, swap(inner))
    relayed_pair = (relayed, swap(relayed))

    *own, late_first = project_slots(
        info, [own_pair], qkv_weight, (0,), ahead=((3, 1, 0),)
    )
    own = exchange(own)
    two_weight, one_weight = fetch_weights(info, qkv_weight, ((2, 2, 0), (1, 2, 0)))
    *mid, late_second = project_slots(
        info,
        [two_pair, one_pair],
        qkv_weight,
        (2, 1),
        ready=(two_weight, one_weight),
        ahead=((3, 1, 1),),
    )
    mid = exchange(mid)
    late = project_late(inner_pair, relayed_pair, (late_first, late_second), 3 * HDIM, chips)
    late = exchange(late)
    sets = (((0,), own), ((2, 1), mid), ((3,), late))

    def attend(slot):
        *rows, kept = attend_slots(info, docs, sets, (slot,), chips, Prefetch(out_weight, (slot,)))
        return exchange(rows), kept

    def finish(pieces, kept):
        own_share, partner_share = output_rows(pieces, kept)
        return own_share, swap(partner_share)

    sum_a = add_rows(*finish(*attend(3)))
    from_one = along(sum_a, [(i, i ^ 1) for i in range(chips)])
    from_inner = along(sum_a, [(1, 2), (2, 1)])
    sum_b = relay_rows(chips, *finish(*attend(2)), from_one)
    from_two = along(sum_b, [(i, i ^ 2) for i in range(chips)])
    sum_c = add_rows(*finish(*attend(1)))
    from_end = along(sum_c, [(i, i ^ 1) for i in range(chips)])
    early = tokens.astype(jnp.float32)
    for share in (*finish(*attend(0)), from_inner):
        early = early + share.astype(jnp.float32)
    return last_rows(early, from_two, from_end)


def solution(mesh):
    fits = mesh.shape["seq"] == 8 and mesh.shape["mod"] == 4

    def body(tokens, norm_gain, qkv_weight, out_weight, modality, doc_lengths):
        whole = tokens.shape[0] * 2 == BLOCK and qkv_weight.shape[2] == 12 * HDIM
        chosen = line_body if fits and whole else general_body
        return chosen(tokens, norm_gain, qkv_weight, out_weight, modality, doc_lengths)

    return jax.shard_map(
        body,
        mesh=mesh,
        in_specs=(
            P(("mod", "seq"), None),
            P(),
            P(None, None, "seq"),
            P(None, "seq", None),
            P(),
            P(),
        ),
        out_specs=P(("mod", "seq"), None),
        check_vma=False,
    )
```
